32 devices in a mesh: dp: 1 (over z), tp: 4 (over y), pp: 8 (over x, core).
Axes of the slice: x: 4, y: 4, z: 1, core: 2. Of those that a mesh axis runs over, the one named last changes fastest.
The devices are a block of a 4x4x8 slice.
Arguments:
- x_in: bfloat16 [2, 2, 384, 1024], P(None, 'dp')
- dy_out: bfloat16 [2, 2, 384, 1024], P(None, 'dp')
- w_qkv: bfloat16 [8, 3, 1024, 16, 64], P('pp', None, None, 'tp')
- b_qkv: bfloat16 [8, 3, 16, 64], P('pp', None, 'tp')
- w_out: bfloat16 [8, 16, 64, 1024], P('pp', 'tp')
- b_out: bfloat16 [8, 1024], P('pp')
- ln_par: bfloat16 [8, 4, 1024], P('pp')
- w_fc1: bfloat16 [8, 1024, 4096], P('pp', None, 'tp')
- b_fc1: bfloat16 [8, 4096], P('pp', 'tp')
- w_fc2: bfloat16 [8, 4096, 1024], P('pp', 'tp')
- b_fc2: bfloat16 [8, 1024], P('pp')
Outputs:
- output 1: bfloat16 [8, 2, 2, 384, 1024], P('pp', None, 'dp')
- output 2: bfloat16 [8, 2, 2, 384, 1024], P('pp', None, 'dp')
- output 3: float32 [8, 3, 1024, 16, 64], P(('dp', 'pp'), None, None, 'tp')
- output 4: float32 [8, 3, 16, 64], P(('dp', 'pp'), None, 'tp')
- output 5: float32 [8, 16, 64, 1024], P(('dp', 'pp'), 'tp')
- output 6: float32 [8, 1024], P(('dp', 'pp'))
- output 7: float32 [8, 4, 1024], P(('dp', 'pp'))
- output 8: float32 [8, 1024, 4096], P(('dp', 'pp'), None, 'tp')
- output 9: float32 [8, 4096], P(('dp', 'pp'), 'tp')
- output 10: float32 [8, 4096, 1024], P(('dp', 'pp'), 'tp')
- output 11: float32 [8, 1024], P(('dp', 'pp'))
All inputs are finite; a program needn't handle non-finite values.
Results may differ from the reference program's by a relative error of at most 0.02.
Values are sent between devices in bfloat16 or wider.
A program may use at most 768 MiB of HBM per device.

```python
import jax
import jax.numpy as jnp
from jax import lax

NUM_STAGES = 8
NUM_MICRO = 2
MICRO_ROWS = 2
SEQ_LEN = 384
D_MODEL = 1024
NUM_HEADS = 16
D_FF = 4096

HEAD_DIM = D_MODEL // NUM_HEADS
LN_EPS = 1e-5


def setup_inputs(seed: int = 0, part: int = 0) -> dict:
    base_key = jax.random.key(seed)
    data_keys = jax.random.split(jax.random.fold_in(base_key, part), 2)
    param_keys = jax.random.split(base_key, 9)
    act_shape = (NUM_MICRO, MICRO_ROWS, SEQ_LEN, D_MODEL)
    in_scale = D_MODEL ** -0.5
    ff_scale = D_FF ** -0.5
    ln_offset = jnp.array([1.0, 0.0, 1.0, 0.0], jnp.float32)[None, :, None]

    def normal_draw(key_item, shape_tuple, draw_scale):
        return jax.random.normal(key_item, shape_tuple, jnp.float32) * draw_scale

    return {
        "x_in": normal_draw(data_keys[0], act_shape, 1.0).astype(jnp.bfloat16),
        "dy_out": normal_draw(data_keys[1], act_shape, 1.0).astype(jnp.bfloat16),
        "w_qkv": normal_draw(param_keys[0], (NUM_STAGES, 3, D_MODEL, NUM_HEADS, HEAD_DIM), in_scale).astype(jnp.bfloat16),
        "b_qkv": normal_draw(param_keys[1], (NUM_STAGES, 3, NUM_HEADS, HEAD_DIM), 0.5).astype(jnp.bfloat16),
        "w_out": normal_draw(param_keys[2], (NUM_STAGES, NUM_HEADS, HEAD_DIM, D_MODEL), in_scale).astype(jnp.bfloat16),
        "b_out": normal_draw(param_keys[3], (NUM_STAGES, D_MODEL), 0.3).astype(jnp.bfloat16),
        "ln_par": (normal_draw(param_keys[4], (NUM_STAGES, 4, D_MODEL), 0.3) + ln_offset).astype(jnp.bfloat16),
        "w_fc1": normal_draw(param_keys[5], (NUM_STAGES, D_MODEL, D_FF), in_scale).astype(jnp.bfloat16),
        "b_fc1": normal_draw(param_keys[6], (NUM_STAGES, D_FF), 0.5).astype(jnp.bfloat16),
        "w_fc2": normal_draw(param_keys[7], (NUM_STAGES, D_FF, D_MODEL), ff_scale).astype(jnp.bfloat16),
        "b_fc2": normal_draw(param_keys[8], (NUM_STAGES, D_MODEL), 0.3).astype(jnp.bfloat16),
    }


def layer_norm(x_act, ln_gain, ln_shift):
    x_wide = x_act.astype(jnp.float32)
    row_mean = jnp.mean(x_wide, axis=-1, keepdims=True)
    centered = x_wide - row_mean
    row_var = jnp.mean(centered * centered, axis=-1, keepdims=True)
    normed = centered * lax.rsqrt(row_var + LN_EPS)
    return (normed * ln_gain.astype(jnp.float32) + ln_shift.astype(jnp.float32)).astype(jnp.bfloat16)


def causal_attention(q_heads, k_heads, v_heads):
    scores = jnp.einsum("bqhe,bkhe->bhqk", q_heads.astype(jnp.float32), k_heads.astype(jnp.float32)) * (HEAD_DIM ** -0.5)
    positions = jnp.arange(SEQ_LEN)
    causal = positions[:, None] >= positions[None, :]
    scores = jnp.where(causal, scores, -1e30)
    attn_probs = jax.nn.softmax(scores, axis=-1).astype(jnp.bfloat16)
    attn_mix = jnp.einsum("bhqk,bkhe->bqhe", attn_probs.astype(jnp.float32), v_heads.astype(jnp.float32))
    return attn_mix.astype(jnp.bfloat16)


def gpt_layer(x_act, w_qkv, b_qkv, w_out, b_out, ln_par, w_fc1, b_fc1, w_fc2, b_fc2):
    h_one = layer_norm(x_act, ln_par[0], ln_par[1])
    qkv_pre = jnp.einsum("bsd,cdhe->bsche", h_one.astype(jnp.float32), w_qkv.astype(jnp.float32)) + b_qkv.astype(jnp.float32)
    qkv_all = qkv_pre.astype(jnp.bfloat16)
    attn_mix = causal_attention(qkv_all[:, :, 0], qkv_all[:, :, 1], qkv_all[:, :, 2])
    attn_sum = jnp.einsum("bshe,hed->bsd", attn_mix.astype(jnp.float32), w_out.astype(jnp.float32))
    x_mid = (x_act.astype(jnp.float32) + attn_sum + b_out.astype(jnp.float32)).astype(jnp.bfloat16)
    h_two = layer_norm(x_mid, ln_par[2], ln_par[3])
    pre_act = jnp.einsum("bsd,df->bsf", h_two.astype(jnp.float32), w_fc1.astype(jnp.float32)) + b_fc1.astype(jnp.float32)
    gelu_out = jax.nn.gelu(pre_act, approximate=True).astype(jnp.bfloat16)
    mlp_sum = jnp.einsum("bsf,fd->bsd", gelu_out.astype(jnp.float32), w_fc2.astype(jnp.float32))
    return (x_mid.astype(jnp.float32) + mlp_sum + b_fc2.astype(jnp.float32)).astype(jnp.bfloat16)


def reference(x_in, dy_out, w_qkv, b_qkv, w_out, b_out, ln_par, w_fc1, b_fc1, w_fc2, b_fc2):
    weights = (w_qkv, b_qkv, w_out, b_out, ln_par, w_fc1, b_fc1, w_fc2, b_fc2)

    def forward_step(x_act, layer_w):
        y_act = gpt_layer(x_act, *layer_w)
        return y_act, (x_act, y_act)

    def backward_step(grad_act, layer_pack):
        layer_in, layer_w = layer_pack
        wide_w = tuple(w_item.astype(jnp.float32) for w_item in layer_w)
        _, pullback = jax.vjp(gpt_layer, layer_in, *wide_w)
        grad_list = pullback(grad_act)
        return grad_list[0], (grad_list[0], grad_list[1:])

    def one_micro(grad_acc, micro_pack):
        x_micro, dy_micro = micro_pack
        _, (stage_in, stage_out) = lax.scan(forward_step, x_micro, weights)
        _, (stage_grad, weight_grad) = lax.scan(backward_step, dy_micro, (stage_in, weights), reverse=True)
        grad_acc = tuple(acc_item + new_item for acc_item, new_item in zip(grad_acc, weight_grad))
        return grad_acc, (stage_out, stage_grad)

    grad_init = tuple(jnp.zeros(w_item.shape, jnp.float32) for w_item in weights)
    grad_sum, (all_out, all_grad) = lax.scan(one_micro, grad_init, (x_in, dy_out))
    h_out = jnp.swapaxes(all_out, 0, 1)
    g_in = jnp.swapaxes(all_grad, 0, 1)
    return (h_out, g_in, grad_sum[0], grad_sum[1], grad_sum[2], grad_sum[3], grad_sum[4], grad_sum[5], grad_sum[6], grad_sum[7], grad_sum[8])
```

```python
import functools

import jax
import jax.numpy as jnp
from jax import lax
from jax.experimental import pallas as pl
from jax.experimental.pallas import tpu as pltpu
from jax.sharding import PartitionSpec as P

LN_EPS = 1e-5
F32 = jnp.float32
BF16 = jnp.bfloat16
MESH = pl.DeviceIdType.MESH
GELU_A = 0.7978845608028654
GELU_B = 0.044715
ANY = pl.BlockSpec(memory_space=pl.ANY)
VMEM = pl.BlockSpec(memory_space=pltpu.VMEM)


def dot_nn(lhs, rhs):
    return jnp.dot(lhs, rhs, preferred_element_type=F32)


def dot_nt(lhs, rhs):
    return lax.dot_general(lhs, rhs, (((1,), (1,)), ((), ())), preferred_element_type=F32)


def dot_tn(lhs, rhs):
    return lax.dot_general(lhs, rhs, (((0,), (0,)), ((), ())), preferred_element_type=F32)


def norm_stats(x_wide):
    row_mean = jnp.mean(x_wide, axis=-1, keepdims=True)
    centered = x_wide - row_mean
    row_var = jnp.mean(centered * centered, axis=-1, keepdims=True)
    inv_std = lax.rsqrt(row_var + LN_EPS)
    return centered * inv_std, inv_std


def norm_backward(x_wide, gain, grad_h):
    normed, inv_std = norm_stats(x_wide)
    g_normed = grad_h * gain
    mean_g = jnp.mean(g_normed, axis=-1, keepdims=True)
    mean_gn = jnp.mean(g_normed * normed, axis=-1, keepdims=True)
    grad_x = (g_normed - mean_g - normed * mean_gn) * inv_std
    return grad_x, jnp.sum(grad_h * normed, axis=0, keepdims=True), jnp.sum(grad_h, axis=0, keepdims=True)


def chain_kernel(stages, tp, chunk, head_dim,
                 x_first, dy_last, wq_own, wo_own, w1_own, w2_own, bias_own, bias_rep,
                 h_all, mid_all, gin_all, gmid_all, mix_all, gqkv_all, x_all, dy_all, small_out,
                 wq, wo, w1, w2, bias, x_buf, dy_buf, qkv, mix, mid, y_buf, gmid, gin, gqkv, dkv, prob, dgelu, acc, hbuf,
                 own_sem, ring_send, ring_recv, fwd_send, fwd_recv, bias_send, bias_recv,
                 hop_send, hop_recv, ag_send, ag_recv, bw_send, bw_recv, gq_send, gq_recv, out_sem, all_send, all_recv):
    stage = lax.axis_index("pp")
    me = lax.axis_index("tp")
    seq_len = x_first.shape[0]
    chunks = seq_len // chunk
    group = wo_own.shape[0]
    heads = group // head_dim
    d_model = x_first.shape[1]
    last = stages - 1
    right, left = lax.rem(me + 1, tp), lax.rem(me + tp - 1, tp)
    not_first, not_last = stage > 0, stage < last
    peers = [lax.rem(me + off, tp) for off in range(1, tp)]

    barrier = pltpu.get_barrier_semaphore()
    for peer in peers:
        pl.semaphore_signal(barrier, inc=1, device_id={"tp": peer}, device_id_type=MESH)

    @pl.when(not_first)
    def _():
        pl.semaphore_signal(barrier, inc=1, device_id={"pp": stage - 1}, device_id_type=MESH)

    @pl.when(not_last)
    def _():
        pl.semaphore_signal(barrier, inc=1, device_id={"pp": stage + 1}, device_id_type=MESH)

    pl.semaphore_wait(barrier, tp - 1 + jnp.minimum(stage, 1) + jnp.minimum(last - stage, 1))

    shards = ((wq_own, wq), (wo_own, wo), (w1_own, w1), (w2_own, w2))

    def half(ref, idx):
        size = ref.shape[0] // 2
        return ref.at[pl.ds(idx * size, size)]

    def ring_copy(w_idx, h_idx, side):
        own, full = shards[w_idx]
        target = right if side == 0 else left
        return pltpu.make_async_remote_copy(
            src_ref=half(own, h_idx), dst_ref=half(full.at[me], h_idx),
            send_sem=ring_send.at[w_idx, h_idx, side], recv_sem=ring_recv.at[w_idx, h_idx, side],
            device_id={"tp": target}, device_id_type=MESH)

    def forward_copy(w_idx, side):
        own, full = shards[w_idx]
        origin = left if side == 0 else right
        target = right if side == 0 else left
        block = half(full.at[origin], side)
        return pltpu.make_async_remote_copy(
            src_ref=block, dst_ref=block,
            send_sem=fwd_send.at[w_idx, side], recv_sem=fwd_recv.at[w_idx, side],
            device_id={"tp": target}, device_id_type=MESH)

    def bias_copy(slot):
        return pltpu.make_async_remote_copy(
            src_ref=bias_own, dst_ref=bias.at[me], send_sem=bias_send.at[slot], recv_sem=bias_recv.at[slot],
            device_id={"tp": peers[slot]}, device_id_type=MESH)

    for w_idx in range(4):
        for h_idx in range(2):
            ring_copy(w_idx, h_idx, 0).start()
            ring_copy(w_idx, 1 - h_idx, 1).start()
        if w_idx == 0:
            for slot in range(tp - 1):
                bias_copy(slot).start()
    own_copies = [pltpu.make_async_copy(own, full.at[me], own_sem.at[w_idx]) for w_idx, (own, full) in enumerate(shards)]
    own_copies.append(pltpu.make_async_copy(bias_own, bias.at[me], own_sem.at[4]))
    first_copy = pltpu.make_async_copy(x_first, x_buf, own_sem.at[5])
    last_copy = pltpu.make_async_copy(dy_last, dy_buf, own_sem.at[6])
    for own_copy in own_copies:
        own_copy.start()

    @pl.when(stage == 0)
    def _():
        first_copy.start()
        first_copy.wait()

    @pl.when(stage == last)
    def _():
        last_copy.start()
        last_copy.wait()

    qkv[...] = jnp.zeros_like(qkv)
    dkv[...] = jnp.zeros_like(dkv)
    small_out[...] = jnp.zeros_like(small_out)

    for w_idx in range(4):
        ring_copy(w_idx, 0, 0).wait_recv()
        forward_copy(w_idx, 0).start()
        ring_copy(w_idx, 1, 1).wait_recv()
        forward_copy(w_idx, 1).start()
    for own_copy in own_copies:
        own_copy.wait()
    for slot in range(tp - 1):
        bias_copy(slot).wait()
    for w_idx in range(4):
        ring_copy(w_idx, 1, 0).wait_recv()
        ring_copy(w_idx, 0, 1).wait_recv()
        forward_copy(w_idx, 0).wait()
        forward_copy(w_idx, 1).wait()
        for h_idx in range(2):
            ring_copy(w_idx, h_idx, 0).wait_send()
            ring_copy(w_idx, h_idx, 1).wait_send()

    rep = bias_rep
    lane = lax.broadcasted_iota(jnp.int32, (chunk, group), 1)
    lane_head = lane // head_dim

    def stack_heads(block):
        zero = jnp.zeros_like(block)
        return jnp.concatenate([jnp.where(lane_head == h_idx, block, zero) for h_idx in range(heads)], axis=0)

    def unstack_heads(stacked):
        total = jnp.where(lane_head == 0, stacked[:chunk], 0.0)
        for h_idx in range(1, heads):
            total = total + jnp.where(lane_head == h_idx, stacked[h_idx * chunk:(h_idx + 1) * chunk], 0.0)
        return total

    def hop_copy(c_idx, forward):
        rows = pl.ds(c_idx * chunk, chunk)
        src, dst, way, target = (y_buf, x_buf, 0, stage + 1) if forward else (gin, dy_buf, 1, stage - 1)
        return pltpu.make_async_remote_copy(
            src_ref=src.at[rows], dst_ref=dst.at[rows],
            send_sem=hop_send.at[way, c_idx], recv_sem=hop_recv.at[way, c_idx],
            device_id={"pp": target}, device_id_type=MESH)

    def fwd_chunk(c_idx, carry):
        rows = pl.ds(pl.multiple_of(c_idx * chunk, chunk), chunk)

        @pl.when(not_first)
        def _():
            hop_copy(c_idx, True).wait_recv()

        normed, _ = norm_stats(x_buf[rows, :].astype(F32))
        hbuf[...] = (normed * rep[0:1, :] + rep[1:2, :]).astype(BF16)

        @pl.loop(0, tp)
        def _(t_idx):
            for part in range(3):
                w_part = wq[t_idx, pl.ds(part * group, group), :]
                b_part = bias[t_idx, 1:2, part * group:(part + 1) * group]
                qkv[part, t_idx, rows, :] = (dot_nt(hbuf[...], w_part) + b_part).astype(BF16)

        row_pos = c_idx * chunk + lax.rem(lax.broadcasted_iota(jnp.int32, (heads * chunk, seq_len), 0), chunk)
        col_pos = lax.broadcasted_iota(jnp.int32, (heads * chunk, seq_len), 1)
        causal = row_pos >= col_pos

        @pl.loop(0, tp)
        def _(t_idx):
            scores = dot_nt(stack_heads(qkv[0, t_idx, rows, :]), qkv[1, t_idx]) * (head_dim ** -0.5)
            scores = jnp.where(causal, scores, -1e30)
            expd = jnp.exp(scores - jnp.max(scores, axis=-1, keepdims=True))
            probs = expd / jnp.sum(expd, axis=-1, keepdims=True)
            prob[c_idx, t_idx] = probs
            mix[t_idx, rows, :] = unstack_heads(dot_nn(probs.astype(BF16), qkv[2, t_idx])).astype(BF16)

        full_mix = jnp.concatenate([mix[t_idx, rows, :] for t_idx in range(tp)], axis=1)
        attn_sum = dot_nn(full_mix, wo[...].reshape(tp * group, d_model))
        x_mid = (x_buf[rows, :].astype(F32) + attn_sum + rep[4:5, :]).astype(BF16)
        mid[rows, :] = x_mid
        normed_two, _ = norm_stats(x_mid.astype(F32))
        hbuf[...] = (normed_two * rep[2:3, :] + rep[3:4, :]).astype(BF16)
        acc[...] = jnp.zeros_like(acc)

        @pl.loop(0, tp)
        def _(t_idx):
            pre = dot_nn(hbuf[...], w1[t_idx]) + bias[t_idx, 0:1, :]
            tanh = jnp.tanh(GELU_A * (pre + GELU_B * (pre * pre * pre)))
            cdf = 0.5 * (1.0 + tanh)
            dgelu[t_idx, rows, :] = cdf + 0.5 * pre * (1.0 - tanh * tanh) * (GELU_A * (1.0 + 3.0 * GELU_B * (pre * pre)))
            acc[...] += dot_nn((pre * cdf).astype(BF16), w2[t_idx])

        y_buf[rows, :] = (mid[rows, :].astype(F32) + acc[...] + rep[5:6, :]).astype(BF16)

        @pl.when(not_last)
        def _():
            hop_copy(c_idx, True).start()

        return carry

    lax.fori_loop(0, chunks, fwd_chunk, 0)

    def ag_copy(kind, slot):
        src, dst = (y_buf, h_all) if kind == 0 else (mid, mid_all)
        return pltpu.make_async_remote_copy(
            src_ref=src, dst_ref=dst.at[me], send_sem=ag_send.at[kind, slot], recv_sem=ag_recv.at[kind, slot],
            device_id={"tp": peers[slot]}, device_id_type=MESH)

    def mix_copy(slot):
        return pltpu.make_async_remote_copy(
            src_ref=mix.at[peers[slot]], dst_ref=mix_all.at[me], send_sem=ag_send.at[2, slot], recv_sem=ag_recv.at[2, slot],
            device_id={"tp": peers[slot]}, device_id_type=MESH)

    for slot in range(tp - 1):
        ag_copy(0, slot).start()
        ag_copy(1, slot).start()
        mix_copy(slot).start()
    fwd_out = [pltpu.make_async_copy(y_buf, h_all.at[me], out_sem.at[0]),
               pltpu.make_async_copy(mid, mid_all.at[me], out_sem.at[1]),
               pltpu.make_async_copy(mix.at[me], mix_all.at[me], out_sem.at[2]),
               pltpu.make_async_copy(x_buf, x_all.at[me], out_sem.at[3])]
    for out_copy in fwd_out:
        out_copy.start()

    def bw_copy(kind, c_idx, slot):
        rows = pl.ds(c_idx * chunk, chunk)
        src, dst = (gmid, gmid_all) if kind == 0 else (gin, gin_all)
        return pltpu.make_async_remote_copy(
            src_ref=src.at[rows], dst_ref=dst.at[me, rows], send_sem=bw_send.at[kind, c_idx, slot], recv_sem=bw_recv.at[kind, c_idx, slot],
            device_id={"tp": peers[slot]}, device_id_type=MESH)

    def gq_copy(c_idx, part, slot):
        rows = pl.ds(c_idx * chunk, chunk)
        return pltpu.make_async_remote_copy(
            src_ref=gqkv.at[peers[slot], part, rows], dst_ref=gqkv_all.at[me, part, rows],
            send_sem=gq_send.at[part, c_idx, slot], recv_sem=gq_recv.at[part, c_idx, slot],
            device_id={"tp": peers[slot]}, device_id_type=MESH)

    def bwd_chunk(step, carry):
        c_idx = chunks - 1 - step
        rows = pl.ds(pl.multiple_of(c_idx * chunk, chunk), chunk)

        @pl.when(not_last)
        def _():
            hop_copy(c_idx, False).wait_recv()

        acc[...] = jnp.zeros_like(acc)

        @pl.loop(0, tp)
        def _(t_idx):
            g_gelu = dot_nt(dy_buf[rows, :], w2[t_idx]).astype(BF16).astype(F32)
            g_pre = (g_gelu * dgelu[t_idx, rows, :]).astype(BF16)
            acc[...] += dot_nt(g_pre, w1[t_idx])

        g_h_two = acc[...].astype(BF16).astype(F32)
        dy_wide = dy_buf[rows, :].astype(F32)
        g_ln, g_gain, g_shift = norm_backward(mid[rows, :].astype(F32), rep[2:3, :], g_h_two)
        g_mid = (dy_wide + g_ln.astype(BF16).astype(F32)).astype(BF16)
        gmid[rows, :] = g_mid
        small_out[2:3, :] += g_gain
        small_out[3:4, :] += g_shift
        small_out[4:5, :] += jnp.sum(g_mid.astype(F32), axis=0, keepdims=True)
        small_out[5:6, :] += jnp.sum(dy_wide, axis=0, keepdims=True)
        acc[...] = jnp.zeros_like(acc)

        @pl.loop(0, tp)
        def _(t_idx):
            g_mix = dot_nt(gmid[rows, :], wo[t_idx]).astype(BF16)
            g_stack = stack_heads(g_mix)
            q_stack = stack_heads(qkv[0, t_idx, rows, :])
            probs = prob[c_idx, t_idx]
            g_prob = dot_nt(g_stack, qkv[2, t_idx]).astype(BF16).astype(F32)
            inner = jnp.sum(g_prob * probs, axis=-1, keepdims=True)
            g_score = (probs * (g_prob - inner) * (head_dim ** -0.5)).astype(BF16)
            gqkv[t_idx, 0, rows, :] = unstack_heads(dot_nn(g_score, qkv[1, t_idx])).astype(BF16)
            dkv[0, t_idx] += dot_tn(g_score, q_stack)
            dkv[1, t_idx] += dot_tn(probs.astype(BF16), g_stack)
            gqkv[t_idx, 1, rows, :] = dkv[0, t_idx, rows, :].astype(BF16)
            gqkv[t_idx, 2, rows, :] = dkv[1, t_idx, rows, :].astype(BF16)
            g_three = jnp.concatenate([gqkv[t_idx, part, rows, :] for part in range(3)], axis=1)
            acc[...] += dot_nn(g_three, wq[t_idx])

        g_h_one = acc[...].astype(BF16).astype(F32)
        g_ln_one, g_gain_one, g_shift_one = norm_backward(x_buf[rows, :].astype(F32), rep[0:1, :], g_h_one)
        gin[rows, :] = (gmid[rows, :].astype(F32) + g_ln_one.astype(BF16).astype(F32)).astype(BF16)
        small_out[0:1, :] += g_gain_one
        small_out[1:2, :] += g_shift_one

        @pl.when(not_first)
        def _():
            hop_copy(c_idx, False).start()

        for slot in range(tp - 1):
            bw_copy(1, c_idx, slot).start()
        for slot in range(tp - 1):
            bw_copy(0, c_idx, slot).start()
            for part in range(3):
                gq_copy(c_idx, part, slot).start()
        return carry

    lax.fori_loop(0, chunks, bwd_chunk, 0)

    bwd_out = [pltpu.make_async_copy(gin, gin_all.at[me], out_sem.at[4]),
               pltpu.make_async_copy(gmid, gmid_all.at[me], out_sem.at[5]),
               pltpu.make_async_copy(gqkv.at[me], gqkv_all.at[me], out_sem.at[6]),
               pltpu.make_async_copy(dy_buf, dy_all.at[me], out_sem.at[7])]
    for out_copy in bwd_out:
        out_copy.start()

    def pass_copy(way, slot):
        src, dst, target = (h_all, x_all, stage + 1) if way == 0 else (gin_all, dy_all, stage - 1)
        origin = peers[slot]
        return pltpu.make_async_remote_copy(
            src_ref=src.at[origin], dst_ref=dst.at[origin], send_sem=all_send.at[way, slot], recv_sem=all_recv.at[way, slot],
            device_id={"pp": target}, device_id_type=MESH)

    def came(make, slot):
        make(slot).wait_recv()

    for slot in range(tp - 1):
        ag_copy(0, slot).wait_recv()

    @pl.when(not_last)
    def _():
        for slot in range(tp - 1):
            pass_copy(0, slot).start()

    for slot in range(tp - 1):
        for c_idx in range(chunks):
            bw_copy(1, c_idx, slot).wait_recv()

    @pl.when(not_first)
    def _():
        for slot in range(tp - 1):
            pass_copy(1, slot).start()

    for slot in range(tp - 1):
        ag_copy(1, slot).wait_recv()
        mix_copy(slot).wait_recv()
        for kind in range(3):
            ag_copy(0 if kind == 0 else 1, slot).wait_send() if kind < 2 else mix_copy(slot).wait_send()
        for c_idx in range(chunks):
            bw_copy(0, c_idx, slot).wait()
            bw_copy(1, c_idx, slot).wait_send()
            for part in range(3):
                gq_copy(c_idx, part, slot).wait()
    for out_copy in fwd_out + bwd_out:
        out_copy.wait()

    @pl.when(not_last)
    def _():
        for c_idx in range(chunks):
            hop_copy(c_idx, True).wait_send()
        for slot in range(tp - 1):
            pass_copy(0, slot).wait_send()
            pass_copy(1, slot).wait_recv()

    @pl.when(not_first)
    def _():
        for c_idx in range(chunks):
            hop_copy(c_idx, False).wait_send()
        for slot in range(tp - 1):
            pass_copy(1, slot).wait_send()
            pass_copy(0, slot).wait_recv()


def run_chain(stages, tp, x_first, dy_last, wq, wo, w1, w2, bias_own, bias_rep, head_dim):
    seq_len, d_model = x_first.shape
    chunk = min(128, seq_len)
    chunks = seq_len // chunk
    group = wo.shape[0]
    heads = group // head_dim
    ff_local = w1.shape[1]
    rows = (tp, seq_len, d_model)
    outs = [jax.ShapeDtypeStruct(rows, BF16)] * 4
    outs += [jax.ShapeDtypeStruct((tp, seq_len, group), BF16), jax.ShapeDtypeStruct((tp, 3, seq_len, group), BF16)]
    outs += [jax.ShapeDtypeStruct(rows, BF16)] * 2 + [jax.ShapeDtypeStruct((8, d_model), F32)]
    act = pltpu.VMEM((seq_len, d_model), BF16)
    dma = pltpu.SemaphoreType.DMA
    scratch = [
        pltpu.VMEM((tp,) + wq.shape, BF16), pltpu.VMEM((tp,) + wo.shape, BF16),
        pltpu.VMEM((tp,) + w1.shape, BF16), pltpu.VMEM((tp,) + w2.shape, BF16),
        pltpu.VMEM((tp,) + bias_own.shape, F32),
        act, act,
        pltpu.VMEM((3, tp, seq_len, group), BF16), pltpu.VMEM((tp, seq_len, group), BF16),
        act, act, act, act,
        pltpu.VMEM((tp, 3, seq_len, group), BF16), pltpu.VMEM((2, tp, seq_len, group), F32),
        pltpu.VMEM((chunks, tp, heads * chunk, seq_len), F32), pltpu.VMEM((tp, seq_len, ff_local), F32),
        pltpu.VMEM((chunk, d_model), F32), pltpu.VMEM((chunk, d_model), BF16),
        dma((7,)), dma((4, 2, 2)), dma((4, 2, 2)), dma((4, 2)), dma((4, 2)), dma((tp - 1,)), dma((tp - 1,)),
        dma((2, chunks)), dma((2, chunks)), dma((3, tp - 1)), dma((3, tp - 1)),
        dma((2, chunks, tp - 1)), dma((2, chunks, tp - 1)), dma((3, chunks, tp - 1)), dma((3, chunks, tp - 1)),
        dma((8,)), dma((2, tp - 1)), dma((2, tp - 1)),
    ]
    return pl.pallas_call(
        functools.partial(chain_kernel, stages, tp, chunk, head_dim),
        out_shape=outs,
        in_specs=[ANY] * 7 + [VMEM],
        out_specs=[ANY] * 8 + [VMEM],
        scratch_shapes=scratch,
        compiler_params=pltpu.CompilerParams(collective_id=0, has_side_effects=True, vmem_limit_bytes=67043328),
        name="chain",
    )(x_first, dy_last, wq, wo, w1, w2, bias_own, bias_rep)


def layer_norm(x_act, ln_gain, ln_shift):
    normed, _ = norm_stats(x_act.astype(F32))
    return (normed * ln_gain + ln_shift).astype(BF16)


def gelu_tanh(pre_act):
    return jax.nn.gelu(pre_act, approximate=True)


def solution(mesh):
    stages = mesh.shape["pp"]
    tp = mesh.shape["tp"]

    def stage_program(x_in, dy_out, w_qkv, b_qkv, w_out, b_out, ln_par, w_fc1, b_fc1, w_fc2, b_fc2):
        micro_count, batch_rows, seq_len, d_model = x_in.shape
        head_dim = w_qkv.shape[4]
        group = w_qkv.shape[3] * head_dim
        ff_local = w_fc1.shape[2]
        seqs = micro_count * batch_rows
        stage = lax.axis_index("pp")
        me = lax.axis_index("tp")
        wq = jnp.transpose(w_qkv[0], (0, 2, 3, 1)).reshape(3 * group, d_model)
        wo = w_out[0].reshape(group, d_model)
        w1, w2 = w_fc1[0], w_fc2[0]
        bias_own = jnp.zeros((8, ff_local), F32)
        bias_own = bias_own.at[0, :].set(b_fc1[0].astype(F32)).at[1, :3 * group].set(b_qkv[0].reshape(3 * group).astype(F32))
        ln_wide = ln_par[0].astype(F32)
        bias_rep = jnp.concatenate([ln_wide, b_out.astype(F32), b_fc2.astype(F32), jnp.zeros((2, d_model), F32)], axis=0)
        x_flat = x_in.reshape(seqs, seq_len, d_model)
        dy_flat = dy_out.reshape(seqs, seq_len, d_model)
        x_first = lax.dynamic_index_in_dim(x_flat, me, 0, keepdims=False)
        dy_last = lax.dynamic_index_in_dim(dy_flat, me, 0, keepdims=False)
        h_all, mid_all, gin_all, gmid_all, mix_all, gqkv_all, x_all, dy_all, small = run_chain(
            stages, tp, x_first, dy_last, wq, wo, w1, w2, bias_own, bias_rep, head_dim)
        small = lax.psum(small, "tp")
        x_all = jnp.where(stage == 0, x_flat, x_all)
        dy_all = jnp.where(stage == stages - 1, dy_flat, dy_all)
        h_two = layer_norm(mid_all, ln_wide[2], ln_wide[3])
        pre_act = jnp.einsum("bsd,df->bsf", h_two, w1, preferred_element_type=F32) + b_fc1[0].astype(F32)
        g_gelu = jnp.einsum("bsd,fd->bsf", dy_all, w2, preferred_element_type=F32).astype(BF16)
        gelu_wide, gelu_pull = jax.vjp(gelu_tanh, pre_act)
        g_pre = gelu_pull(g_gelu.astype(F32))[0]
        g_b_fc1 = jnp.sum(g_pre, axis=(0, 1))
        g_w_fc2 = jnp.einsum("bsf,bsd->fd", gelu_wide.astype(BF16), dy_all, preferred_element_type=F32)
        g_w_fc1 = jnp.einsum("bsd,bsf->df", h_two, g_pre.astype(BF16), preferred_element_type=F32)
        g_w_out = jnp.einsum("bsf,bsd->fd", mix_all, gmid_all, preferred_element_type=F32)
        h_one = layer_norm(x_all, ln_wide[0], ln_wide[1])
        g_w_qkv = jnp.einsum("bcsf,bsd->cfd", gqkv_all, h_one, preferred_element_type=F32)
        g_w_qkv = jnp.transpose(g_w_qkv.reshape(3, group // head_dim, head_dim, d_model), (0, 3, 1, 2))
        g_b_qkv = jnp.sum(gqkv_all.astype(F32), axis=(0, 2)).reshape(3, group // head_dim, head_dim)
        shape = (micro_count, batch_rows, seq_len, d_model)
        grads = (g_w_qkv, g_b_qkv, g_w_out.reshape(group // head_dim, head_dim, d_model), small[4], small[:4], g_w_fc1, g_b_fc1, g_w_fc2, small[5])
        return (h_all.reshape(shape)[None], gin_all.reshape(shape)[None]) + tuple(g_item[None] for g_item in grads)

    act_spec = P(None, "dp", None, None)
    arg_specs = (act_spec, act_spec,
                 P("pp", None, None, "tp", None), P("pp", None, "tp", None), P("pp", "tp", None, None),
                 P("pp", None), P("pp", None, None), P("pp", None, "tp"), P("pp", "tp"),
                 P("pp", "tp", None), P("pp", None))
    stage_spec = P("pp", None, "dp", None, None)
    grad_axes = ("dp", "pp")
    result_specs = (stage_spec, stage_spec,
                    P(grad_axes, None, None, "tp", None), P(grad_axes, None, "tp", None), P(grad_axes, "tp", None, None),
                    P(grad_axes, None), P(grad_axes, None, None), P(grad_axes, None, "tp"), P(grad_axes, "tp"),
                    P(grad_axes, "tp", None), P(grad_axes, None))
    return jax.shard_map(stage_program, mesh=mesh, in_specs=arg_specs, out_specs=result_specs, check_vma=False)
```

```python
import functools

import jax
import jax.numpy as jnp
from jax import lax
from jax.experimental import pallas as pl
from jax.experimental.pallas import tpu as pltpu
from jax.sharding import PartitionSpec as P

LN_EPS = 1e-5
F32 = jnp.float32
BF16 = jnp.bfloat16
MESH = pl.DeviceIdType.MESH
GELU_A = 0.7978845608028654
GELU_B = 0.044715
LOG2_E = 1.4426950408889634
ANY = pl.BlockSpec(memory_space=pl.ANY)
VMEM = pl.BlockSpec(memory_space=pltpu.VMEM)


def dot_nn(lhs, rhs):
    return jnp.dot(lhs, rhs, preferred_element_type=F32)


def dot_nt(lhs, rhs):
    return lax.dot_general(lhs, rhs, (((1,), (1,)), ((), ())), preferred_element_type=F32)


def dot_tn(lhs, rhs):
    return lax.dot_general(lhs, rhs, (((0,), (0,)), ((), ())), preferred_element_type=F32)


def norm_stats(x_wide):
    row_mean = jnp.mean(x_wide, axis=-1, keepdims=True)
    centered = x_wide - row_mean
    row_var = jnp.mean(centered * centered, axis=-1, keepdims=True)
    inv_std = lax.rsqrt(row_var + LN_EPS)
    return centered * inv_std, inv_std


def norm_backward(x_wide, gain, grad_h):
    normed, inv_std = norm_stats(x_wide)
    g_normed = grad_h * gain
    mean_g = jnp.mean(g_normed, axis=-1, keepdims=True)
    mean_gn = jnp.mean(g_normed * normed, axis=-1, keepdims=True)
    grad_x = (g_normed - mean_g - normed * mean_gn) * inv_std
    return grad_x, jnp.sum(grad_h * normed, axis=0, keepdims=True), jnp.sum(grad_h, axis=0, keepdims=True)


def gelu_parts(pre):
    square = pre * pre
    tanh = jnp.tanh(pre * (GELU_A + (GELU_A * GELU_B) * square))
    cdf = 0.5 + 0.5 * tanh
    return cdf, cdf + pre * (0.5 * GELU_A + (1.5 * GELU_A * GELU_B) * square) * (1.0 - tanh * tanh)


def chain_kernel(stages, tp, chunk, head_dim,
                 x_flat, dy_flat, wq_own, wo_own, w1_own, w2_own, params,
                 h_all, mid_all, gin_all, gmid_all, mix_all, gqkv_all, x_all, dy_all, h_one_all, h_two_all, act_all, gpre_all, slope_all, small_out,
                 wq, wq_t, wo, w1, w2, bias, x_buf, dy_buf, qkv, mix, mid, y_buf, gmid, gin, dkv, prob, dgelu, acc, hbuf, small,
                 own_sem, go_sem, done_sem, ring_send, ring_recv, fwd_send, fwd_recv, bias_send, bias_recv,
                 hop_send, hop_recv, ag_send, ag_recv, mix_send, mix_recv, bw_send, bw_recv, gq_send, gq_recv,
                 out_sem, px_send, px_recv, py_send, py_recv, sum_send, sum_recv, prep_sem, post_sem):
    stage = lax.axis_index("pp")
    me = lax.axis_index("tp")
    seq_len, d_model = x_buf.shape
    chunks = seq_len // chunk
    group = wo_own.shape[0]
    heads = group // head_dim
    last = stages - 1
    right, left = lax.rem(me + 1, tp), lax.rem(me + tp - 1, tp)
    not_first, not_last = stage > 0, stage < last
    peers = [lax.rem(me + off, tp) for off in range(1, tp)]
    even = lax.rem(stage, 2) == 0
    score_scale = head_dim ** -0.5

    def remote(src, dst, send, recv, axis, target):
        return pltpu.make_async_remote_copy(src_ref=src, dst_ref=dst, send_sem=send, recv_sem=recv,
                                            device_id={axis: target}, device_id_type=MESH)

    small[...] = jnp.zeros_like(small)
    small_out[...] = jnp.zeros_like(small_out)
    barrier = pltpu.get_barrier_semaphore()
    for peer in peers:
        pl.semaphore_signal(barrier, inc=1, device_id={"tp": peer}, device_id_type=MESH)

    @pl.when(not_first)
    def _():
        pl.semaphore_signal(barrier, inc=1, device_id={"pp": stage - 1}, device_id_type=MESH)

    @pl.when(not_last)
    def _():
        pl.semaphore_signal(barrier, inc=1, device_id={"pp": stage + 1}, device_id_type=MESH)

    pl.semaphore_wait(barrier, tp - 1 + jnp.minimum(stage, 1) + jnp.minimum(last - stage, 1))

    def shard(w_idx, origin):
        if w_idx == 1:
            return wo.at[pl.ds(pl.multiple_of(origin * group, group), group)]
        return (wq, None, w1, w2)[w_idx].at[origin]

    owns = (wq_own, wo_own, w1_own, w2_own)

    def half(ref, idx):
        size = ref.shape[0] // 2
        return ref.at[pl.ds(idx * size, size)]

    def ring_copy(w_idx, h_idx, side):
        return remote(half(owns[w_idx], h_idx), half(shard(w_idx, me), h_idx),
                      ring_send.at[w_idx, h_idx, side], ring_recv.at[w_idx, h_idx, side], "tp", left if side else right)

    def forward_copy(w_idx, side):
        block = half(shard(w_idx, right if side else left), side)
        return remote(block, block, fwd_send.at[w_idx, side], fwd_recv.at[w_idx, side], "tp", left if side else right)

    def bias_copy(slot):
        return remote(params.at[pl.ds(0, 8)], bias.at[me], bias_send.at[slot], bias_recv.at[slot], "tp", peers[slot])

    own_copies = [pltpu.make_async_copy(owns[w_idx], shard(w_idx, me), own_sem.at[w_idx]) for w_idx in range(4)]
    own_copies.append(pltpu.make_async_copy(params.at[pl.ds(0, 8)], bias.at[me], own_sem.at[4]))
    for own_copy in own_copies:
        own_copy.start()
    for slot in range(tp - 1):
        bias_copy(slot).start()

    def own_input(src, buf, dst):
        bounce = (y_buf, mid, gmid)
        copies = [pltpu.make_async_copy(src.at[me], buf, own_sem.at[5])]
        copies += [pltpu.make_async_copy(src.at[peers[slot]], bounce[slot], own_sem.at[6 + slot]) for slot in range(tp - 1)]
        for copy in copies:
            copy.start()
        for copy in copies:
            copy.wait()
        copies = [pltpu.make_async_copy(bounce[slot], dst.at[peers[slot]], own_sem.at[6 + slot]) for slot in range(tp - 1)]
        for copy in copies:
            copy.start()
        for copy in copies:
            copy.wait()

    @pl.when(jnp.logical_not(even))
    def _():
        pl.semaphore_wait(go_sem, 1)

    for w_idx in range(4):
        for h_idx in range(2):
            ring_copy(w_idx, h_idx, 0).start()
            ring_copy(w_idx, 1 - h_idx, 1).start()

    @pl.when(stage == 0)
    def _():
        own_input(x_flat, x_buf, x_all)

    @pl.when(stage == last)
    def _():
        own_input(dy_flat, dy_buf, dy_all)

    qkv[...] = jnp.zeros_like(qkv)
    dkv[...] = jnp.zeros_like(dkv)

    for w_idx in range(4):
        ring_copy(w_idx, 0, 0).wait_recv()
        forward_copy(w_idx, 0).start()
        ring_copy(w_idx, 1, 1).wait_recv()
        forward_copy(w_idx, 1).start()
    for own_copy in own_copies:
        own_copy.wait()
    for slot in range(tp - 1):
        bias_copy(slot).wait()
    for w_idx in range(4):
        ring_copy(w_idx, 1, 0).wait_recv()
        ring_copy(w_idx, 0, 1).wait_recv()
        forward_copy(w_idx, 0).wait()
        forward_copy(w_idx, 1).wait()
        for h_idx in range(2):
            ring_copy(w_idx, h_idx, 0).wait_send()
            ring_copy(w_idx, h_idx, 1).wait_send()
        if w_idx == 0:
            @pl.loop(0, tp)
            def _(t_idx):
                for part in range(3):
                    wq_t[t_idx, :, part * group:(part + 1) * group] = wq[t_idx, part * group:(part + 1) * group, :].T

    @pl.when(even)
    def _():
        pl.semaphore_signal(go_sem, inc=1, device_id={"pp": stage + 1}, device_id_type=MESH)

    @pl.when(jnp.logical_not(even))
    def _():
        pl.semaphore_signal(done_sem, inc=1, device_id={"pp": stage - 1}, device_id_type=MESH)

    rep = params.at[pl.ds(8, 8)]
    lane_head = lax.broadcasted_iota(jnp.int32, (chunk, group), 1) // head_dim

    def stack_heads(block):
        zero = jnp.zeros_like(block)
        return jnp.concatenate([jnp.where(lane_head == h_idx, block, zero) for h_idx in range(heads)], axis=0)

    def unstack_heads(stacked):
        total = stacked[:chunk]
        for h_idx in range(1, heads):
            total = jnp.where(lane_head == h_idx, stacked[h_idx * chunk:(h_idx + 1) * chunk], total)
        return total

    def hop_copy(c_idx, forward):
        rows = pl.ds(c_idx * chunk, chunk)
        src, dst, way, target = (y_buf, x_buf, 0, stage + 1) if forward else (gin, dy_buf, 1, stage - 1)
        return remote(src.at[rows], dst.at[rows], hop_send.at[way, c_idx], hop_recv.at[way, c_idx], "pp", target)

    def fwd_chunk(c_idx, carry):
        rows = pl.ds(pl.multiple_of(c_idx * chunk, chunk), chunk)

        @pl.when(not_first)
        def _():
            hop_copy(c_idx, True).wait_recv()

        normed, _ = norm_stats(x_buf[rows, :].astype(F32))
        hbuf[...] = (normed * rep[0:1, :] + rep[1:2, :]).astype(BF16)

        groups = range(tp)
        for t_idx in groups:
            pre = dot_nn(hbuf[...], wq_t[t_idx]) + bias[t_idx, 1:2, :3 * group]
            for part in range(3):
                qkv[part, t_idx, rows, :] = pre[:, part * group:(part + 1) * group].astype(BF16)

        row_pos = c_idx * chunk + lax.rem(lax.broadcasted_iota(jnp.int32, (heads * chunk, seq_len), 0), chunk)
        causal = row_pos >= lax.broadcasted_iota(jnp.int32, (heads * chunk, seq_len), 1)
        all_scores = [dot_nt(stack_heads(qkv[0, t_idx, rows, :]), qkv[1, t_idx]) for t_idx in groups]
        all_probs = []
        for t_idx in groups:
            scores = jnp.where(causal, all_scores[t_idx], -1e30)
            expd = jnp.exp2((scores - jnp.max(scores, axis=-1, keepdims=True)) * (score_scale * LOG2_E))
            probs = expd * (1.0 / jnp.sum(expd, axis=-1, keepdims=True))
            prob[c_idx, t_idx] = probs
            all_probs.append(probs.astype(BF16))
        for t_idx in groups:
            mix[t_idx, rows, :] = unstack_heads(dot_nn(all_probs[t_idx], qkv[2, t_idx])).astype(BF16)

        full_mix = jnp.concatenate([mix[t_idx, rows, :] for t_idx in groups], axis=1)
        x_mid = (x_buf[rows, :].astype(F32) + dot_nn(full_mix, wo[...]) + rep[4:5, :]).astype(BF16)
        mid[rows, :] = x_mid
        normed_two, _ = norm_stats(x_mid.astype(F32))
        hbuf[...] = (normed_two * rep[2:3, :] + rep[3:4, :]).astype(BF16)
        total = jnp.zeros((chunk, d_model), F32)
        for t_idx in groups:
            pre = dot_nn(hbuf[...], w1[t_idx]) + bias[t_idx, 0:1, :]
            cdf, slope = gelu_parts(pre)
            dgelu[t_idx, rows, :] = slope
            total = total + dot_nn((pre * cdf).astype(BF16), w2[t_idx])

        y_buf[rows, :] = (mid[rows, :].astype(F32) + total + rep[5:6, :]).astype(BF16)

        @pl.when(not_last)
        def _():
            hop_copy(c_idx, True).start()

        return carry

    lax.fori_loop(0, chunks, fwd_chunk, 0)

    def ag_copy(kind, side):
        src, dst = ((y_buf, h_all), (mid, mid_all), (gmid, gmid_all))[kind]
        return remote(src, dst.at[me], ag_send.at[kind, side], ag_recv.at[kind, side], "tp", left if side else right)

    def ag_forward(kind, side):
        rows = pl.ds(side * (seq_len // 2), seq_len // 2)
        block = (h_all, mid_all, gmid_all)[kind].at[right if side else left, rows]
        return remote(block, block, ag_send.at[kind, 2 + side], ag_recv.at[kind, 2 + side], "tp", left if side else right)

    def mix_copy(slot):
        return remote(mix.at[peers[slot]], mix_all.at[me], mix_send.at[slot], mix_recv.at[slot], "tp", peers[slot])

    def start_fwd_gather():
        for kind in range(2):
            for side in range(2):
                ag_copy(kind, side).start()
        for slot in range(tp - 1):
            mix_copy(slot).start()

    @pl.when(jnp.logical_not(even))
    def _():
        start_fwd_gather()

    fwd_out = [pltpu.make_async_copy(y_buf, h_all.at[me], out_sem.at[0]),
               pltpu.make_async_copy(mid, mid_all.at[me], out_sem.at[1]),
               pltpu.make_async_copy(mix.at[me], mix_all.at[me], out_sem.at[2]),
               pltpu.make_async_copy(x_buf, x_all.at[me], out_sem.at[3])]
    for out_copy in fwd_out:
        out_copy.start()

    def pass_x(slot):
        origin = peers[slot]
        return remote(h_all.at[origin], x_all.at[origin], px_send.at[slot], px_recv.at[slot], "pp", stage + 1)

    def finish_fwd_gather():
        for kind in range(2):
            for side in range(2):
                ag_copy(kind, side).wait_recv()
                ag_forward(kind, side).start()
        for kind in range(2):
            for side in range(2):
                ag_forward(kind, side).wait_recv()

        @pl.when(not_last)
        def _():
            for slot in range(tp - 1):
                pass_x(slot).start()

    size = group

    def flip(ref_get, ref_set, count):
        for row in range(count):
            ref_set(row, row, ref_get(row, row).T)
            for col in range(row):
                upper, lower = ref_get(col, row).T, ref_get(row, col).T
                ref_set(row, col, upper)
                ref_set(col, row, lower)

    def tile(row, col):
        return slice(row * size, (row + 1) * size), slice(col * size, (col + 1) * size)

    @pl.loop(0, tp)
    def _(t_idx):
        for ref in (w2, w1):
            def ref_set(row, col, value, ref=ref):
                ref[(t_idx,) + tile(row, col)] = value

            flip(lambda row, col, ref=ref: ref[(t_idx,) + tile(row, col)], ref_set, d_model // size)

    def wo_set(row, col, value):
        wo[tile(row, col)] = value

    flip(lambda row, col: wo[tile(row, col)], wo_set, d_model // size)

    @pl.when(even)
    def _():
        pl.semaphore_wait(done_sem, 1)
        start_fwd_gather()

    @pl.when(stage < stages // 2)
    def _():
        finish_fwd_gather()

    def bw_copy(c_idx, side):
        rows = pl.ds(c_idx * chunk, chunk)
        return remote(gin.at[rows], gin_all.at[me, rows], bw_send.at[c_idx, side], bw_recv.at[c_idx, side], "tp", left if side else right)

    def bw_forward(c_idx, side):
        rows = pl.ds(c_idx * chunk + side * (chunk // 2), chunk // 2)
        block = gin_all.at[right if side else left, rows]
        return remote(block, block, bw_send.at[c_idx, 2 + side], bw_recv.at[c_idx, 2 + side], "tp", left if side else right)

    def gqkv_of(t_idx):
        return wq_t.at[t_idx, pl.ds(0, seq_len)]

    def gq_copy(slot):
        return remote(gqkv_of(peers[slot]), gqkv_all.at[me], gq_send.at[slot], gq_recv.at[slot], "tp", peers[slot])

    def pass_dy(c_idx, slot):
        rows = pl.ds(c_idx * chunk, chunk)
        origin = peers[slot]
        return remote(gin_all.at[origin, rows], dy_all.at[origin, rows], py_send.at[c_idx, slot], py_recv.at[c_idx, slot], "pp", stage - 1)

    def forward_chunk(c_idx):
        for side in range(2):
            bw_copy(c_idx, side).wait_recv()
            bw_forward(c_idx, side).start()

    def pass_chunk(c_idx):
        for side in range(2):
            bw_forward(c_idx, side).wait_recv()

        @pl.when(not_first)
        def _():
            for slot in range(tp - 1):
                pass_dy(c_idx, slot).start()

    w1_own_t, w2_own_t = w1.at[me], w2.at[me]
    early = stage < stages // 2 - 1

    def prep(two_buf, one_buf, act_buf, keep_slopes):
        @pl.when(not_first)
        def _():
            for slot in range(tp - 1):
                pass_x(slot).wait_recv()

        def prep_seq(t_idx, carry):
            loads = [pltpu.make_async_copy(mid_all.at[t_idx], two_buf, prep_sem.at[0]), pltpu.make_async_copy(x_all.at[t_idx], one_buf, prep_sem.at[1])]
            for load in loads:
                load.start()
            for load in loads:
                load.wait()

            def prep_rows(c_idx, inner):
                rows = pl.ds(pl.multiple_of(c_idx * chunk, chunk), chunk)
                normed, _ = norm_stats(two_buf[rows, :].astype(F32))
                two_buf[rows, :] = (normed * rep[2:3, :] + rep[3:4, :]).astype(BF16)
                normed_one, _ = norm_stats(one_buf[rows, :].astype(F32))
                one_buf[rows, :] = (normed_one * rep[0:1, :] + rep[1:2, :]).astype(BF16)
                pre = dot_nt(two_buf[rows, :], w1_own_t[...]) + bias[me, 0:1, :]
                cdf, slope = gelu_parts(pre)
                act_buf[rows, :] = (pre * cdf).astype(BF16)
                if keep_slopes:
                    keep = pltpu.make_async_copy(acc, slope_all.at[t_idx, rows], prep_sem.at[2])

                    @pl.when(c_idx > 0)
                    def _():
                        keep.wait()

                    acc[...] = slope
                    keep.start()
                else:
                    dgelu[t_idx, rows, :] = slope
                return inner

            lax.fori_loop(0, chunks, prep_rows, 0)
            if keep_slopes:
                pltpu.make_async_copy(acc, slope_all.at[t_idx, pl.ds(0, chunk)], prep_sem.at[2]).wait()
            keeps = [pltpu.make_async_copy(two_buf, h_two_all.at[t_idx], prep_sem.at[0]), pltpu.make_async_copy(one_buf, h_one_all.at[t_idx], prep_sem.at[1]),
                     pltpu.make_async_copy(act_buf, act_all.at[t_idx], prep_sem.at[2])]
            for keep in keeps:
                keep.start()
            for keep in keeps:
                keep.wait()
            return carry

        lax.fori_loop(0, tp, prep_seq, 0)

    def end_fwd_sends():
        for kind in range(2):
            for side in range(2):
                ag_copy(kind, side).wait_send()
        for slot in range(tp - 1):
            mix_copy(slot).wait_send()
        for out_copy in fwd_out:
            out_copy.wait()

        @pl.when(not_last)
        def _():
            for c_idx in range(chunks):
                hop_copy(c_idx, True).wait_send()

    @pl.when(early)
    def _():
        end_fwd_sends()
        prep(gmid, gin, y_buf, True)

    def bwd_chunk(step, carry):
        c_idx = chunks - 1 - step
        rows = pl.ds(pl.multiple_of(c_idx * chunk, chunk), chunk)

        @pl.when(not_last)
        def _():
            hop_copy(c_idx, False).wait_recv()

        groups = range(tp)
        g_h_sum = jnp.zeros((chunk, d_model), F32)
        for t_idx in groups:
            g_gelu = dot_nn(dy_buf[rows, :], w2[t_idx]).astype(BF16).astype(F32)
            g_h_sum = g_h_sum + dot_nn((g_gelu * dgelu[t_idx, rows, :]).astype(BF16), w1[t_idx])

        g_h_two = g_h_sum.astype(BF16).astype(F32)
        dy_wide = dy_buf[rows, :].astype(F32)
        g_ln, g_gain, g_shift = norm_backward(mid[rows, :].astype(F32), rep[2:3, :], g_h_two)
        g_mid = (dy_wide + g_ln.astype(BF16).astype(F32)).astype(BF16)
        gmid[rows, :] = g_mid
        small[me, 2:3, :] += g_gain
        small[me, 3:4, :] += g_shift
        small[me, 4:5, :] += jnp.sum(g_mid.astype(F32), axis=0, keepdims=True)
        small[me, 5:6, :] += jnp.sum(dy_wide, axis=0, keepdims=True)
        g_mix_all = dot_nn(gmid[rows, :], wo[...]).astype(BF16)
        g_stacks = [stack_heads(g_mix_all[:, t_idx * group:(t_idx + 1) * group]) for t_idx in groups]
        g_probs = [dot_nt(g_stacks[t_idx], qkv[2, t_idx]).astype(BF16).astype(F32) for t_idx in groups]
        g_values = [dot_tn(prob[c_idx, t_idx].astype(BF16), g_stacks[t_idx]) for t_idx in groups]
        g_scores = []
        for t_idx in groups:
            probs = prob[c_idx, t_idx]
            inner = jnp.sum(g_probs[t_idx] * probs, axis=-1, keepdims=True)
            g_scores.append((probs * (g_probs[t_idx] - inner)).astype(BF16))
            dkv[1, t_idx] += g_values[t_idx]
        for t_idx in groups:
            wq_t[t_idx, rows, 0:group] = (unstack_heads(dot_nn(g_scores[t_idx], qkv[1, t_idx])) * score_scale).astype(BF16)
            dkv[0, t_idx] += dot_tn(g_scores[t_idx], stack_heads(qkv[0, t_idx, rows, :])) * score_scale
        g_h_sum = jnp.zeros((chunk, d_model), F32)
        for t_idx in groups:
            wq_t[t_idx, rows, group:2 * group] = dkv[0, t_idx, rows, :].astype(BF16)
            wq_t[t_idx, rows, 2 * group:3 * group] = dkv[1, t_idx, rows, :].astype(BF16)
            g_h_sum = g_h_sum + dot_nn(wq_t[t_idx, rows, :], wq[t_idx])

        g_h_one = g_h_sum.astype(BF16).astype(F32)
        g_ln_one, g_gain_one, g_shift_one = norm_backward(x_buf[rows, :].astype(F32), rep[0:1, :], g_h_one)
        gin[rows, :] = (gmid[rows, :].astype(F32) + g_ln_one.astype(BF16).astype(F32)).astype(BF16)
        small[me, 0:1, :] += g_gain_one
        small[me, 1:2, :] += g_shift_one

        @pl.when(not_first)
        def _():
            hop_copy(c_idx, False).start()

        for side in range(2):
            bw_copy(c_idx, side).start()

        @pl.when((step >= 2) & (stage < last - 1))
        def _():
            forward_chunk(c_idx + 2)

        return carry

    lax.fori_loop(0, chunks, bwd_chunk, 0)

    def sum_copy(slot):
        return remote(small.at[me], small.at[me], sum_send.at[slot], sum_recv.at[slot], "tp", peers[slot])

    for slot in range(tp - 1):
        sum_copy(slot).start()
    bwd_out = [pltpu.make_async_copy(gin, gin_all.at[me], out_sem.at[4]),
               pltpu.make_async_copy(gmid, gmid_all.at[me], out_sem.at[5]),
               pltpu.make_async_copy(gqkv_of(me), gqkv_all.at[me], out_sem.at[6]),
               pltpu.make_async_copy(dy_buf, dy_all.at[me], out_sem.at[7])]
    for out_copy in bwd_out:
        out_copy.start()

    @pl.when(stage >= last - 1)
    def _():
        forward_chunk(chunks - 1)

    for c_idx in range(chunks - 2, -1, -1):
        forward_chunk(c_idx)

    @pl.when(stage >= stages // 2)
    def _():
        finish_fwd_gather()

    for side in range(2):
        ag_copy(2, side).start()
    for slot in range(tp - 1):
        gq_copy(slot).start()
    for c_idx in range(chunks - 1, -1, -1):
        pass_chunk(c_idx)

    @pl.when(early)
    def _():
        slopes = pltpu.make_async_copy(slope_all, dgelu, prep_sem.at[0])
        slopes.start()
        slopes.wait()

    @pl.when(jnp.logical_not(early))
    def _():
        end_fwd_sends()
        prep(mid, x_buf, y_buf, False)

    def finish_rows(t_idx, src, dst, rows):
        grad = dot_nn(src[rows, :], w2_own_t[...]).astype(BF16).astype(F32) * dgelu[t_idx, rows, :]
        small_out[6:7, :] += jnp.sum(grad, axis=0, keepdims=True)
        dst[rows, :] = grad.astype(BF16)

    def finish_own(c_idx, carry):
        finish_rows(me, dy_buf, y_buf, pl.ds(pl.multiple_of(c_idx * chunk, chunk), chunk))
        return carry

    lax.fori_loop(0, chunks, finish_own, 0)
    own_keep = pltpu.make_async_copy(y_buf, gpre_all.at[me], prep_sem.at[0])
    own_keep.start()
    for side in range(2):
        ag_copy(2, side).wait_recv()
        ag_forward(2, side).start()
    own_keep.wait()

    def finish_peers(step, carry):
        c_idx = chunks - 1 - step
        rows = pl.ds(pl.multiple_of(c_idx * chunk, chunk), chunk)
        bufs = (x_buf, mid, y_buf)

        @pl.when(not_last)
        def _():
            for slot in range(tp - 1):
                pass_dy(c_idx, slot).wait_recv()

        loads = [pltpu.make_async_copy(dy_all.at[peers[slot], rows], bufs[slot].at[rows], post_sem.at[slot]) for slot in range(tp - 1)]
        keeps = [pltpu.make_async_copy(bufs[slot].at[rows], gpre_all.at[peers[slot], rows], post_sem.at[slot]) for slot in range(tp - 1)]
        for load in loads:
            load.start()
        for slot in range(tp - 1):
            loads[slot].wait()
            finish_rows(peers[slot], bufs[slot], bufs[slot], rows)
            keeps[slot].start()
        for keep in keeps:
            keep.wait()
        return carry

    lax.fori_loop(0, chunks, finish_peers, 0)
    for slot in range(tp - 1):
        sum_copy(slot).wait()
    total_small = small[0, 0:6, :]
    for t_idx in range(1, tp):
        total_small = total_small + small[t_idx, 0:6, :]
    small_out[0:6, :] = total_small

    for slot in range(tp - 1):
        mix_copy(slot).wait_recv()
        gq_copy(slot).wait()
    for side in range(2):
        for kind in range(3):
            ag_forward(kind, side).wait_send()
        ag_copy(2, side).wait_send()
        ag_forward(2, side).wait_recv()
        for c_idx in range(chunks):
            bw_copy(c_idx, side).wait_send()
            bw_forward(c_idx, side).wait_send()
    for out_copy in bwd_out:
        out_copy.wait()

    @pl.when(not_last)
    def _():
        for slot in range(tp - 1):
            pass_x(slot).wait_send()

    @pl.when(not_first)
    def _():
        for c_idx in range(chunks):
            hop_copy(c_idx, False).wait_send()
            for slot in range(tp - 1):
                pass_dy(c_idx, slot).wait_send()


def run_chain(stages, tp, x_flat, dy_flat, wq, wo, w1, w2, params, head_dim):
    _, seq_len, d_model = x_flat.shape
    chunk = min(128, seq_len)
    chunks = seq_len // chunk
    group = wo.shape[0]
    heads = group // head_dim
    ff_local = w1.shape[1]
    rows = (tp, seq_len, d_model)
    outs = [jax.ShapeDtypeStruct(rows, BF16)] * 4
    outs += [jax.ShapeDtypeStruct((tp, seq_len, group), BF16), jax.ShapeDtypeStruct((tp, seq_len, 3 * group), BF16)]
    outs += [jax.ShapeDtypeStruct(rows, BF16)] * 4 + [jax.ShapeDtypeStruct((tp, seq_len, ff_local), BF16)] * 2
    outs += [jax.ShapeDtypeStruct((tp, seq_len, ff_local), F32), jax.ShapeDtypeStruct((8, d_model), F32)]
    act = pltpu.VMEM((seq_len, d_model), BF16)
    dma = pltpu.SemaphoreType.DMA
    scratch = [
        pltpu.VMEM((tp,) + wq.shape, BF16), pltpu.VMEM((tp,) + wq.shape[::-1], BF16), pltpu.VMEM((tp * group, d_model), BF16),
        pltpu.VMEM((tp,) + w1.shape, BF16), pltpu.VMEM((tp,) + w2.shape, BF16),
        pltpu.VMEM((tp, 8, d_model), F32),
        act, act,
        pltpu.VMEM((3, tp, seq_len, group), BF16), pltpu.VMEM((tp, seq_len, group), BF16),
        act, act, act, act,
        pltpu.VMEM((2, tp, seq_len, group), F32),
        pltpu.VMEM((chunks, tp, heads * chunk, seq_len), F32), pltpu.VMEM((tp, seq_len, ff_local), F32),
        pltpu.VMEM((chunk, d_model), F32), pltpu.VMEM((chunk, d_model), BF16), pltpu.VMEM((tp, 8, d_model), F32),
        dma((9,)), pltpu.SemaphoreType.REGULAR, pltpu.SemaphoreType.REGULAR, dma((4, 2, 2)), dma((4, 2, 2)), dma((4, 2)), dma((4, 2)), dma((tp - 1,)), dma((tp - 1,)),
        dma((2, chunks)), dma((2, chunks)), dma((3, 4)), dma((3, 4)), dma((tp - 1,)), dma((tp - 1,)),
        dma((chunks, 4)), dma((chunks, 4)), dma((tp - 1,)), dma((tp - 1,)),
        dma((8,)), dma((tp - 1,)), dma((tp - 1,)), dma((chunks, tp - 1)), dma((chunks, tp - 1)), dma((tp - 1,)), dma((tp - 1,)), dma((3,)), dma((tp - 1,)),
    ]
    return pl.pallas_call(
        functools.partial(chain_kernel, stages, tp, chunk, head_dim),
        out_shape=outs,
        in_specs=[ANY] * 6 + [VMEM],
        out_specs=[ANY] * 13 + [VMEM],
        scratch_shapes=scratch,
        compiler_params=pltpu.CompilerParams(collective_id=0, has_side_effects=True, vmem_limit_bytes=67043328),
        name="chain",
    )(x_flat, dy_flat, wq, wo, w1, w2, params)


def wgrad_kernel(act, dy, gpre, h_two, gqkv, h_one, mix, gmid, h_all, gin_all, small,
                 gw_two, gw_one, gw_qkv, gw_out, h_out, g_in, g_ln, gb_out, gb_two, gb_one, gb_qkv,
                 act_v, dy_v, gpre_v, h_two_v, gq_v, h_one_v, mix_v, gmid_v, h_v, gin_v, two_v, one_v, qkv_v, out_v,
                 in_sem, two_sem, one_sem, qkv_sem, res_sem, keep_sem):
    heads, head_dim = gb_qkv.shape[1:]
    group = heads * head_dim
    pairs = ((act, act_v), (dy, dy_v), (gpre, gpre_v), (h_two, h_two_v), (gqkv, gq_v), (h_one, h_one_v), (mix, mix_v), (gmid, gmid_v), (h_all, h_v), (gin_all, gin_v))
    loads = [pltpu.make_async_copy(src, dst, in_sem.at[idx]) for idx, (src, dst) in enumerate(pairs)]
    for load in loads:
        load.start()
    g_ln[...] = small[0:4, :]
    gb_out[...] = small[4:5, :]
    gb_two[...] = small[5:6, :]
    gb_one[...] = small[6:7, :]

    def product(lhs, rhs, buf, dst, sem):
        def copy_of(row):
            rows = pl.ds(pl.multiple_of(row * group, group), group)
            return pltpu.make_async_copy(buf.at[rows], dst.at[rows], sem.at[row])

        @pl.loop(0, buf.shape[0] // group)
        def _(row):
            cols = pl.ds(pl.multiple_of(row * group, group), group)
            buf[cols, :] = dot_tn(lhs(row, cols), rhs[...])
            copy_of(row).start()

        return lambda: [copy_of(row).wait() for row in range(buf.shape[0] // group)]

    loads[0].wait()
    loads[1].wait()
    ends = [product(lambda row, cols: act_v[:, cols], dy_v, two_v, gw_two, two_sem)]
    loads[2].wait()
    loads[3].wait()
    ends.append(product(lambda row, cols: h_two_v[:, cols], gpre_v, one_v, gw_one, one_sem))
    loads[4].wait()
    loads[5].wait()
    ends.append(product(lambda row, cols: gq_v[:, cols], h_one_v, qkv_v, gw_qkv, qkv_sem))
    for part in range(3):
        total = jnp.sum(gq_v[:, part * group:(part + 1) * group].astype(F32), axis=0, keepdims=True)
        for h_idx in range(heads):
            gb_qkv[part, h_idx:h_idx + 1, :] = total[:, h_idx * head_dim:(h_idx + 1) * head_dim]
    loads[8].wait()
    loads[9].wait()
    keeps = [pltpu.make_async_copy(h_v, h_out, keep_sem.at[0]), pltpu.make_async_copy(gin_v, g_in, keep_sem.at[1])]
    for keep in keeps:
        keep.start()
    loads[6].wait()
    loads[7].wait()
    ends.append(product(lambda row, cols: mix_v[:, cols], gmid_v, out_v, gw_out, res_sem))
    for end in ends:
        end()
    for keep in keeps:
        keep.wait()


def run_wgrad(act, dy, gpre, h_two, gqkv, h_one, mix, gmid, h_all, gin_all, small, head_dim):
    def flat(array):
        return array.reshape(array.shape[0] * array.shape[1], array.shape[2])

    group, d_model, ff_local = mix.shape[2], dy.shape[2], act.shape[2]
    seqs, seq_len = dy.shape[:2]
    total = seqs * seq_len
    dma = pltpu.SemaphoreType.DMA
    grads = [(ff_local, d_model), (d_model, ff_local), (3 * group, d_model), (group, d_model)]
    rows = jax.ShapeDtypeStruct((total, d_model), BF16)
    smalls = [(4, d_model), (1, d_model), (1, d_model), (1, ff_local), (3, group // head_dim, head_dim)]
    widths = (ff_local, d_model, ff_local, d_model)
    return pl.pallas_call(
        wgrad_kernel,
        in_specs=[ANY] * 10 + [VMEM],
        out_specs=[ANY] * 6 + [VMEM] * 5,
        out_shape=[jax.ShapeDtypeStruct(shape, F32) for shape in grads] + [rows, rows] + [jax.ShapeDtypeStruct(shape, F32) for shape in smalls],
        scratch_shapes=[pltpu.VMEM((total, width), BF16) for width in widths]
        + [pltpu.VMEM((total, 3 * group), BF16), pltpu.VMEM((total, d_model), BF16), pltpu.VMEM((total, group), BF16)]
        + [pltpu.VMEM((total, d_model), BF16)] * 3 + [pltpu.VMEM(shape, F32) for shape in grads]
        + [dma((10,))] + [dma((shape[0] // group,)) for shape in grads] + [dma((2,))],
        compiler_params=pltpu.CompilerParams(vmem_limit_bytes=67043328),
        name="wgrad",
    )(flat(act), flat(dy), flat(gpre), flat(h_two), flat(gqkv), flat(h_one), flat(mix), flat(gmid), flat(h_all), flat(gin_all), small)


def solution(mesh):
    stages = mesh.shape["pp"]
    tp = mesh.shape["tp"]

    def stage_program(x_in, dy_out, w_qkv, b_qkv, w_out, b_out, ln_par, w_fc1, b_fc1, w_fc2, b_fc2):
        micro_count, batch_rows, seq_len, d_model = x_in.shape
        head_dim = w_qkv.shape[4]
        group = w_qkv.shape[3] * head_dim
        heads = group // head_dim
        seqs = micro_count * batch_rows
        wq = jnp.transpose(w_qkv[0], (0, 2, 3, 1)).reshape(3 * group, d_model)
        wo = w_out[0].reshape(group, d_model)
        w1, w2 = w_fc1[0], w_fc2[0]
        b_row = jnp.pad(b_qkv.reshape(1, 3 * group), ((0, 0), (0, d_model - 3 * group)))
        gap = jnp.zeros((6, d_model), BF16)
        params = jnp.concatenate([b_fc1, b_row, gap, ln_par[0], b_out, b_fc2, gap[:2]], axis=0).astype(F32)
        x_flat = x_in.reshape(seqs, seq_len, d_model)
        dy_flat = dy_out.reshape(seqs, seq_len, d_model)
        h_all, _, gin_all, gmid_all, mix_all, gqkv_all, _, dy_all, h_one, h_two, act, gpre, _, small = run_chain(
            stages, tp, x_flat, dy_flat, wq, wo, w1, w2, params, head_dim)
        gw_two, gw_one, gw_qkv, gw_out, h_out, g_in, g_ln, gb_out, gb_two, gb_one, gb_qkv = run_wgrad(
            act, dy_all, gpre, h_two, gqkv_all, h_one, mix_all, gmid_all, h_all, gin_all, small, head_dim)
        gw_qkv = jnp.transpose(gw_qkv.reshape(3, heads, head_dim, d_model), (0, 3, 1, 2))
        shape = (1, micro_count, batch_rows, seq_len, d_model)
        return (h_out.reshape(shape), g_in.reshape(shape), gw_qkv[None], gb_qkv[None], gw_out.reshape(1, heads, head_dim, d_model), gb_out,
                g_ln[None], gw_one[None], gb_one, gw_two[None], gb_two)

    act_spec = P(None, "dp", None, None)
    arg_specs = (act_spec, act_spec,
                 P("pp", None, None, "tp", None), P("pp", None, "tp", None), P("pp", "tp", None, None),
                 P("pp", None), P("pp", None, None), P("pp", None, "tp"), P("pp", "tp"),
                 P("pp", "tp", None), P("pp", None))
    stage_spec = P("pp", None, "dp", None, None)
    grad_axes = ("dp", "pp")
    result_specs = (stage_spec, stage_spec,
                    P(grad_axes, None, None, "tp", None), P(grad_axes, None, "tp", None), P(grad_axes, "tp", None, None),
                    P(grad_axes, None), P(grad_axes, None, None), P(grad_axes, None, "tp"), P(grad_axes, "tp"),
                    P(grad_axes, "tp", None), P(grad_axes, None))
    return jax.shard_map(stage_program, mesh=mesh, in_specs=arg_specs, out_specs=result_specs, check_vma=False)
```

```python
import functools

import jax
import jax.numpy as jnp
from jax import lax
from jax.experimental import pallas as pl
from jax.experimental.pallas import tpu as pltpu
from jax.sharding import PartitionSpec as P

LN_EPS = 1e-5
F32 = jnp.float32
BF16 = jnp.bfloat16
MESH = pl.DeviceIdType.MESH
GELU_A = 0.7978845608028654
GELU_B = 0.044715
LOG2_E = 1.4426950408889634
ANY = pl.BlockSpec(memory_space=pl.ANY)
VMEM = pl.BlockSpec(memory_space=pltpu.VMEM)


def dot_nn(lhs, rhs):
    return jnp.dot(lhs, rhs, preferred_element_type=F32)


def dot_nt(lhs, rhs):
    return lax.dot_general(lhs, rhs, (((1,), (1,)), ((), ())), preferred_element_type=F32)


def dot_tn(lhs, rhs):
    return lax.dot_general(lhs, rhs, (((0,), (0,)), ((), ())), preferred_element_type=F32)


def norm_stats(x_wide):
    row_mean = jnp.mean(x_wide, axis=-1, keepdims=True)
    centered = x_wide - row_mean
    row_var = jnp.mean(centered * centered, axis=-1, keepdims=True)
    inv_std = lax.rsqrt(row_var + LN_EPS)
    return centered * inv_std, inv_std


def norm_backward(x_wide, gain, grad_h):
    normed, inv_std = norm_stats(x_wide)
    g_normed = grad_h * gain
    mean_g = jnp.mean(g_normed, axis=-1, keepdims=True)
    mean_gn = jnp.mean(g_normed * normed, axis=-1, keepdims=True)
    grad_x = (g_normed - mean_g - normed * mean_gn) * inv_std
    return grad_x, jnp.sum(grad_h * normed, axis=0, keepdims=True), jnp.sum(grad_h, axis=0, keepdims=True)


def gelu_parts(pre):
    square = pre * pre
    tanh = jnp.tanh(pre * (GELU_A + (GELU_A * GELU_B) * square))
    cdf = 0.5 + 0.5 * tanh
    return cdf, cdf + pre * (0.5 * GELU_A + (1.5 * GELU_A * GELU_B) * square) * (1.0 - tanh * tanh)


def chain_kernel(stages, tp, chunk, head_dim,
                 x_flat, dy_flat, wq_own, wo_own, w1_own, w2_own, ln_ref, b_qkv_ref, b_out_ref, b_one_ref, b_two_ref,
                 h_all, mid_all, gin_all, gmid_all, mix_all, gqkv_all, x_all, dy_all, h_one_all, h_two_all, act_all, gpre_all, slope_all, land_one, land_two, land_gq, land_gm, small_out,
                 wq, wq_t, wo, w1, w2, bias, x_buf, dy_buf, qkv, mix, mid, y_buf, gmid, gin, dkv, prob, dgelu, acc, hbuf, small, rep, bias_own,
                 own_sem, go_sem, done_sem, ring_send, ring_recv, fwd_send, fwd_recv, bias_send, bias_recv,
                 hop_send, hop_recv, ag_send, ag_recv, mix_send, mix_recv, bw_send, bw_recv, gq_send, gq_recv,
                 out_sem, px_send, px_recv, py_send, py_recv, sum_send, sum_recv, prep_sem, post_sem,
                 lw_send, lw_recv, lf_send, lf_recv, lg_send, lg_recv):
    stage = lax.axis_index("pp")
    me = lax.axis_index("tp")
    seq_len, d_model = x_buf.shape
    chunks = seq_len // chunk
    group = wo_own.shape[0]
    heads = group // head_dim
    last = stages - 1
    right, left, across = lax.rem(me + 1, tp), lax.rem(me + tp - 1, tp), lax.rem(me + 2, tp)
    not_first, not_last = stage > 0, stage < last
    peers = [lax.rem(me + off, tp) for off in range(1, tp)]
    even = lax.rem(stage, 2) == 0
    score_scale = head_dim ** -0.5

    middle = stages // 2
    eased, easing = stage == 1, stage == last
    helped, helping = stage < 2, (stage >= middle) & (stage < middle + 2)
    mate = lax.rem(stage + middle, stages)
    far = jnp.where(eased, last, 1)

    def remote(src, dst, send, recv, axis, target):
        return pltpu.make_async_remote_copy(src_ref=src, dst_ref=dst, send_sem=send, recv_sem=recv,
                                            device_id={axis: target}, device_id_type=MESH)

    bias_own[...] = jnp.zeros_like(bias_own)
    bias_own[0:1, :] = b_one_ref[...].astype(F32)
    for part in range(3):
        for h_idx in range(heads):
            col = part * group + h_idx * head_dim
            bias_own[1:2, col:col + head_dim] = b_qkv_ref[part, h_idx:h_idx + 1, :].astype(F32)
    rep[0:4, :] = ln_ref[...].astype(F32)
    rep[4:5, :] = b_out_ref[...].astype(F32)
    rep[5:6, :] = b_two_ref[...].astype(F32)
    small[...] = jnp.zeros_like(small)
    small_out[...] = jnp.zeros_like(small_out)
    barrier = pltpu.get_barrier_semaphore()
    for peer in peers:
        pl.semaphore_signal(barrier, inc=1, device_id={"tp": peer}, device_id_type=MESH)

    @pl.when(not_first)
    def _():
        pl.semaphore_signal(barrier, inc=1, device_id={"pp": stage - 1}, device_id_type=MESH)

    @pl.when(not_last)
    def _():
        pl.semaphore_signal(barrier, inc=1, device_id={"pp": stage + 1}, device_id_type=MESH)

    @pl.when(helped | helping)
    def _():
        for there in (me, across):
            pl.semaphore_signal(barrier, inc=1, device_id={"pp": mate, "tp": there}, device_id_type=MESH)

    @pl.when(eased | easing)
    def _():
        for there in (me, across):
            pl.semaphore_signal(barrier, inc=1, device_id={"pp": far, "tp": there}, device_id_type=MESH)

    near = tp - 1 + jnp.minimum(stage, 1) + jnp.minimum(last - stage, 1)
    pl.semaphore_wait(barrier, near + jnp.where(helped | helping, 2, 0) + jnp.where(eased | easing, 2, 0))

    def shard(w_idx, origin):
        if w_idx == 1:
            return wo.at[pl.ds(pl.multiple_of(origin * group, group), group)]
        return (wq, None, w1, w2)[w_idx].at[origin]

    owns = (wq_own, wo_own, w1_own, w2_own)

    def half(ref, idx):
        size = ref.shape[0] // 2
        return ref.at[pl.ds(idx * size, size)]

    def ring_copy(w_idx, h_idx, side):
        return remote(half(owns[w_idx], h_idx), half(shard(w_idx, me), h_idx),
                      ring_send.at[w_idx, h_idx, side], ring_recv.at[w_idx, h_idx, side], "tp", left if side else right)

    def forward_copy(w_idx, side):
        block = half(shard(w_idx, right if side else left), side)
        return remote(block, block, fwd_send.at[w_idx, side], fwd_recv.at[w_idx, side], "tp", left if side else right)

    def bias_copy(slot):
        return remote(bias_own, bias.at[me], bias_send.at[slot], bias_recv.at[slot], "tp", peers[slot])

    def detour(src, dst, send, recv, target, target_tp):
        return pltpu.make_async_remote_copy(src_ref=src, dst_ref=dst, send_sem=send, recv_sem=recv,
                                            device_id={"pp": target, "tp": target_tp}, device_id_type=MESH)

    routes = ((2, 0, land_one, mate), (2, 1, land_one, far), (3, None, land_two, far))

    def piece(ref, h_idx):
        return ref if h_idx is None else half(ref, h_idx)

    def lw_copy(idx):
        w_idx, h_idx, land, target = routes[idx]
        return detour(piece(owns[w_idx], h_idx), piece(land, h_idx), lw_send.at[idx], lw_recv.at[idx], target, across)

    def lf_copy(idx):
        w_idx, h_idx, land, target = routes[idx]
        return detour(piece(land, h_idx), piece(shard(w_idx, across), h_idx), lf_send.at[idx], lf_recv.at[idx], target, me)

    own_copies = [pltpu.make_async_copy(owns[w_idx], shard(w_idx, me), own_sem.at[w_idx]) for w_idx in range(4)]
    own_copies.append(pltpu.make_async_copy(bias_own, bias.at[me], own_sem.at[4]))
    for own_copy in own_copies:
        own_copy.start()
    for slot in range(tp - 1):
        bias_copy(slot).start()

    def own_input(src, buf, dst):
        bounce = (y_buf, mid, gmid)
        copies = [pltpu.make_async_copy(src.at[me], buf, own_sem.at[5])]
        copies += [pltpu.make_async_copy(src.at[peers[slot]], bounce[slot], own_sem.at[6 + slot]) for slot in range(tp - 1)]
        for copy in copies:
            copy.start()
        for copy in copies:
            copy.wait()
        copies = [pltpu.make_async_copy(bounce[slot], dst.at[peers[slot]], own_sem.at[6 + slot]) for slot in range(tp - 1)]
        for copy in copies:
            copy.start()
        for copy in copies:
            copy.wait()

    @pl.when(eased)
    def _():
        for idx in range(3):
            lw_copy(idx).start()

    @pl.when(stage == middle + 1)
    def _():
        lw_copy(0).wait_recv()
        lf_copy(0).start()

    @pl.when(easing)
    def _():
        for idx in (1, 2):
            lw_copy(idx).wait_recv()
            lf_copy(idx).start()

    @pl.when(jnp.logical_not(even))
    def _():
        pl.semaphore_wait(go_sem, 1)

    for w_idx in range(4):
        for h_idx in range(2):
            ring_copy(w_idx, h_idx, 0).start()
            ring_copy(w_idx, 1 - h_idx, 1).start()

    @pl.when(stage == 0)
    def _():
        own_input(x_flat, x_buf, x_all)

    @pl.when(stage == last)
    def _():
        own_input(dy_flat, dy_buf, dy_all)

    qkv[...] = jnp.zeros_like(qkv)
    dkv[...] = jnp.zeros_like(dkv)

    for w_idx in range(4):
        for side in range(2):
            ring_copy(w_idx, side, side).wait_recv()
            if w_idx < 2:
                forward_copy(w_idx, side).start()
            else:
                @pl.when(jnp.logical_not(eased))
                def _():
                    forward_copy(w_idx, side).start()
    for own_copy in own_copies:
        own_copy.wait()
    for slot in range(tp - 1):
        bias_copy(slot).wait()
    for w_idx in range(4):
        ring_copy(w_idx, 1, 0).wait_recv()
        ring_copy(w_idx, 0, 1).wait_recv()
        if w_idx < 2:
            forward_copy(w_idx, 0).wait()
            forward_copy(w_idx, 1).wait()
        for h_idx in range(2):
            ring_copy(w_idx, h_idx, 0).wait_send()
            ring_copy(w_idx, h_idx, 1).wait_send()
        if w_idx == 0:
            @pl.loop(0, tp)
            def _(t_idx):
                for part in range(3):
                    wq_t[t_idx, :, part * group:(part + 1) * group] = wq[t_idx, part * group:(part + 1) * group, :].T

    @pl.when(jnp.logical_not(eased))
    def _():
        for w_idx in (2, 3):
            forward_copy(w_idx, 0).wait()
            forward_copy(w_idx, 1).wait()

    @pl.when(eased)
    def _():
        for idx in range(3):
            lf_copy(idx).wait_recv()
            lw_copy(idx).wait_send()

    @pl.when(stage == middle + 1)
    def _():
        lf_copy(0).wait_send()

    @pl.when(easing)
    def _():
        for idx in (1, 2):
            lf_copy(idx).wait_send()

    @pl.when(even)
    def _():
        pl.semaphore_signal(go_sem, inc=1, device_id={"pp": stage + 1}, device_id_type=MESH)

    @pl.when(jnp.logical_not(even))
    def _():
        pl.semaphore_signal(done_sem, inc=1, device_id={"pp": stage - 1}, device_id_type=MESH)

    lane_head = lax.broadcasted_iota(jnp.int32, (chunk, group), 1) // head_dim

    def stack_heads(block):
        zero = jnp.zeros_like(block)
        return jnp.concatenate([jnp.where(lane_head == h_idx, block, zero) for h_idx in range(heads)], axis=0)

    def unstack_heads(stacked):
        total = stacked[:chunk]
        for h_idx in range(1, heads):
            total = jnp.where(lane_head == h_idx, stacked[h_idx * chunk:(h_idx + 1) * chunk], total)
        return total

    def hop_copy(c_idx, forward):
        rows = pl.ds(c_idx * chunk, chunk)
        src, dst, way, target = (y_buf, x_buf, 0, stage + 1) if forward else (gin, dy_buf, 1, stage - 1)
        return remote(src.at[rows], dst.at[rows], hop_send.at[way, c_idx], hop_recv.at[way, c_idx], "pp", target)

    def fwd_chunk(c_idx, carry):
        rows = pl.ds(pl.multiple_of(c_idx * chunk, chunk), chunk)

        @pl.when(not_first)
        def _():
            hop_copy(c_idx, True).wait_recv()

        normed, _ = norm_stats(x_buf[rows, :].astype(F32))
        hbuf[...] = (normed * rep[0:1, :] + rep[1:2, :]).astype(BF16)

        groups = range(tp)
        for t_idx in groups:
            pre = dot_nn(hbuf[...], wq_t[t_idx]) + bias[t_idx, 1:2, :3 * group]
            for part in range(3):
                qkv[part, t_idx, rows, :] = pre[:, part * group:(part + 1) * group].astype(BF16)

        row_pos = c_idx * chunk + lax.rem(lax.broadcasted_iota(jnp.int32, (heads * chunk, seq_len), 0), chunk)
        causal = row_pos >= lax.broadcasted_iota(jnp.int32, (heads * chunk, seq_len), 1)
        all_scores = [dot_nt(stack_heads(qkv[0, t_idx, rows, :]), qkv[1, t_idx]) for t_idx in groups]
        all_probs = []
        for t_idx in groups:
            scores = jnp.where(causal, all_scores[t_idx], -1e30)
            expd = jnp.exp2((scores - jnp.max(scores, axis=-1, keepdims=True)) * (score_scale * LOG2_E))
            probs = expd * (1.0 / jnp.sum(expd, axis=-1, keepdims=True))
            prob[c_idx, t_idx] = probs
            all_probs.append(probs.astype(BF16))
        for t_idx in groups:
            mix[t_idx, rows, :] = unstack_heads(dot_nn(all_probs[t_idx], qkv[2, t_idx])).astype(BF16)

        full_mix = jnp.concatenate([mix[t_idx, rows, :] for t_idx in groups], axis=1)
        x_mid = (x_buf[rows, :].astype(F32) + dot_nn(full_mix, wo[...]) + rep[4:5, :]).astype(BF16)
        mid[rows, :] = x_mid
        normed_two, _ = norm_stats(x_mid.astype(F32))
        hbuf[...] = (normed_two * rep[2:3, :] + rep[3:4, :]).astype(BF16)
        total = jnp.zeros((chunk, d_model), F32)
        for t_idx in groups:
            pre = dot_nn(hbuf[...], w1[t_idx]) + bias[t_idx, 0:1, :]
            cdf, slope = gelu_parts(pre)
            dgelu[t_idx, rows, :] = slope
            total = total + dot_nn((pre * cdf).astype(BF16), w2[t_idx])

        y_buf[rows, :] = (mid[rows, :].astype(F32) + total + rep[5:6, :]).astype(BF16)

        @pl.when(not_last)
        def _():
            hop_copy(c_idx, True).start()

        return carry

    lax.fori_loop(0, chunks, fwd_chunk, 0)

    def ag_copy(kind, side):
        src, dst = ((y_buf, h_all), (mid, mid_all), (gmid, gmid_all))[kind]
        return remote(src, dst.at[me], ag_send.at[kind, side], ag_recv.at[kind, side], "tp", left if side else right)

    def ag_forward(kind, side):
        rows = pl.ds(side * (seq_len // 2), seq_len // 2)
        block = (h_all, mid_all, gmid_all)[kind].at[right if side else left, rows]
        return remote(block, block, ag_send.at[kind, 2 + side], ag_recv.at[kind, 2 + side], "tp", left if side else right)

    def mix_copy(slot):
        return remote(mix.at[peers[slot]], mix_all.at[me], mix_send.at[slot], mix_recv.at[slot], "tp", peers[slot])

    def start_fwd_gather():
        for kind in range(2):
            for side in range(2):
                ag_copy(kind, side).start()
        for slot in range(tp - 1):
            mix_copy(slot).start()

    @pl.when(jnp.logical_not(even))
    def _():
        start_fwd_gather()

    fwd_out = [pltpu.make_async_copy(y_buf, h_all.at[me], out_sem.at[0]),
               pltpu.make_async_copy(mid, mid_all.at[me], out_sem.at[1]),
               pltpu.make_async_copy(mix.at[me], mix_all.at[me], out_sem.at[2]),
               pltpu.make_async_copy(x_buf, x_all.at[me], out_sem.at[3])]
    for out_copy in fwd_out:
        out_copy.start()

    def pass_x(slot):
        origin = peers[slot]
        return remote(h_all.at[origin], x_all.at[origin], px_send.at[slot], px_recv.at[slot], "pp", stage + 1)

    def forward_fwd_gather():
        for kind in range(2):
            for side in range(2):
                ag_copy(kind, side).wait_recv()
                ag_forward(kind, side).start()

    def finish_fwd_gather():
        for kind in range(2):
            for side in range(2):
                ag_forward(kind, side).wait_recv()

        @pl.when(not_last)
        def _():
            for slot in range(tp - 1):
                pass_x(slot).start()

    size = group

    def flip(ref_get, ref_set, count):
        for row in range(count):
            ref_set(row, row, ref_get(row, row).T)
            for col in range(row):
                upper, lower = ref_get(col, row).T, ref_get(row, col).T
                ref_set(row, col, upper)
                ref_set(col, row, lower)

    def tile(row, col):
        return slice(row * size, (row + 1) * size), slice(col * size, (col + 1) * size)

    @pl.loop(0, tp)
    def _(t_idx):
        for ref in (w2, w1):
            def ref_set(row, col, value, ref=ref):
                ref[(t_idx,) + tile(row, col)] = value

            flip(lambda row, col, ref=ref: ref[(t_idx,) + tile(row, col)], ref_set, d_model // size)

    def wo_set(row, col, value):
        wo[tile(row, col)] = value

    flip(lambda row, col: wo[tile(row, col)], wo_set, d_model // size)

    @pl.when(even)
    def _():
        pl.semaphore_wait(done_sem, 1)
        start_fwd_gather()

    @pl.when(stage < last - 1)
    def _():
        forward_fwd_gather()

    @pl.when(stage < stages // 2)
    def _():
        finish_fwd_gather()

    def bw_copy(c_idx, side):
        rows = pl.ds(c_idx * chunk, chunk)
        return remote(gin.at[rows], gin_all.at[me, rows], bw_send.at[c_idx, side], bw_recv.at[c_idx, side], "tp", left if side else right)

    def bw_forward(c_idx, side):
        rows = pl.ds(c_idx * chunk + side * (chunk // 2), chunk // 2)
        block = gin_all.at[right if side else left, rows]
        return remote(block, block, bw_send.at[c_idx, 2 + side], bw_recv.at[c_idx, 2 + side], "tp", left if side else right)

    def gqkv_of(t_idx):
        return wq_t.at[t_idx, pl.ds(0, seq_len)]

    def gq_copy(slot):
        return remote(gqkv_of(peers[slot]), gqkv_all.at[me], gq_send.at[slot], gq_recv.at[slot], "tp", peers[slot])

    def gl_copy(idx):
        return detour(gmid if idx else gqkv_of(across), land_gm if idx else land_gq, lg_send.at[idx], lg_recv.at[idx], mate, across)

    def gf_copy(idx):
        return detour(land_gm if idx else land_gq, (gmid_all if idx else gqkv_all).at[across], lg_send.at[2 + idx], lg_recv.at[2 + idx], mate, me)

    def pass_dy(c_idx, slot):
        rows = pl.ds(c_idx * chunk, chunk)
        origin = peers[slot]
        return remote(gin_all.at[origin, rows], dy_all.at[origin, rows], py_send.at[c_idx, slot], py_recv.at[c_idx, slot], "pp", stage - 1)

    def forward_chunk(c_idx):
        for side in range(2):
            bw_copy(c_idx, side).wait_recv()
            bw_forward(c_idx, side).start()

    def pass_chunk(c_idx):
        for side in range(2):
            bw_forward(c_idx, side).wait_recv()

        @pl.when(not_first)
        def _():
            for slot in range(tp - 1):
                pass_dy(c_idx, slot).start()

    w1_own_t, w2_own_t = w1.at[me], w2.at[me]
    early = stage < stages // 2 - 1

    def prep(two_buf, one_buf, act_buf, keep_slopes):
        @pl.when(not_first)
        def _():
            for slot in range(tp - 1):
                pass_x(slot).wait_recv()

        def prep_seq(t_idx, carry):
            loads = [pltpu.make_async_copy(mid_all.at[t_idx], two_buf, prep_sem.at[0]), pltpu.make_async_copy(x_all.at[t_idx], one_buf, prep_sem.at[1])]
            for load in loads:
                load.start()
            for load in loads:
                load.wait()

            def prep_rows(c_idx, inner):
                rows = pl.ds(pl.multiple_of(c_idx * chunk, chunk), chunk)
                normed, _ = norm_stats(two_buf[rows, :].astype(F32))
                two_buf[rows, :] = (normed * rep[2:3, :] + rep[3:4, :]).astype(BF16)
                normed_one, _ = norm_stats(one_buf[rows, :].astype(F32))
                one_buf[rows, :] = (normed_one * rep[0:1, :] + rep[1:2, :]).astype(BF16)
                pre = dot_nt(two_buf[rows, :], w1_own_t[...]) + bias[me, 0:1, :]
                cdf, slope = gelu_parts(pre)
                act_buf[rows, :] = (pre * cdf).astype(BF16)
                if keep_slopes:
                    keep = pltpu.make_async_copy(acc, slope_all.at[t_idx, rows], prep_sem.at[2])

                    @pl.when(c_idx > 0)
                    def _():
                        keep.wait()

                    acc[...] = slope
                    keep.start()
                else:
                    dgelu[t_idx, rows, :] = slope
                return inner

            lax.fori_loop(0, chunks, prep_rows, 0)
            if keep_slopes:
                pltpu.make_async_copy(acc, slope_all.at[t_idx, pl.ds(0, chunk)], prep_sem.at[2]).wait()
            keeps = [pltpu.make_async_copy(two_buf, h_two_all.at[t_idx], prep_sem.at[0]), pltpu.make_async_copy(one_buf, h_one_all.at[t_idx], prep_sem.at[1]),
                     pltpu.make_async_copy(act_buf, act_all.at[t_idx], prep_sem.at[2])]
            for keep in keeps:
                keep.start()
            for keep in keeps:
                keep.wait()
            return carry

        lax.fori_loop(0, tp, prep_seq, 0)

    def end_fwd_sends():
        for kind in range(2):
            for side in range(2):
                ag_copy(kind, side).wait_send()
        for slot in range(tp - 1):
            mix_copy(slot).wait_send()
        for out_copy in fwd_out:
            out_copy.wait()

        @pl.when(not_last)
        def _():
            for c_idx in range(chunks):
                hop_copy(c_idx, True).wait_send()

    @pl.when(early)
    def _():
        end_fwd_sends()
        prep(gmid, gin, y_buf, True)

    def bwd_chunk(step, carry):
        c_idx = chunks - 1 - step
        rows = pl.ds(pl.multiple_of(c_idx * chunk, chunk), chunk)

        @pl.when(not_last)
        def _():
            hop_copy(c_idx, False).wait_recv()

        groups = range(tp)
        g_h_sum = jnp.zeros((chunk, d_model), F32)
        for t_idx in groups:
            g_gelu = dot_nn(dy_buf[rows, :], w2[t_idx]).astype(BF16).astype(F32)
            g_h_sum = g_h_sum + dot_nn((g_gelu * dgelu[t_idx, rows, :]).astype(BF16), w1[t_idx])

        g_h_two = g_h_sum.astype(BF16).astype(F32)
        dy_wide = dy_buf[rows, :].astype(F32)
        g_ln, g_gain, g_shift = norm_backward(mid[rows, :].astype(F32), rep[2:3, :], g_h_two)
        g_mid = (dy_wide + g_ln.astype(BF16).astype(F32)).astype(BF16)
        gmid[rows, :] = g_mid
        small[me, 2:3, :] += g_gain
        small[me, 3:4, :] += g_shift
        small[me, 4:5, :] += jnp.sum(g_mid.astype(F32), axis=0, keepdims=True)
        small[me, 5:6, :] += jnp.sum(dy_wide, axis=0, keepdims=True)
        g_mix_all = dot_nn(gmid[rows, :], wo[...]).astype(BF16)
        g_stacks = [stack_heads(g_mix_all[:, t_idx * group:(t_idx + 1) * group]) for t_idx in groups]
        g_probs = [dot_nt(g_stacks[t_idx], qkv[2, t_idx]).astype(BF16).astype(F32) for t_idx in groups]
        g_values = [dot_tn(prob[c_idx, t_idx].astype(BF16), g_stacks[t_idx]) for t_idx in groups]
        g_scores = []
        for t_idx in groups:
            probs = prob[c_idx, t_idx]
            inner = jnp.sum(g_probs[t_idx] * probs, axis=-1, keepdims=True)
            g_scores.append((probs * (g_probs[t_idx] - inner)).astype(BF16))
            dkv[1, t_idx] += g_values[t_idx]
        for t_idx in groups:
            wq_t[t_idx, rows, 0:group] = (unstack_heads(dot_nn(g_scores[t_idx], qkv[1, t_idx])) * score_scale).astype(BF16)
            dkv[0, t_idx] += dot_tn(g_scores[t_idx], stack_heads(qkv[0, t_idx, rows, :])) * score_scale
        g_h_sum = jnp.zeros((chunk, d_model), F32)
        for t_idx in groups:
            wq_t[t_idx, rows, group:2 * group] = dkv[0, t_idx, rows, :].astype(BF16)
            wq_t[t_idx, rows, 2 * group:3 * group] = dkv[1, t_idx, rows, :].astype(BF16)
            g_h_sum = g_h_sum + dot_nn(wq_t[t_idx, rows, :], wq[t_idx])

        g_h_one = g_h_sum.astype(BF16).astype(F32)
        g_ln_one, g_gain_one, g_shift_one = norm_backward(x_buf[rows, :].astype(F32), rep[0:1, :], g_h_one)
        gin[rows, :] = (gmid[rows, :].astype(F32) + g_ln_one.astype(BF16).astype(F32)).astype(BF16)
        small[me, 0:1, :] += g_gain_one
        small[me, 1:2, :] += g_shift_one

        @pl.when(not_first)
        def _():
            hop_copy(c_idx, False).start()

        for side in range(2):
            bw_copy(c_idx, side).start()

        @pl.when((step >= 2) & (stage < last - 1))
        def _():
            forward_chunk(c_idx + 2)

        return carry

    lax.fori_loop(0, chunks, bwd_chunk, 0)

    def sum_copy(slot):
        return remote(small.at[me], small.at[me], sum_send.at[slot], sum_recv.at[slot], "tp", peers[slot])

    for slot in range(tp - 1):
        sum_copy(slot).start()
    bwd_out = [pltpu.make_async_copy(gin, gin_all.at[me], out_sem.at[4]),
               pltpu.make_async_copy(gmid, gmid_all.at[me], out_sem.at[5]),
               pltpu.make_async_copy(gqkv_of(me), gqkv_all.at[me], out_sem.at[6]),
               pltpu.make_async_copy(dy_buf, dy_all.at[me], out_sem.at[7])]
    for out_copy in bwd_out:
        out_copy.start()

    @pl.when(helped)
    def _():
        gl_copy(0).start()

    @pl.when(stage == 0)
    def _():
        gl_copy(1).start()

    @pl.when((stage >= stages // 2) & (stage < last - 1))
    def _():
        finish_fwd_gather()

    @pl.when(stage >= last - 1)
    def _():
        forward_fwd_gather()
        forward_chunk(chunks - 1)

    for c_idx in range(chunks - 2, -1, -1):
        forward_chunk(c_idx)

    @pl.when(stage >= last - 1)
    def _():
        finish_fwd_gather()

    for side in range(2):
        ag_copy(2, side).start()
    for slot in (0, 2, 1):
        if slot == 1:
            @pl.when(jnp.logical_not(helped))
            def _():
                gq_copy(slot).start()
        else:
            gq_copy(slot).start()
    def pass_all():
        for c_idx in range(chunks - 1, -1, -1):
            pass_chunk(c_idx)

    @pl.when(not_last)
    def _():
        pass_all()

    @pl.when(early)
    def _():
        slopes = pltpu.make_async_copy(slope_all, dgelu, prep_sem.at[0])
        slopes.start()
        slopes.wait()

    @pl.when(jnp.logical_not(early))
    def _():
        end_fwd_sends()
        prep(mid, x_buf, y_buf, False)

    @pl.when(stage == last)
    def _():
        pass_all()

    def finish_rows(t_idx, src, dst, rows):
        grad = dot_nn(src[rows, :], w2_own_t[...]).astype(BF16).astype(F32) * dgelu[t_idx, rows, :]
        small_out[6:7, :] += jnp.sum(grad, axis=0, keepdims=True)
        dst[rows, :] = grad.astype(BF16)

    def finish_own(c_idx, carry):
        finish_rows(me, dy_buf, y_buf, pl.ds(pl.multiple_of(c_idx * chunk, chunk), chunk))
        return carry

    lax.fori_loop(0, chunks, finish_own, 0)
    own_keep = pltpu.make_async_copy(y_buf, gpre_all.at[me], prep_sem.at[0])
    own_keep.start()
    @pl.when(not_first)
    def _():
        for side in range(2):
            ag_copy(2, side).wait_recv()
            ag_forward(2, side).start()

    own_keep.wait()

    def finish_peers(step, carry):
        c_idx = chunks - 1 - step
        rows = pl.ds(pl.multiple_of(c_idx * chunk, chunk), chunk)
        bufs = (x_buf, mid, y_buf)

        @pl.when(not_last)
        def _():
            for slot in range(tp - 1):
                pass_dy(c_idx, slot).wait_recv()

        loads = [pltpu.make_async_copy(dy_all.at[peers[slot], rows], bufs[slot].at[rows], post_sem.at[slot]) for slot in range(tp - 1)]
        keeps = [pltpu.make_async_copy(bufs[slot].at[rows], gpre_all.at[peers[slot], rows], post_sem.at[slot]) for slot in range(tp - 1)]
        for load in loads:
            load.start()
        for slot in range(tp - 1):
            loads[slot].wait()
            finish_rows(peers[slot], bufs[slot], bufs[slot], rows)
            keeps[slot].start()
        for keep in keeps:
            keep.wait()
        return carry

    lax.fori_loop(0, chunks, finish_peers, 0)

    @pl.when(helping)
    def _():
        gl_copy(0).wait_recv()
        gf_copy(0).start()

    @pl.when(stage == middle)
    def _():
        gl_copy(1).wait_recv()
        gf_copy(1).start()

    for slot in range(tp - 1):
        sum_copy(slot).wait()
    total_small = small[0, 0:6, :]
    for t_idx in range(1, tp):
        total_small = total_small + small[t_idx, 0:6, :]
    small_out[0:6, :] = total_small

    for slot in range(tp - 1):
        mix_copy(slot).wait_recv()
        if slot != 1:
            gq_copy(slot).wait()

    @pl.when(jnp.logical_not(helped))
    def _():
        gq_copy(1).wait()

    @pl.when(not_first)
    def _():
        for side in range(2):
            ag_forward(2, side).wait()

    @pl.when(helped)
    def _():
        gl_copy(0).wait_send()
        gf_copy(0).wait_recv()

    @pl.when(stage == 0)
    def _():
        for side in range(2):
            ag_copy(2, side).wait_recv()
        gl_copy(1).wait_send()
        gf_copy(1).wait_recv()

    @pl.when(helping)
    def _():
        gf_copy(0).wait_send()

    @pl.when(stage == middle)
    def _():
        gf_copy(1).wait_send()

    for side in range(2):
        for kind in range(2):
            ag_forward(kind, side).wait_send()
        ag_copy(2, side).wait_send()
        for c_idx in range(chunks):
            bw_copy(c_idx, side).wait_send()
            bw_forward(c_idx, side).wait_send()
    for out_copy in bwd_out:
        out_copy.wait()

    @pl.when(not_last)
    def _():
        for slot in range(tp - 1):
            pass_x(slot).wait_send()

    @pl.when(not_first)
    def _():
        for c_idx in range(chunks):
            hop_copy(c_idx, False).wait_send()
            for slot in range(tp - 1):
                pass_dy(c_idx, slot).wait_send()


def run_chain(stages, tp, x_flat, dy_flat, wq, wo, w1, w2, ln_par, b_qkv, b_out, b_one, b_two, head_dim):
    _, seq_len, d_model = x_flat.shape
    chunk = min(128, seq_len)
    chunks = seq_len // chunk
    group = wo.shape[0]
    heads = group // head_dim
    ff_local = w1.shape[1]
    rows = (tp, seq_len, d_model)
    outs = [jax.ShapeDtypeStruct(rows, BF16)] * 4
    outs += [jax.ShapeDtypeStruct((tp, seq_len, group), BF16), jax.ShapeDtypeStruct((tp, seq_len, 3 * group), BF16)]
    outs += [jax.ShapeDtypeStruct(rows, BF16)] * 4 + [jax.ShapeDtypeStruct((tp, seq_len, ff_local), BF16)] * 2
    outs += [jax.ShapeDtypeStruct((tp, seq_len, ff_local), F32), jax.ShapeDtypeStruct(w1.shape, BF16), jax.ShapeDtypeStruct(w2.shape, BF16)]
    outs += [jax.ShapeDtypeStruct((seq_len, 3 * group), BF16), jax.ShapeDtypeStruct((seq_len, d_model), BF16), jax.ShapeDtypeStruct((8, d_model), F32)]
    act = pltpu.VMEM((seq_len, d_model), BF16)
    dma = pltpu.SemaphoreType.DMA
    scratch = [
        pltpu.VMEM((tp,) + wq.shape, BF16), pltpu.VMEM((tp,) + wq.shape[::-1], BF16), pltpu.VMEM((tp * group, d_model), BF16),
        pltpu.VMEM((tp,) + w1.shape, BF16), pltpu.VMEM((tp,) + w2.shape, BF16),
        pltpu.VMEM((tp, 8, d_model), F32),
        act, act,
        pltpu.VMEM((3, tp, seq_len, group), BF16), pltpu.VMEM((tp, seq_len, group), BF16),
        act, act, act, act,
        pltpu.VMEM((2, tp, seq_len, group), F32),
        pltpu.VMEM((chunks, tp, heads * chunk, seq_len), F32), pltpu.VMEM((tp, seq_len, ff_local), F32),
        pltpu.VMEM((chunk, d_model), F32), pltpu.VMEM((chunk, d_model), BF16), pltpu.VMEM((tp, 8, d_model), F32),
        pltpu.VMEM((8, d_model), F32), pltpu.VMEM((8, d_model), F32),
        dma((9,)), pltpu.SemaphoreType.REGULAR, pltpu.SemaphoreType.REGULAR, dma((4, 2, 2)), dma((4, 2, 2)), dma((4, 2)), dma((4, 2)), dma((tp - 1,)), dma((tp - 1,)),
        dma((2, chunks)), dma((2, chunks)), dma((3, 4)), dma((3, 4)), dma((tp - 1,)), dma((tp - 1,)),
        dma((chunks, 4)), dma((chunks, 4)), dma((tp - 1,)), dma((tp - 1,)),
        dma((8,)), dma((tp - 1,)), dma((tp - 1,)), dma((chunks, tp - 1)), dma((chunks, tp - 1)), dma((tp - 1,)), dma((tp - 1,)), dma((3,)), dma((tp - 1,)),
        dma((3,)), dma((3,)), dma((3,)), dma((3,)), dma((4,)), dma((4,)),
    ]
    return pl.pallas_call(
        functools.partial(chain_kernel, stages, tp, chunk, head_dim),
        out_shape=outs,
        in_specs=[ANY] * 6 + [VMEM] * 5,
        out_specs=[ANY] * 17 + [VMEM],
        scratch_shapes=scratch,
        compiler_params=pltpu.CompilerParams(collective_id=0, has_side_effects=True, vmem_limit_bytes=67043328),
        name="chain",
    )(x_flat, dy_flat, wq, wo, w1, w2, ln_par, b_qkv, b_out, b_one, b_two)


def wgrad_kernel(act, dy, gpre, h_two, gqkv, h_one, mix, gmid, h_all, gin_all, small,
                 gw_two, gw_one, gw_qkv, gw_out, h_out, g_in, g_ln, gb_out, gb_two, gb_one, gb_qkv,
                 act_v, dy_v, gpre_v, h_two_v, gq_v, h_one_v, mix_v, gmid_v, h_v, gin_v, two_v, one_v, qkv_v, out_v,
                 in_sem, two_sem, one_sem, qkv_sem, res_sem, keep_sem):
    heads, head_dim = gb_qkv.shape[1:]
    group = heads * head_dim
    pairs = ((act, act_v), (dy, dy_v), (gpre, gpre_v), (h_two, h_two_v), (gqkv, gq_v), (h_one, h_one_v), (mix, mix_v), (gmid, gmid_v), (h_all, h_v), (gin_all, gin_v))
    loads = [pltpu.make_async_copy(src, dst, in_sem.at[idx]) for idx, (src, dst) in enumerate(pairs)]
    for load in loads:
        load.start()
    g_ln[...] = small[0:4, :]
    gb_out[...] = small[4:5, :]
    gb_two[...] = small[5:6, :]
    gb_one[...] = small[6:7, :]

    def product(lhs, rhs, buf, dst, sem, tiles):
        tile = buf.shape[0] // tiles

        def copy_of(row):
            rows = pl.ds(pl.multiple_of(row * tile, tile), tile)
            return pltpu.make_async_copy(buf.at[rows], dst.at[rows], sem.at[row])

        @pl.loop(0, tiles)
        def _(row):
            cols = pl.ds(pl.multiple_of(row * tile, tile), tile)
            buf[cols, :] = dot_tn(lhs[:, cols], rhs[...])
            copy_of(row).start()

        return lambda: [copy_of(row).wait() for row in range(tiles)]

    loads[0].wait()
    loads[1].wait()
    ends = [product(act_v, dy_v, two_v, gw_two, two_sem, 2)]
    loads[2].wait()
    loads[3].wait()
    ends.append(product(h_two_v, gpre_v, one_v, gw_one, one_sem, 2))
    loads[4].wait()
    loads[5].wait()
    ends.append(product(gq_v, h_one_v, qkv_v, gw_qkv, qkv_sem, 2))
    for part in range(3):
        total = jnp.sum(gq_v[:, part * group:(part + 1) * group].astype(F32), axis=0, keepdims=True)
        for h_idx in range(heads):
            gb_qkv[part, h_idx:h_idx + 1, :] = total[:, h_idx * head_dim:(h_idx + 1) * head_dim]
    loads[8].wait()
    loads[9].wait()
    keeps = [pltpu.make_async_copy(h_v, h_out, keep_sem.at[0]), pltpu.make_async_copy(gin_v, g_in, keep_sem.at[1])]
    for keep in keeps:
        keep.start()
    loads[6].wait()
    loads[7].wait()
    ends.append(product(mix_v, gmid_v, out_v, gw_out, res_sem, 1))
    for end in ends:
        end()
    for keep in keeps:
        keep.wait()


def run_wgrad(act, dy, gpre, h_two, gqkv, h_one, mix, gmid, h_all, gin_all, small, head_dim):
    def flat(array):
        return array.reshape(array.shape[0] * array.shape[1], array.shape[2])

    group, d_model, ff_local = mix.shape[2], dy.shape[2], act.shape[2]
    seqs, seq_len = dy.shape[:2]
    total = seqs * seq_len
    dma = pltpu.SemaphoreType.DMA
    grads = [(ff_local, d_model), (d_model, ff_local), (3 * group, d_model), (group, d_model)]
    rows = jax.ShapeDtypeStruct((total, d_model), BF16)
    smalls = [(4, d_model), (1, d_model), (1, d_model), (1, ff_local), (3, group // head_dim, head_dim)]
    widths = (ff_local, d_model, ff_local, d_model)
    return pl.pallas_call(
        wgrad_kernel,
        in_specs=[ANY] * 10 + [VMEM],
        out_specs=[ANY] * 6 + [VMEM] * 5,
        out_shape=[jax.ShapeDtypeStruct(shape, F32) for shape in grads] + [rows, rows] + [jax.ShapeDtypeStruct(shape, F32) for shape in smalls],
        scratch_shapes=[pltpu.VMEM((total, width), BF16) for width in widths]
        + [pltpu.VMEM((total, 3 * group), BF16), pltpu.VMEM((total, d_model), BF16), pltpu.VMEM((total, group), BF16)]
        + [pltpu.VMEM((total, d_model), BF16)] * 3 + [pltpu.VMEM(shape, F32) for shape in grads]
        + [dma((10,))] + [dma((shape[0] // group,)) for shape in grads] + [dma((2,))],
        compiler_params=pltpu.CompilerParams(vmem_limit_bytes=67043328),
        name="wgrad",
    )(flat(act), flat(dy), flat(gpre), flat(h_two), flat(gqkv), flat(h_one), flat(mix), flat(gmid), flat(h_all), flat(gin_all), small)


def solution(mesh):
    stages = mesh.shape["pp"]
    tp = mesh.shape["tp"]

    def stage_program(x_in, dy_out, w_qkv, b_qkv, w_out, b_out, ln_par, w_fc1, b_fc1, w_fc2, b_fc2):
        micro_count, batch_rows, seq_len, d_model = x_in.shape
        head_dim = w_qkv.shape[4]
        group = w_qkv.shape[3] * head_dim
        heads = group // head_dim
        seqs = micro_count * batch_rows
        wq = jnp.transpose(w_qkv[0], (0, 2, 3, 1)).reshape(3 * group, d_model)
        wo = w_out[0].reshape(group, d_model)
        w1, w2 = w_fc1[0], w_fc2[0]
        x_flat = x_in.reshape(seqs, seq_len, d_model)
        dy_flat = dy_out.reshape(seqs, seq_len, d_model)
        h_all, _, gin_all, gmid_all, mix_all, gqkv_all, _, dy_all, h_one, h_two, act, gpre, _, _, _, _, _, small = run_chain(
            stages, tp, x_flat, dy_flat, wq, wo, w1, w2, ln_par[0], b_qkv[0], b_out, b_fc1, b_fc2, head_dim)
        gw_two, gw_one, gw_qkv, gw_out, h_out, g_in, g_ln, gb_out, gb_two, gb_one, gb_qkv = run_wgrad(
            act, dy_all, gpre, h_two, gqkv_all, h_one, mix_all, gmid_all, h_all, gin_all, small, head_dim)
        gw_qkv = jnp.transpose(gw_qkv.reshape(3, heads, head_dim, d_model), (0, 3, 1, 2))
        shape = (1, micro_count, batch_rows, seq_len, d_model)
        return (h_out.reshape(shape), g_in.reshape(shape), gw_qkv[None], gb_qkv[None], gw_out.reshape(1, heads, head_dim, d_model), gb_out,
                g_ln[None], gw_one[None], gb_one, gw_two[None], gb_two)

    act_spec = P(None, "dp", None, None)
    arg_specs = (act_spec, act_spec,
                 P("pp", None, None, "tp", None), P("pp", None, "tp", None), P("pp", "tp", None, None),
                 P("pp", None), P("pp", None, None), P("pp", None, "tp"), P("pp", "tp"),
                 P("pp", "tp", None), P("pp", None))
    stage_spec = P("pp", None, "dp", None, None)
    grad_axes = ("dp", "pp")
    result_specs = (stage_spec, stage_spec,
                    P(grad_axes, None, None, "tp", None), P(grad_axes, None, "tp", None), P(grad_axes, "tp", None, None),
                    P(grad_axes, None), P(grad_axes, None, None), P(grad_axes, None, "tp"), P(grad_axes, "tp"),
                    P(grad_axes, "tp", None), P(grad_axes, None))
    return jax.shard_map(stage_program, mesh=mesh, in_specs=arg_specs, out_specs=result_specs, check_vma=False)
```

```python
import functools

import jax
import jax.numpy as jnp
from jax import lax
from jax.experimental import pallas as pl
from jax.experimental.pallas import tpu as pltpu
from jax.sharding import PartitionSpec as P

LN_EPS = 1e-5
F32 = jnp.float32
BF16 = jnp.bfloat16
MESH = pl.DeviceIdType.MESH
GELU_A = 0.7978845608028654
GELU_B = 0.044715
LOG2_E = 1.4426950408889634
ANY = pl.BlockSpec(memory_space=pl.ANY)
VMEM = pl.BlockSpec(memory_space=pltpu.VMEM)


def dot_nn(lhs, rhs):
    return jnp.dot(lhs, rhs, preferred_element_type=F32)


def dot_nt(lhs, rhs):
    return lax.dot_general(lhs, rhs, (((1,), (1,)), ((), ())), preferred_element_type=F32)


def dot_tn(lhs, rhs):
    return lax.dot_general(lhs, rhs, (((0,), (0,)), ((), ())), preferred_element_type=F32)


def norm_stats(x_wide):
    row_mean = jnp.mean(x_wide, axis=-1, keepdims=True)
    centered = x_wide - row_mean
    row_var = jnp.mean(centered * centered, axis=-1, keepdims=True)
    inv_std = lax.rsqrt(row_var + LN_EPS)
    return centered * inv_std, inv_std


def norm_backward(x_wide, gain, grad_h):
    normed, inv_std = norm_stats(x_wide)
    g_normed = grad_h * gain
    mean_g = jnp.mean(g_normed, axis=-1, keepdims=True)
    mean_gn = jnp.mean(g_normed * normed, axis=-1, keepdims=True)
    grad_x = (g_normed - mean_g - normed * mean_gn) * inv_std
    return grad_x, jnp.sum(grad_h * normed, axis=0, keepdims=True), jnp.sum(grad_h, axis=0, keepdims=True)


def gelu_parts(pre):
    square = pre * pre
    tanh = jnp.tanh(pre * (GELU_A + (GELU_A * GELU_B) * square))
    cdf = 0.5 + 0.5 * tanh
    return cdf, cdf + pre * (0.5 * GELU_A + (1.5 * GELU_A * GELU_B) * square) * (1.0 - tanh * tanh)


def chain_kernel(stages, tp, chunk, head_dim,
                 x_flat, dy_flat, wq_own, wo_own, w1_own, w2_own, ln_ref, b_qkv_ref, b_out_ref, b_one_ref, b_two_ref,
                 h_all, mid_all, gin_all, gmid_all, mix_all, gqkv_all, x_all, dy_all, h_one_all, h_two_all, act_all, gpre_all, slope_all, land_one, land_two, land_out, land_gq, land_gm, small_out,
                 wq, wq_t, wo, w1, w2, bias, x_buf, dy_buf, qkv, mix, mid, y_buf, gmid, gin, dkv, prob, dgelu, acc, hbuf, small, rep, bias_own, gscore,
                 own_sem, go_sem, done_sem, ring_send, ring_recv, fwd_send, fwd_recv, bias_send, bias_recv,
                 hop_send, hop_recv, gm_send, gm_recv, mix_send, mix_recv, row_send, row_recv, gq_send, gq_recv,
                 out_sem, px_send, px_recv, py_send, py_recv, sum_send, sum_recv, prep_sem, post_sem,
                 lw_send, lw_recv, lf_send, lf_recv, lg_send, lg_recv):
    stage = lax.axis_index("pp")
    me = lax.axis_index("tp")
    seq_len, d_model = x_buf.shape
    chunks = seq_len // chunk
    group = wo_own.shape[0]
    heads = group // head_dim
    last = stages - 1
    right, left, across = lax.rem(me + 1, tp), lax.rem(me + tp - 1, tp), lax.rem(me + 2, tp)
    not_first, not_last = stage > 0, stage < last
    peers = [lax.rem(me + off, tp) for off in range(1, tp)]
    even = lax.rem(stage, 2) == 0
    score_scale = head_dim ** -0.5

    middle = stages // 2
    eased, easing = stage == 1, stage == last
    helped, helping = stage < 2, (stage >= middle) & (stage < middle + 2)
    mate = lax.rem(stage + middle, stages)
    far = jnp.where(eased, last, 1)
    third, thirding = stage == middle - 1, stage == last

    def remote(src, dst, send, recv, axis, target):
        return pltpu.make_async_remote_copy(src_ref=src, dst_ref=dst, send_sem=send, recv_sem=recv,
                                            device_id={axis: target}, device_id_type=MESH)

    bias_own[...] = jnp.zeros_like(bias_own)
    bias_own[0:1, :] = b_one_ref[...].astype(F32)
    for part in range(3):
        for h_idx in range(heads):
            col = part * group + h_idx * head_dim
            bias_own[1:2, col:col + head_dim] = b_qkv_ref[part, h_idx:h_idx + 1, :].astype(F32)
    rep[0:4, :] = ln_ref[...].astype(F32)
    rep[4:5, :] = b_out_ref[...].astype(F32)
    rep[5:6, :] = b_two_ref[...].astype(F32)
    small[...] = jnp.zeros_like(small)
    small_out[...] = jnp.zeros_like(small_out)
    barrier = pltpu.get_barrier_semaphore()
    for peer in peers:
        pl.semaphore_signal(barrier, inc=1, device_id={"tp": peer}, device_id_type=MESH)

    @pl.when(not_first)
    def _():
        pl.semaphore_signal(barrier, inc=1, device_id={"pp": stage - 1}, device_id_type=MESH)

    @pl.when(not_last)
    def _():
        pl.semaphore_signal(barrier, inc=1, device_id={"pp": stage + 1}, device_id_type=MESH)

    @pl.when(helped | helping)
    def _():
        for there in (me, across):
            pl.semaphore_signal(barrier, inc=1, device_id={"pp": mate, "tp": there}, device_id_type=MESH)

    @pl.when(eased | easing)
    def _():
        for there in (me, across):
            pl.semaphore_signal(barrier, inc=1, device_id={"pp": far, "tp": there}, device_id_type=MESH)

    @pl.when(third | thirding)
    def _():
        for there in (me, across):
            pl.semaphore_signal(barrier, inc=1, device_id={"pp": mate, "tp": there}, device_id_type=MESH)

    near = tp - 1 + jnp.minimum(stage, 1) + jnp.minimum(last - stage, 1)
    pl.semaphore_wait(barrier, near + jnp.where(helped | helping, 2, 0) + jnp.where(eased | easing, 2, 0) + jnp.where(third | thirding, 2, 0))

    def shard(w_idx, origin):
        if w_idx == 1:
            return wo.at[pl.ds(pl.multiple_of(origin * group, group), group)]
        return (wq, None, w1, w2)[w_idx].at[origin]

    owns = (wq_own, wo_own, w1_own, w2_own)

    def half(ref, idx):
        size = ref.shape[0] // 2
        return ref.at[pl.ds(idx * size, size)]

    def ring_copy(w_idx, h_idx, side):
        return remote(half(owns[w_idx], h_idx), half(shard(w_idx, me), h_idx),
                      ring_send.at[w_idx, h_idx, side], ring_recv.at[w_idx, h_idx, side], "tp", left if side else right)

    def forward_copy(w_idx, side):
        block = half(shard(w_idx, right if side else left), side)
        return remote(block, block, fwd_send.at[w_idx, side], fwd_recv.at[w_idx, side], "tp", left if side else right)

    def bias_copy(slot):
        return remote(bias_own, bias.at[me], bias_send.at[slot], bias_recv.at[slot], "tp", peers[slot])

    def detour(src, dst, send, recv, target, target_tp):
        return pltpu.make_async_remote_copy(src_ref=src, dst_ref=dst, send_sem=send, recv_sem=recv,
                                            device_id={"pp": target, "tp": target_tp}, device_id_type=MESH)

    routes = ((2, 0, land_one, mate), (2, 1, land_one, far), (3, None, land_two, far), (1, None, land_out, mate))

    def piece(ref, h_idx):
        return ref if h_idx is None else half(ref, h_idx)

    def lw_copy(idx):
        w_idx, h_idx, land, target = routes[idx]
        return detour(piece(owns[w_idx], h_idx), piece(land, h_idx), lw_send.at[idx], lw_recv.at[idx], target, across)

    def lf_copy(idx):
        w_idx, h_idx, land, target = routes[idx]
        return detour(piece(land, h_idx), piece(shard(w_idx, across), h_idx), lf_send.at[idx], lf_recv.at[idx], target, me)

    own_copies = [pltpu.make_async_copy(owns[w_idx], shard(w_idx, me), own_sem.at[w_idx]) for w_idx in range(4)]
    own_copies.append(pltpu.make_async_copy(bias_own, bias.at[me], own_sem.at[4]))
    for own_copy in own_copies:
        own_copy.start()
    for slot in range(tp - 1):
        bias_copy(slot).start()

    def own_input(src, buf, dst):
        bounce = (y_buf, mid, gmid)
        copies = [pltpu.make_async_copy(src.at[me], buf, own_sem.at[5])]
        copies += [pltpu.make_async_copy(src.at[peers[slot]], bounce[slot], own_sem.at[6 + slot]) for slot in range(tp - 1)]
        for copy in copies:
            copy.start()
        for copy in copies:
            copy.wait()
        copies = [pltpu.make_async_copy(bounce[slot], dst.at[peers[slot]], own_sem.at[6 + slot]) for slot in range(tp - 1)]
        for copy in copies:
            copy.start()
        for copy in copies:
            copy.wait()

    @pl.when(eased)
    def _():
        for idx in range(4):
            lw_copy(idx).start()

    @pl.when(third)
    def _():
        lw_copy(3).start()

    @pl.when(stage == middle + 1)
    def _():
        for idx in (0, 3):
            lw_copy(idx).wait_recv()
            lf_copy(idx).start()

    @pl.when(easing)
    def _():
        for idx in (1, 2, 3):
            lw_copy(idx).wait_recv()
            lf_copy(idx).start()

    @pl.when(jnp.logical_not(even))
    def _():
        pl.semaphore_wait(go_sem, 1)

    for w_idx in range(4):
        for h_idx in range(2):
            ring_copy(w_idx, h_idx, 0).start()
            ring_copy(w_idx, 1 - h_idx, 1).start()

    @pl.when(stage == 0)
    def _():
        own_input(x_flat, x_buf, x_all)

    @pl.when(stage == last)
    def _():
        own_input(dy_flat, dy_buf, dy_all)

    qkv[...] = jnp.zeros_like(qkv)
    dkv[...] = jnp.zeros_like(dkv)

    for w_idx in range(4):
        for side in range(2):
            ring_copy(w_idx, side, side).wait_recv()
            if w_idx == 0:
                forward_copy(w_idx, side).start()
            else:
                @pl.when(jnp.logical_not(eased | third) if w_idx == 1 else jnp.logical_not(eased))
                def _():
                    forward_copy(w_idx, side).start()
    @pl.when(even)
    def _():
        pl.semaphore_signal(go_sem, inc=1, device_id={"pp": stage + 1}, device_id_type=MESH)

    for own_copy in own_copies:
        own_copy.wait()
    for slot in range(tp - 1):
        bias_copy(slot).wait()
    for w_idx in range(4):
        ring_copy(w_idx, 1, 0).wait_recv()
        ring_copy(w_idx, 0, 1).wait_recv()
        for h_idx in range(2):
            ring_copy(w_idx, h_idx, 0).wait_send()
            ring_copy(w_idx, h_idx, 1).wait_send()
    for side in range(2):
        forward_copy(0, side).wait()

    @pl.loop(0, tp)
    def _(t_idx):
        for part in range(3):
            wq_t[t_idx, :, part * group:(part + 1) * group] = wq[t_idx, part * group:(part + 1) * group, :].T

    @pl.when(jnp.logical_not(eased))
    def _():
        for w_idx in (2, 3):
            for side in range(2):
                forward_copy(w_idx, side).wait()

    @pl.when(jnp.logical_not(eased | third))
    def _():
        for side in range(2):
            forward_copy(1, side).wait()

    @pl.when(eased)
    def _():
        for idx in range(4):
            lf_copy(idx).wait_recv()
            lw_copy(idx).wait_send()

    @pl.when(third)
    def _():
        lf_copy(3).wait_recv()
        lw_copy(3).wait_send()

    @pl.when(stage == middle + 1)
    def _():
        for idx in (0, 3):
            lf_copy(idx).wait_send()

    @pl.when(easing)
    def _():
        for idx in (1, 2, 3):
            lf_copy(idx).wait_send()

    @pl.when(jnp.logical_not(even))
    def _():
        pl.semaphore_signal(done_sem, inc=1, device_id={"pp": stage - 1}, device_id_type=MESH)

    lane_head = lax.broadcasted_iota(jnp.int32, (chunk, group), 1) // head_dim

    def stack_heads(block):
        zero = jnp.zeros_like(block)
        return jnp.concatenate([jnp.where(lane_head == h_idx, block, zero) for h_idx in range(heads)], axis=0)

    def unstack_heads(stacked):
        total = stacked[:chunk]
        for h_idx in range(1, heads):
            total = jnp.where(lane_head == h_idx, stacked[h_idx * chunk:(h_idx + 1) * chunk], total)
        return total

    def hop_copy(c_idx, forward):
        rows = pl.ds(c_idx * chunk, chunk)
        src, dst, way, target = (y_buf, x_buf, 0, stage + 1) if forward else (gin, dy_buf, 1, stage - 1)
        return remote(src.at[rows], dst.at[rows], hop_send.at[way, c_idx], hop_recv.at[way, c_idx], "pp", target)

    size = group

    def flip(ref_get, ref_set, count):
        for row in range(count):
            ref_set(row, row, ref_get(row, row).T)
            for col in range(row):
                upper, lower = ref_get(col, row).T, ref_get(row, col).T
                ref_set(row, col, upper)
                ref_set(col, row, lower)

    def tile(row, col):
        return slice(row * size, (row + 1) * size), slice(col * size, (col + 1) * size)

    def flip_ff(ref, t_idx):
        def ref_set(row, col, value):
            ref[(t_idx,) + tile(row, col)] = value

        flip(lambda row, col: ref[(t_idx,) + tile(row, col)], ref_set, d_model // size)

    def flip_wo():
        def ref_set(row, col, value):
            wo[tile(row, col)] = value

        flip(lambda row, col: wo[tile(row, col)], ref_set, d_model // size)

    def layer_rows(c_idx, rows, flipping):
        normed, _ = norm_stats(x_buf[rows, :].astype(F32))
        hbuf[...] = (normed * rep[0:1, :] + rep[1:2, :]).astype(BF16)

        groups = range(tp)
        for t_idx in groups:
            pre = dot_nn(hbuf[...], wq_t[t_idx]) + bias[t_idx, 1:2, :3 * group]
            for part in range(3):
                qkv[part, t_idx, rows, :] = pre[:, part * group:(part + 1) * group].astype(BF16)

        row_pos = c_idx * chunk + lax.rem(lax.broadcasted_iota(jnp.int32, (heads * chunk, seq_len), 0), chunk)
        causal = row_pos >= lax.broadcasted_iota(jnp.int32, (heads * chunk, seq_len), 1)
        all_scores = [dot_nt(stack_heads(qkv[0, t_idx, rows, :]), qkv[1, t_idx]) for t_idx in groups]
        all_probs = []
        for t_idx in groups:
            scores = jnp.where(causal, all_scores[t_idx], -1e30)
            expd = jnp.exp2((scores - jnp.max(scores, axis=-1, keepdims=True)) * (score_scale * LOG2_E))
            probs = expd * (1.0 / jnp.sum(expd, axis=-1, keepdims=True))
            prob[c_idx, t_idx] = probs
            all_probs.append(probs.astype(BF16))
        for t_idx in groups:
            mix[t_idx, rows, :] = unstack_heads(dot_nn(all_probs[t_idx], qkv[2, t_idx])).astype(BF16)

        full_mix = jnp.concatenate([mix[t_idx, rows, :] for t_idx in groups], axis=1)
        x_mid = (x_buf[rows, :].astype(F32) + dot_nn(full_mix, wo[...]) + rep[4:5, :]).astype(BF16)
        mid[rows, :] = x_mid
        if flipping:
            flip_wo()
        normed_two, _ = norm_stats(x_mid.astype(F32))
        hbuf[...] = (normed_two * rep[2:3, :] + rep[3:4, :]).astype(BF16)
        total = jnp.zeros((chunk, d_model), F32)
        for t_idx in groups:
            pre = dot_nn(hbuf[...], w1[t_idx]) + bias[t_idx, 0:1, :]
            cdf, slope = gelu_parts(pre)
            dgelu[t_idx, rows, :] = slope
            total = total + dot_nn((pre * cdf).astype(BF16), w2[t_idx])
            if flipping:
                flip_ff(w1, t_idx)

        y_buf[rows, :] = (mid[rows, :].astype(F32) + total + rep[5:6, :]).astype(BF16)

    gathers = ((y_buf, h_all), (mid, mid_all), (gin, gin_all))

    def row_copy(kind, c_idx, side):
        rows = pl.ds(c_idx * chunk, chunk)
        src, dst = gathers[kind]
        return remote(src.at[rows], dst.at[me, rows], row_send.at[kind, c_idx, side], row_recv.at[kind, c_idx, side], "tp", left if side else right)

    def row_forward(kind, c_idx, side):
        rows = pl.ds(c_idx * chunk + side * (chunk // 2), chunk // 2)
        block = gathers[kind][1].at[right if side else left, rows]
        return remote(block, block, row_send.at[kind, c_idx, 2 + side], row_recv.at[kind, c_idx, 2 + side], "tp", left if side else right)

    def start_rows(c_idx):
        for kind in range(2):
            for side in range(2):
                row_copy(kind, c_idx, side).start()

    prompt = (stage >= middle) | jnp.logical_not(even)

    def fwd_chunk(c_idx, carry):
        rows = pl.ds(pl.multiple_of(c_idx * chunk, chunk), chunk)

        @pl.when(not_first)
        def _():
            hop_copy(c_idx, True).wait_recv()

        turning = (stage == last) & (c_idx == chunks - 1)

        @pl.when(jnp.logical_not(turning))
        def _():
            layer_rows(c_idx, rows, False)

        @pl.when(turning)
        def _():
            layer_rows(c_idx, rows, True)

        @pl.when(not_last)
        def _():
            hop_copy(c_idx, True).start()

        @pl.when(prompt & even & (c_idx == 0))
        def _():
            pl.semaphore_wait(done_sem, 1)

        @pl.when(prompt)
        def _():
            start_rows(c_idx)

        return carry

    lax.fori_loop(0, chunks, fwd_chunk, 0)

    def mix_copy(slot):
        return remote(mix.at[peers[slot]], mix_all.at[me], mix_send.at[slot], mix_recv.at[slot], "tp", peers[slot])

    for slot in range(tp - 1):
        mix_copy(slot).start()
    fwd_out = [pltpu.make_async_copy(y_buf, h_all.at[me], out_sem.at[0]),
               pltpu.make_async_copy(mid, mid_all.at[me], out_sem.at[1]),
               pltpu.make_async_copy(mix.at[me], mix_all.at[me], out_sem.at[2]),
               pltpu.make_async_copy(x_buf, x_all.at[me], out_sem.at[3])]
    for out_copy in fwd_out:
        out_copy.start()

    def pass_x(slot):
        origin = peers[slot]
        return remote(h_all.at[origin], x_all.at[origin], px_send.at[slot], px_recv.at[slot], "pp", stage + 1)

    def forward_fwd_gather():
        for c_idx in range(chunks):
            for kind in range(2):
                for side in range(2):
                    row_copy(kind, c_idx, side).wait_recv()
                    row_forward(kind, c_idx, side).start()

    def finish_fwd_gather():
        for c_idx in range(chunks):
            for kind in range(2):
                for side in range(2):
                    row_forward(kind, c_idx, side).wait_recv()

        @pl.when(not_last)
        def _():
            for slot in range(tp - 1):
                pass_x(slot).start()

    @pl.loop(0, tp)
    def _(t_idx):
        flip_ff(w2, t_idx)

    @pl.when(not_last)
    def _():
        @pl.loop(0, tp)
        def _(t_idx):
            flip_ff(w1, t_idx)

        flip_wo()

    @pl.when(jnp.logical_not(prompt))
    def _():
        pl.semaphore_wait(done_sem, 1)
        for c_idx in range(chunks):
            start_rows(c_idx)

    @pl.when(stage < last - 1)
    def _():
        forward_fwd_gather()

    @pl.when(stage < stages // 2)
    def _():
        finish_fwd_gather()

    def gm_copy(side):
        return remote(gmid, gmid_all.at[me], gm_send.at[side], gm_recv.at[side], "tp", left if side else right)

    def gm_forward(side):
        rows = pl.ds(side * (seq_len // 2), seq_len // 2)
        block = gmid_all.at[right if side else left, rows]
        return remote(block, block, gm_send.at[2 + side], gm_recv.at[2 + side], "tp", left if side else right)

    def gqkv_of(t_idx):
        return wq_t.at[t_idx, pl.ds(0, seq_len)]

    def gq_copy(slot):
        return remote(gqkv_of(peers[slot]), gqkv_all.at[me], gq_send.at[slot], gq_recv.at[slot], "tp", peers[slot])

    gm_way = jnp.where(eased | easing, far, mate)
    gm_helping = (stage == middle) | easing

    def gl_copy(idx):
        return detour(gmid if idx else gqkv_of(across), land_gm if idx else land_gq, lg_send.at[idx], lg_recv.at[idx], gm_way if idx else mate, across)

    def gf_copy(idx):
        return detour(land_gm if idx else land_gq, (gmid_all if idx else gqkv_all).at[across], lg_send.at[2 + idx], lg_recv.at[2 + idx], gm_way if idx else mate, me)

    def pass_dy(c_idx, slot):
        rows = pl.ds(c_idx * chunk, chunk)
        origin = peers[slot]
        return remote(gin_all.at[origin, rows], dy_all.at[origin, rows], py_send.at[c_idx, slot], py_recv.at[c_idx, slot], "pp", stage - 1)

    def forward_chunk(c_idx):
        for side in range(2):
            row_copy(2, c_idx, side).wait_recv()
            row_forward(2, c_idx, side).start()

    def pass_chunk(c_idx):
        for side in range(2):
            row_forward(2, c_idx, side).wait_recv()

        @pl.when(not_first)
        def _():
            for slot in range(tp - 1):
                pass_dy(c_idx, slot).start()

    w1_own_t, w2_own_t = w1.at[me], w2.at[me]
    early = stage < stages // 2 - 1

    def prep(two_buf, one_buf, act_buf, keep_slopes):
        @pl.when(not_first)
        def _():
            for slot in range(tp - 1):
                pass_x(slot).wait_recv()

        def prep_seq(t_idx, carry):
            loads = [pltpu.make_async_copy(mid_all.at[t_idx], two_buf, prep_sem.at[0]), pltpu.make_async_copy(x_all.at[t_idx], one_buf, prep_sem.at[1])]
            for load in loads:
                load.start()
            for load in loads:
                load.wait()

            def prep_rows(c_idx, inner):
                rows = pl.ds(pl.multiple_of(c_idx * chunk, chunk), chunk)
                normed, _ = norm_stats(two_buf[rows, :].astype(F32))
                two_buf[rows, :] = (normed * rep[2:3, :] + rep[3:4, :]).astype(BF16)
                normed_one, _ = norm_stats(one_buf[rows, :].astype(F32))
                one_buf[rows, :] = (normed_one * rep[0:1, :] + rep[1:2, :]).astype(BF16)
                pre = dot_nt(two_buf[rows, :], w1_own_t[...]) + bias[me, 0:1, :]
                cdf, slope = gelu_parts(pre)
                act_buf[rows, :] = (pre * cdf).astype(BF16)
                if keep_slopes:
                    keep = pltpu.make_async_copy(acc, slope_all.at[t_idx, rows], prep_sem.at[2])

                    @pl.when(c_idx > 0)
                    def _():
                        keep.wait()

                    acc[...] = slope
                    keep.start()
                else:
                    dgelu[t_idx, rows, :] = slope
                return inner

            lax.fori_loop(0, chunks, prep_rows, 0)
            if keep_slopes:
                pltpu.make_async_copy(acc, slope_all.at[t_idx, pl.ds(0, chunk)], prep_sem.at[2]).wait()
            keeps = [pltpu.make_async_copy(two_buf, h_two_all.at[t_idx], prep_sem.at[0]), pltpu.make_async_copy(one_buf, h_one_all.at[t_idx], prep_sem.at[1]),
                     pltpu.make_async_copy(act_buf, act_all.at[t_idx], prep_sem.at[2])]
            for keep in keeps:
                keep.start()
            for keep in keeps:
                keep.wait()
            return carry

        lax.fori_loop(0, tp, prep_seq, 0)

    def end_fwd_sends():
        for c_idx in range(chunks):
            for kind in range(2):
                for side in range(2):
                    row_copy(kind, c_idx, side).wait_send()
        for slot in range(tp - 1):
            mix_copy(slot).wait_send()
        for out_copy in fwd_out:
            out_copy.wait()

        @pl.when(not_last)
        def _():
            for c_idx in range(chunks):
                hop_copy(c_idx, True).wait_send()

    @pl.when(early)
    def _():
        end_fwd_sends()
        prep(gmid, gin, y_buf, True)

    def bwd_chunk(step, carry):
        c_idx = chunks - 1 - step
        rows = pl.ds(pl.multiple_of(c_idx * chunk, chunk), chunk)

        @pl.when(not_last)
        def _():
            hop_copy(c_idx, False).wait_recv()

        groups = range(tp)
        g_h_sum = jnp.zeros((chunk, d_model), F32)
        for t_idx in groups:
            g_gelu = dot_nn(dy_buf[rows, :], w2[t_idx]).astype(BF16).astype(F32)
            g_h_sum = g_h_sum + dot_nn((g_gelu * dgelu[t_idx, rows, :]).astype(BF16), w1[t_idx])

        g_h_two = g_h_sum.astype(BF16).astype(F32)
        dy_wide = dy_buf[rows, :].astype(F32)
        g_ln, g_gain, g_shift = norm_backward(mid[rows, :].astype(F32), rep[2:3, :], g_h_two)
        g_mid = (dy_wide + g_ln.astype(BF16).astype(F32)).astype(BF16)
        gmid[rows, :] = g_mid
        small[me, 2:3, :] += g_gain
        small[me, 3:4, :] += g_shift
        small[me, 4:5, :] += jnp.sum(g_mid.astype(F32), axis=0, keepdims=True)
        small[me, 5:6, :] += jnp.sum(dy_wide, axis=0, keepdims=True)
        hbuf[...] = dot_nn(gmid[rows, :], wo[...]).astype(BF16)
        g_stacks = [stack_heads(hbuf[:, t_idx * group:(t_idx + 1) * group]) for t_idx in groups]
        g_probs = [dot_nt(g_stacks[t_idx], qkv[2, t_idx]).astype(BF16).astype(F32) for t_idx in groups]
        g_values = [dot_tn(prob[c_idx, t_idx, :, rows].astype(BF16), g_stacks[t_idx]) for t_idx in groups]
        for t_idx in groups:
            probs = prob[c_idx, t_idx]
            inner = jnp.sum(g_probs[t_idx] * probs, axis=-1, keepdims=True)
            gscore[t_idx] = (probs * (g_probs[t_idx] - inner)).astype(BF16)
            wq_t[t_idx, rows, 2 * group:3 * group] = (dkv[1, t_idx, rows, :] + g_values[t_idx]).astype(BF16)
        for t_idx in groups:
            wq_t[t_idx, rows, 0:group] = (unstack_heads(dot_nn(gscore[t_idx], qkv[1, t_idx])) * score_scale).astype(BF16)
            g_keys = dot_tn(gscore[t_idx, :, rows], stack_heads(qkv[0, t_idx, rows, :]))
            wq_t[t_idx, rows, group:2 * group] = ((dkv[0, t_idx, rows, :] + g_keys) * score_scale).astype(BF16)
        g_h_sum = jnp.zeros((chunk, d_model), F32)
        for t_idx in groups:
            g_h_sum = g_h_sum + dot_nn(wq_t[t_idx, rows, :], wq[t_idx])

        g_h_one = g_h_sum.astype(BF16).astype(F32)
        g_ln_one, g_gain_one, g_shift_one = norm_backward(x_buf[rows, :].astype(F32), rep[0:1, :], g_h_one)
        gin[rows, :] = (gmid[rows, :].astype(F32) + g_ln_one.astype(BF16).astype(F32)).astype(BF16)
        small[me, 0:1, :] += g_gain_one
        small[me, 1:2, :] += g_shift_one

        @pl.when(not_first)
        def _():
            hop_copy(c_idx, False).start()

        for side in range(2):
            row_copy(2, c_idx, side).start()

        def earlier_rows(block, inner):
            keys = pl.ds(pl.multiple_of(block * chunk, chunk), chunk)
            for t_idx in groups:
                dkv[0, t_idx, keys, :] += dot_tn(gscore[t_idx, :, keys], stack_heads(qkv[0, t_idx, rows, :]))
                g_stack = stack_heads(hbuf[:, t_idx * group:(t_idx + 1) * group])
                dkv[1, t_idx, keys, :] += dot_tn(prob[c_idx, t_idx, :, keys].astype(BF16), g_stack)
            return inner

        lax.fori_loop(0, c_idx, earlier_rows, 0)

        @pl.when((step >= 2) & (stage < last - 1))
        def _():
            forward_chunk(c_idx + 2)

        return carry

    lax.fori_loop(0, chunks, bwd_chunk, 0)

    def sum_copy(slot):
        return remote(small.at[me], small.at[me], sum_send.at[slot], sum_recv.at[slot], "tp", peers[slot])

    for slot in range(tp - 1):
        sum_copy(slot).start()
    bwd_out = [pltpu.make_async_copy(gin, gin_all.at[me], out_sem.at[4]),
               pltpu.make_async_copy(gmid, gmid_all.at[me], out_sem.at[5]),
               pltpu.make_async_copy(gqkv_of(me), gqkv_all.at[me], out_sem.at[6]),
               pltpu.make_async_copy(dy_buf, dy_all.at[me], out_sem.at[7])]
    for out_copy in bwd_out:
        out_copy.start()

    @pl.when(helped)
    def _():
        for idx in range(2):
            gl_copy(idx).start()


    @pl.when((stage >= stages // 2) & (stage < last - 1))
    def _():
        finish_fwd_gather()

    @pl.when(stage >= last - 1)
    def _():
        forward_fwd_gather()
        forward_chunk(chunks - 1)

    for c_idx in range(chunks - 2, -1, -1):
        forward_chunk(c_idx)

    @pl.when(stage >= last - 1)
    def _():
        finish_fwd_gather()

    for side in range(2):
        gm_copy(side).start()
    for slot in (0, 2, 1):
        if slot == 1:
            @pl.when(jnp.logical_not(helped))
            def _():
                gq_copy(slot).start()
        else:
            gq_copy(slot).start()

    def pass_all():
        for c_idx in range(chunks - 1, -1, -1):
            pass_chunk(c_idx)

    @pl.when(not_last)
    def _():
        pass_all()

    @pl.when(early)
    def _():
        slopes = pltpu.make_async_copy(slope_all, dgelu, prep_sem.at[0])
        slopes.start()
        slopes.wait()

    @pl.when(jnp.logical_not(early))
    def _():
        end_fwd_sends()
        prep(mid, x_buf, y_buf, False)

    @pl.when(stage == last)
    def _():
        pass_all()

    def finish_rows(t_idx, src, dst, rows):
        grad = dot_nn(src[rows, :], w2_own_t[...]).astype(BF16).astype(F32) * dgelu[t_idx, rows, :]
        small_out[6:7, :] += jnp.sum(grad, axis=0, keepdims=True)
        dst[rows, :] = grad.astype(BF16)

    def finish_own(c_idx, carry):
        finish_rows(me, dy_buf, y_buf, pl.ds(pl.multiple_of(c_idx * chunk, chunk), chunk))
        return carry

    lax.fori_loop(0, chunks, finish_own, 0)
    own_keep = pltpu.make_async_copy(y_buf, gpre_all.at[me], prep_sem.at[0])
    own_keep.start()
    @pl.when(helping)
    def _():
        gl_copy(0).wait_recv()
        gf_copy(0).start()

    @pl.when(gm_helping)
    def _():
        gl_copy(1).wait_recv()
        gf_copy(1).start()

    @pl.when(jnp.logical_not(helped))
    def _():
        for side in range(2):
            gm_copy(side).wait_recv()
            gm_forward(side).start()

    own_keep.wait()

    def finish_peers(step, carry):
        c_idx = chunks - 1 - step
        rows = pl.ds(pl.multiple_of(c_idx * chunk, chunk), chunk)
        bufs = (x_buf, mid, y_buf)

        @pl.when(not_last)
        def _():
            for slot in range(tp - 1):
                pass_dy(c_idx, slot).wait_recv()

        loads = [pltpu.make_async_copy(dy_all.at[peers[slot], rows], bufs[slot].at[rows], post_sem.at[slot]) for slot in range(tp - 1)]
        keeps = [pltpu.make_async_copy(bufs[slot].at[rows], gpre_all.at[peers[slot], rows], post_sem.at[slot]) for slot in range(tp - 1)]
        for load in loads:
            load.start()
        for slot in range(tp - 1):
            loads[slot].wait()
            finish_rows(peers[slot], bufs[slot], bufs[slot], rows)
            keeps[slot].start()
        for keep in keeps:
            keep.wait()
        return carry

    lax.fori_loop(0, chunks, finish_peers, 0)
    for slot in range(tp - 1):
        sum_copy(slot).wait()
    total_small = small[0, 0:6, :]
    for t_idx in range(1, tp):
        total_small = total_small + small[t_idx, 0:6, :]
    small_out[0:6, :] = total_small

    for slot in range(tp - 1):
        mix_copy(slot).wait_recv()
        if slot != 1:
            gq_copy(slot).wait()

    @pl.when(jnp.logical_not(helped))
    def _():
        gq_copy(1).wait()
        for side in range(2):
            gm_forward(side).wait()

    @pl.when(helped)
    def _():
        for side in range(2):
            gm_copy(side).wait_recv()
        for idx in range(2):
            gl_copy(idx).wait_send()
            gf_copy(idx).wait_recv()

    @pl.when(helping)
    def _():
        gf_copy(0).wait_send()

    @pl.when(gm_helping)
    def _():
        gf_copy(1).wait_send()

    for side in range(2):
        gm_copy(side).wait_send()
        for c_idx in range(chunks):
            for kind in range(2):
                row_forward(kind, c_idx, side).wait_send()
            row_copy(2, c_idx, side).wait_send()
            row_forward(2, c_idx, side).wait_send()
    for out_copy in bwd_out:
        out_copy.wait()

    @pl.when(not_last)
    def _():
        for slot in range(tp - 1):
            pass_x(slot).wait_send()

    @pl.when(not_first)
    def _():
        for c_idx in range(chunks):
            hop_copy(c_idx, False).wait_send()
            for slot in range(tp - 1):
                pass_dy(c_idx, slot).wait_send()


def run_chain(stages, tp, x_flat, dy_flat, wq, wo, w1, w2, ln_par, b_qkv, b_out, b_one, b_two, head_dim):
    _, seq_len, d_model = x_flat.shape
    chunk = min(128, seq_len)
    chunks = seq_len // chunk
    group = wo.shape[0]
    heads = group // head_dim
    ff_local = w1.shape[1]
    rows = (tp, seq_len, d_model)
    outs = [jax.ShapeDtypeStruct(rows, BF16)] * 4
    outs += [jax.ShapeDtypeStruct((tp, seq_len, group), BF16), jax.ShapeDtypeStruct((tp, seq_len, 3 * group), BF16)]
    outs += [jax.ShapeDtypeStruct(rows, BF16)] * 4 + [jax.ShapeDtypeStruct((tp, seq_len, ff_local), BF16)] * 2
    outs += [jax.ShapeDtypeStruct((tp, seq_len, ff_local), F32), jax.ShapeDtypeStruct(w1.shape, BF16), jax.ShapeDtypeStruct(w2.shape, BF16)]
    outs += [jax.ShapeDtypeStruct(wo.shape, BF16)]
    outs += [jax.ShapeDtypeStruct((seq_len, 3 * group), BF16), jax.ShapeDtypeStruct((seq_len, d_model), BF16), jax.ShapeDtypeStruct((8, d_model), F32)]
    act = pltpu.VMEM((seq_len, d_model), BF16)
    dma = pltpu.SemaphoreType.DMA
    scratch = [
        pltpu.VMEM((tp,) + wq.shape, BF16), pltpu.VMEM((tp,) + wq.shape[::-1], BF16), pltpu.VMEM((tp * group, d_model), BF16),
        pltpu.VMEM((tp,) + w1.shape, BF16), pltpu.VMEM((tp,) + w2.shape, BF16),
        pltpu.VMEM((tp, 8, d_model), F32),
        act, act,
        pltpu.VMEM((3, tp, seq_len, group), BF16), pltpu.VMEM((tp, seq_len, group), BF16),
        act, act, act, act,
        pltpu.VMEM((2, tp, seq_len, group), F32),
        pltpu.VMEM((chunks, tp, heads * chunk, seq_len), F32), pltpu.VMEM((tp, seq_len, ff_local), F32),
        pltpu.VMEM((chunk, d_model), F32), pltpu.VMEM((chunk, d_model), BF16), pltpu.VMEM((tp, 8, d_model), F32),
        pltpu.VMEM((8, d_model), F32), pltpu.VMEM((8, d_model), F32), pltpu.VMEM((tp, heads * chunk, seq_len), BF16),
        dma((9,)), pltpu.SemaphoreType.REGULAR, pltpu.SemaphoreType.REGULAR, dma((4, 2, 2)), dma((4, 2, 2)), dma((4, 2)), dma((4, 2)), dma((tp - 1,)), dma((tp - 1,)),
        dma((2, chunks)), dma((2, chunks)), dma((4,)), dma((4,)), dma((tp - 1,)), dma((tp - 1,)),
        dma((3, chunks, 4)), dma((3, chunks, 4)), dma((tp - 1,)), dma((tp - 1,)),
        dma((8,)), dma((tp - 1,)), dma((tp - 1,)), dma((chunks, tp - 1)), dma((chunks, tp - 1)), dma((tp - 1,)), dma((tp - 1,)), dma((3,)), dma((tp - 1,)),
        dma((4,)), dma((4,)), dma((4,)), dma((4,)), dma((4,)), dma((4,)),
    ]
    return pl.pallas_call(
        functools.partial(chain_kernel, stages, tp, chunk, head_dim),
        out_shape=outs,
        in_specs=[ANY] * 6 + [VMEM] * 5,
        out_specs=[ANY] * 18 + [VMEM],
        scratch_shapes=scratch,
        compiler_params=pltpu.CompilerParams(collective_id=0, has_side_effects=True, vmem_limit_bytes=67043328),
        name="chain",
    )(x_flat, dy_flat, wq, wo, w1, w2, ln_par, b_qkv, b_out, b_one, b_two)


def wgrad_kernel(act, dy, gpre, h_two, gqkv, h_one, mix, gmid, h_all, gin_all, small,
                 gw_two, gw_one, gw_qkv, gw_out, h_out, g_in, g_ln, gb_out, gb_two, gb_one, gb_qkv,
                 act_v, dy_v, gpre_v, h_two_v, gq_v, h_one_v, mix_v, gmid_v, h_v, gin_v, two_v, one_v, qkv_v, out_v,
                 in_sem, two_sem, one_sem, qkv_sem, res_sem, keep_sem):
    heads, head_dim = gb_qkv.shape[1:]
    group = heads * head_dim
    pairs = ((act, act_v), (dy, dy_v), (gpre, gpre_v), (h_two, h_two_v), (gqkv, gq_v), (h_one, h_one_v), (mix, mix_v), (gmid, gmid_v), (h_all, h_v), (gin_all, gin_v))
    loads = [pltpu.make_async_copy(src, dst, in_sem.at[idx]) for idx, (src, dst) in enumerate(pairs)]
    for load in loads:
        load.start()
    g_ln[...] = small[0:4, :]
    gb_out[...] = small[4:5, :]
    gb_two[...] = small[5:6, :]
    gb_one[...] = small[6:7, :]

    def product(lhs, rhs, buf, dst, sem, tiles):
        tile = buf.shape[0] // tiles

        def copy_of(row):
            rows = pl.ds(pl.multiple_of(row * tile, tile), tile)
            return pltpu.make_async_copy(buf.at[rows], dst.at[rows], sem.at[row])

        @pl.loop(0, tiles)
        def _(row):
            cols = pl.ds(pl.multiple_of(row * tile, tile), tile)
            buf[cols, :] = dot_tn(lhs[:, cols], rhs[...])
            copy_of(row).start()

        return lambda: [copy_of(row).wait() for row in range(tiles)]

    loads[0].wait()
    loads[1].wait()
    ends = [product(act_v, dy_v, two_v, gw_two, two_sem, 2)]
    loads[2].wait()
    loads[3].wait()
    ends.append(product(h_two_v, gpre_v, one_v, gw_one, one_sem, 2))
    loads[4].wait()
    loads[5].wait()
    ends.append(product(gq_v, h_one_v, qkv_v, gw_qkv, qkv_sem, 2))
    for part in range(3):
        total = jnp.sum(gq_v[:, part * group:(part + 1) * group].astype(F32), axis=0, keepdims=True)
        for h_idx in range(heads):
            gb_qkv[part, h_idx:h_idx + 1, :] = total[:, h_idx * head_dim:(h_idx + 1) * head_dim]
    loads[8].wait()
    loads[9].wait()
    keeps = [pltpu.make_async_copy(h_v, h_out, keep_sem.at[0]), pltpu.make_async_copy(gin_v, g_in, keep_sem.at[1])]
    for keep in keeps:
        keep.start()
    loads[6].wait()
    loads[7].wait()
    ends.append(product(mix_v, gmid_v, out_v, gw_out, res_sem, 1))
    for end in ends:
        end()
    for keep in keeps:
        keep.wait()


def run_wgrad(act, dy, gpre, h_two, gqkv, h_one, mix, gmid, h_all, gin_all, small, head_dim):
    def flat(array):
        return array.reshape(array.shape[0] * array.shape[1], array.shape[2])

    group, d_model, ff_local = mix.shape[2], dy.shape[2], act.shape[2]
    seqs, seq_len = dy.shape[:2]
    total = seqs * seq_len
    dma = pltpu.SemaphoreType.DMA
    grads = [(ff_local, d_model), (d_model, ff_local), (3 * group, d_model), (group, d_model)]
    rows = jax.ShapeDtypeStruct((total, d_model), BF16)
    smalls = [(4, d_model), (1, d_model), (1, d_model), (1, ff_local), (3, group // head_dim, head_dim)]
    widths = (ff_local, d_model, ff_local, d_model)
    return pl.pallas_call(
        wgrad_kernel,
        in_specs=[ANY] * 10 + [VMEM],
        out_specs=[ANY] * 6 + [VMEM] * 5,
        out_shape=[jax.ShapeDtypeStruct(shape, F32) for shape in grads] + [rows, rows] + [jax.ShapeDtypeStruct(shape, F32) for shape in smalls],
        scratch_shapes=[pltpu.VMEM((total, width), BF16) for width in widths]
        + [pltpu.VMEM((total, 3 * group), BF16), pltpu.VMEM((total, d_model), BF16), pltpu.VMEM((total, group), BF16)]
        + [pltpu.VMEM((total, d_model), BF16)] * 3 + [pltpu.VMEM(shape, F32) for shape in grads]
        + [dma((10,))] + [dma((shape[0] // group,)) for shape in grads] + [dma((2,))],
        compiler_params=pltpu.CompilerParams(vmem_limit_bytes=67043328),
        name="wgrad",
    )(flat(act), flat(dy), flat(gpre), flat(h_two), flat(gqkv), flat(h_one), flat(mix), flat(gmid), flat(h_all), flat(gin_all), small)


def solution(mesh):
    stages = mesh.shape["pp"]
    tp = mesh.shape["tp"]

    def stage_program(x_in, dy_out, w_qkv, b_qkv, w_out, b_out, ln_par, w_fc1, b_fc1, w_fc2, b_fc2):
        micro_count, batch_rows, seq_len, d_model = x_in.shape
        head_dim = w_qkv.shape[4]
        group = w_qkv.shape[3] * head_dim
        heads = group // head_dim
        seqs = micro_count * batch_rows
        wq = jnp.transpose(w_qkv[0], (0, 2, 3, 1)).reshape(3 * group, d_model)
        wo = w_out[0].reshape(group, d_model)
        w1, w2 = w_fc1[0], w_fc2[0]
        x_flat = x_in.reshape(seqs, seq_len, d_model)
        dy_flat = dy_out.reshape(seqs, seq_len, d_model)
        h_all, _, gin_all, gmid_all, mix_all, gqkv_all, _, dy_all, h_one, h_two, act, gpre, _, _, _, _, _, _, small = run_chain(
            stages, tp, x_flat, dy_flat, wq, wo, w1, w2, ln_par[0], b_qkv[0], b_out, b_fc1, b_fc2, head_dim)
        gw_two, gw_one, gw_qkv, gw_out, h_out, g_in, g_ln, gb_out, gb_two, gb_one, gb_qkv = run_wgrad(
            act, dy_all, gpre, h_two, gqkv_all, h_one, mix_all, gmid_all, h_all, gin_all, small, head_dim)
        gw_qkv = jnp.transpose(gw_qkv.reshape(3, heads, head_dim, d_model), (0, 3, 1, 2))
        shape = (1, micro_count, batch_rows, seq_len, d_model)
        return (h_out.reshape(shape), g_in.reshape(shape), gw_qkv[None], gb_qkv[None], gw_out.reshape(1, heads, head_dim, d_model), gb_out,
                g_ln[None], gw_one[None], gb_one, gw_two[None], gb_two)

    act_spec = P(None, "dp", None, None)
    arg_specs = (act_spec, act_spec,
                 P("pp", None, None, "tp", None), P("pp", None, "tp", None), P("pp", "tp", None, None),
                 P("pp", None), P("pp", None, None), P("pp", None, "tp"), P("pp", "tp"),
                 P("pp", "tp", None), P("pp", None))
    stage_spec = P("pp", None, "dp", None, None)
    grad_axes = ("dp", "pp")
    result_specs = (stage_spec, stage_spec,
                    P(grad_axes, None, None, "tp", None), P(grad_axes, None, "tp", None), P(grad_axes, "tp", None, None),
                    P(grad_axes, None), P(grad_axes, None, None), P(grad_axes, None, "tp"), P(grad_axes, "tp"),
                    P(grad_axes, "tp", None), P(grad_axes, None))
    return jax.shard_map(stage_program, mesh=mesh, in_specs=arg_specs, out_specs=result_specs, check_vma=False)
```

```python
import functools

import jax
import jax.numpy as jnp
from jax import lax
from jax.experimental import pallas as pl
from jax.experimental.pallas import tpu as pltpu
from jax.sharding import PartitionSpec as P

LN_EPS = 1e-5
F32 = jnp.float32
BF16 = jnp.bfloat16
MESH = pl.DeviceIdType.MESH
GELU_A = 0.7978845608028654
GELU_B = 0.044715
LOG2_E = 1.4426950408889634
ANY = pl.BlockSpec(memory_space=pl.ANY)
VMEM = pl.BlockSpec(memory_space=pltpu.VMEM)


def dot_nn(lhs, rhs):
    return jnp.dot(lhs, rhs, preferred_element_type=F32)


def dot_nt(lhs, rhs):
    return lax.dot_general(lhs, rhs, (((1,), (1,)), ((), ())), preferred_element_type=F32)


def dot_tn(lhs, rhs):
    return lax.dot_general(lhs, rhs, (((0,), (0,)), ((), ())), preferred_element_type=F32)


def norm_stats(x_wide):
    row_mean = jnp.mean(x_wide, axis=-1, keepdims=True)
    centered = x_wide - row_mean
    row_var = jnp.mean(centered * centered, axis=-1, keepdims=True)
    inv_std = lax.rsqrt(row_var + LN_EPS)
    return centered * inv_std, inv_std


def norm_backward(x_wide, gain, grad_h):
    normed, inv_std = norm_stats(x_wide)
    g_normed = grad_h * gain
    mean_g = jnp.mean(g_normed, axis=-1, keepdims=True)
    mean_gn = jnp.mean(g_normed * normed, axis=-1, keepdims=True)
    grad_x = (g_normed - mean_g - normed * mean_gn) * inv_std
    return grad_x, jnp.sum(grad_h * normed, axis=0, keepdims=True), jnp.sum(grad_h, axis=0, keepdims=True)


def gelu_parts(pre):
    square = pre * pre
    tanh = jnp.tanh(pre * (GELU_A + (GELU_A * GELU_B) * square))
    cdf = 0.5 + 0.5 * tanh
    return cdf, cdf + pre * (0.5 * GELU_A + (1.5 * GELU_A * GELU_B) * square) * (1.0 - tanh * tanh)


def chain_kernel(stages, tp, chunk, head_dim,
                 x_flat, dy_flat, wq_own, wo_own, w1_own, w2_own, ln_ref, b_qkv_ref, b_out_ref, b_one_ref, b_two_ref,
                 h_all, mid_all, gin_all, gmid_all, mix_all, gqkv_all, x_all, dy_all, h_one_all, h_two_all, act_all, gpre_all, slope_all, land_one, land_two, land_out, land_gq, land_gm, small_out,
                 wq, wq_t, wo, w1, w2, bias, x_buf, dy_buf, qkv, mix, mid, y_buf, gmid, gin, dkv, prob, dgelu, acc, hbuf, small, rep, bias_own, gscore,
                 own_sem, go_sem, done_sem, ring_send, ring_recv, fwd_send, fwd_recv, bias_send, bias_recv,
                 hop_send, hop_recv, gm_send, gm_recv, mix_send, mix_recv, row_send, row_recv, gq_send, gq_recv,
                 out_sem, px_send, px_recv, py_send, py_recv, sum_send, sum_recv, prep_sem, post_sem,
                 lw_send, lw_recv, lf_send, lf_recv, lg_send, lg_recv):
    stage = lax.axis_index("pp")
    me = lax.axis_index("tp")
    seq_len, d_model = x_buf.shape
    chunks = seq_len // chunk
    group = wo_own.shape[0]
    heads = group // head_dim
    last = stages - 1
    right, left, across = lax.rem(me + 1, tp), lax.rem(me + tp - 1, tp), lax.rem(me + 2, tp)
    not_first, not_last = stage > 0, stage < last
    peers = [lax.rem(me + off, tp) for off in range(1, tp)]
    even = lax.rem(stage, 2) == 0
    score_scale = head_dim ** -0.5

    middle = stages // 2
    eased, easing = stage == 1, stage == last
    helped, helping = stage < 2, (stage >= middle) & (stage < middle + 2)
    mate = lax.rem(stage + middle, stages)
    far = jnp.where(eased, last, 1)

    def remote(src, dst, send, recv, axis, target):
        return pltpu.make_async_remote_copy(src_ref=src, dst_ref=dst, send_sem=send, recv_sem=recv,
                                            device_id={axis: target}, device_id_type=MESH)

    bias_own[...] = jnp.zeros_like(bias_own)
    bias_own[0:1, :] = b_one_ref[...].astype(F32)
    for part in range(3):
        for h_idx in range(heads):
            col = part * group + h_idx * head_dim
            bias_own[1:2, col:col + head_dim] = b_qkv_ref[part, h_idx:h_idx + 1, :].astype(F32)
    rep[0:4, :] = ln_ref[...].astype(F32)
    rep[4:5, :] = b_out_ref[...].astype(F32)
    rep[5:6, :] = b_two_ref[...].astype(F32)
    small[...] = jnp.zeros_like(small)
    small_out[...] = jnp.zeros_like(small_out)
    barrier = pltpu.get_barrier_semaphore()
    for peer in peers:
        pl.semaphore_signal(barrier, inc=1, device_id={"tp": peer}, device_id_type=MESH)

    @pl.when(not_first)
    def _():
        pl.semaphore_signal(barrier, inc=1, device_id={"pp": stage - 1}, device_id_type=MESH)

    @pl.when(not_last)
    def _():
        pl.semaphore_signal(barrier, inc=1, device_id={"pp": stage + 1}, device_id_type=MESH)

    @pl.when(helped | helping)
    def _():
        for there in (me, across):
            pl.semaphore_signal(barrier, inc=1, device_id={"pp": mate, "tp": there}, device_id_type=MESH)

    @pl.when(eased | easing)
    def _():
        for there in (me, across):
            pl.semaphore_signal(barrier, inc=1, device_id={"pp": far, "tp": there}, device_id_type=MESH)

    near = tp - 1 + jnp.minimum(stage, 1) + jnp.minimum(last - stage, 1)
    pl.semaphore_wait(barrier, near + jnp.where(helped | helping, 2, 0) + jnp.where(eased | easing, 2, 0))

    def shard(w_idx, origin):
        if w_idx == 1:
            return wo.at[pl.ds(pl.multiple_of(origin * group, group), group)]
        return (wq, None, w1, w2)[w_idx].at[origin]

    owns = (wq_own, wo_own, w1_own, w2_own)

    def half(ref, idx):
        size = ref.shape[0] // 2
        return ref.at[pl.ds(idx * size, size)]

    def ring_copy(w_idx, h_idx, side):
        return remote(half(owns[w_idx], h_idx), half(shard(w_idx, me), h_idx),
                      ring_send.at[w_idx, h_idx, side], ring_recv.at[w_idx, h_idx, side], "tp", left if side else right)

    def forward_copy(w_idx, side):
        block = half(shard(w_idx, right if side else left), side)
        return remote(block, block, fwd_send.at[w_idx, side], fwd_recv.at[w_idx, side], "tp", left if side else right)

    def bias_copy(slot):
        return remote(bias_own, bias.at[me], bias_send.at[slot], bias_recv.at[slot], "tp", peers[slot])

    def detour(src, dst, send, recv, target, target_tp):
        return pltpu.make_async_remote_copy(src_ref=src, dst_ref=dst, send_sem=send, recv_sem=recv,
                                            device_id={"pp": target, "tp": target_tp}, device_id_type=MESH)

    routes = ((2, 0, land_one, mate), (2, 1, land_one, far), (3, None, land_two, far), (1, None, land_out, mate))

    def piece(ref, h_idx):
        return ref if h_idx is None else half(ref, h_idx)

    def lw_copy(idx):
        w_idx, h_idx, land, target = routes[idx]
        return detour(piece(owns[w_idx], h_idx), piece(land, h_idx), lw_send.at[idx], lw_recv.at[idx], target, across)

    def lf_copy(idx):
        w_idx, h_idx, land, target = routes[idx]
        return detour(piece(land, h_idx), piece(shard(w_idx, across), h_idx), lf_send.at[idx], lf_recv.at[idx], target, me)

    own_copies = [pltpu.make_async_copy(owns[w_idx], shard(w_idx, me), own_sem.at[w_idx]) for w_idx in range(4)]
    own_copies.append(pltpu.make_async_copy(bias_own, bias.at[me], own_sem.at[4]))
    for own_copy in own_copies:
        own_copy.start()
    for slot in range(tp - 1):
        bias_copy(slot).start()

    def own_input(src, buf, dst):
        bounce = (y_buf, mid, gmid)
        copies = [pltpu.make_async_copy(src.at[me], buf, own_sem.at[5])]
        copies += [pltpu.make_async_copy(src.at[peers[slot]], bounce[slot], own_sem.at[6 + slot]) for slot in range(tp - 1)]
        for copy in copies:
            copy.start()
        for copy in copies:
            copy.wait()
        copies = [pltpu.make_async_copy(bounce[slot], dst.at[peers[slot]], own_sem.at[6 + slot]) for slot in range(tp - 1)]
        for copy in copies:
            copy.start()
        for copy in copies:
            copy.wait()

    @pl.when(eased)
    def _():
        for idx in range(4):
            lw_copy(idx).start()

    @pl.when(stage == middle + 1)
    def _():
        for idx in (0, 3):
            lw_copy(idx).wait_recv()
            lf_copy(idx).start()

    @pl.when(easing)
    def _():
        for idx in (1, 2):
            lw_copy(idx).wait_recv()
            lf_copy(idx).start()

    @pl.when(jnp.logical_not(even))
    def _():
        pl.semaphore_wait(go_sem, 1)

    for w_idx in range(4):
        for h_idx in range(2):
            ring_copy(w_idx, h_idx, 0).start()
            ring_copy(w_idx, 1 - h_idx, 1).start()

    @pl.when(stage == 0)
    def _():
        own_input(x_flat, x_buf, x_all)

    @pl.when(stage == last)
    def _():
        own_input(dy_flat, dy_buf, dy_all)

    qkv[...] = jnp.zeros_like(qkv)
    dkv[...] = jnp.zeros_like(dkv)

    for w_idx in range(4):
        for side in range(2):
            ring_copy(w_idx, side, side).wait_recv()
            if w_idx == 0:
                forward_copy(w_idx, side).start()
            else:
                @pl.when(jnp.logical_not(eased))
                def _():
                    forward_copy(w_idx, side).start()
    @pl.when(even)
    def _():
        pl.semaphore_signal(go_sem, inc=1, device_id={"pp": stage + 1}, device_id_type=MESH)

    for own_copy in own_copies:
        own_copy.wait()
    for slot in range(tp - 1):
        bias_copy(slot).wait()
    for w_idx in range(4):
        ring_copy(w_idx, 1, 0).wait_recv()
        ring_copy(w_idx, 0, 1).wait_recv()
        for h_idx in range(2):
            ring_copy(w_idx, h_idx, 0).wait_send()
            ring_copy(w_idx, h_idx, 1).wait_send()
    for side in range(2):
        forward_copy(0, side).wait()

    @pl.loop(0, tp)
    def _(t_idx):
        for part in range(3):
            wq_t[t_idx, :, part * group:(part + 1) * group] = wq[t_idx, part * group:(part + 1) * group, :].T

    @pl.when(jnp.logical_not(eased))
    def _():
        for w_idx in (1, 2, 3):
            for side in range(2):
                forward_copy(w_idx, side).wait()

    @pl.when(eased)
    def _():
        for idx in range(4):
            lf_copy(idx).wait_recv()
            lw_copy(idx).wait_send()

    @pl.when(stage == middle + 1)
    def _():
        for idx in (0, 3):
            lf_copy(idx).wait_send()

    @pl.when(easing)
    def _():
        for idx in (1, 2):
            lf_copy(idx).wait_send()

    @pl.when(jnp.logical_not(even))
    def _():
        pl.semaphore_signal(done_sem, inc=1, device_id={"pp": stage - 1}, device_id_type=MESH)

    lane_head = lax.broadcasted_iota(jnp.int32, (chunk, group), 1) // head_dim

    def stack_heads(block):
        zero = jnp.zeros_like(block)
        return jnp.concatenate([jnp.where(lane_head == h_idx, block, zero) for h_idx in range(heads)], axis=0)

    def unstack_heads(stacked):
        total = stacked[:chunk]
        for h_idx in range(1, heads):
            total = jnp.where(lane_head == h_idx, stacked[h_idx * chunk:(h_idx + 1) * chunk], total)
        return total

    def hop_copy(c_idx, forward):
        rows = pl.ds(c_idx * chunk, chunk)
        src, dst, way, target = (y_buf, x_buf, 0, stage + 1) if forward else (gin, dy_buf, 1, stage - 1)
        return remote(src.at[rows], dst.at[rows], hop_send.at[way, c_idx], hop_recv.at[way, c_idx], "pp", target)

    size = group

    def flip(ref_get, ref_set, count):
        for row in range(count):
            ref_set(row, row, ref_get(row, row).T)
            for col in range(row):
                upper, lower = ref_get(col, row).T, ref_get(row, col).T
                ref_set(row, col, upper)
                ref_set(col, row, lower)

    def tile(row, col):
        return slice(row * size, (row + 1) * size), slice(col * size, (col + 1) * size)

    def flip_ff(ref, t_idx):
        def ref_set(row, col, value):
            ref[(t_idx,) + tile(row, col)] = value

        flip(lambda row, col: ref[(t_idx,) + tile(row, col)], ref_set, d_model // size)

    def flip_wo():
        def ref_set(row, col, value):
            wo[tile(row, col)] = value

        flip(lambda row, col: wo[tile(row, col)], ref_set, d_model // size)

    def layer_rows(c_idx, rows, flipping):
        normed, _ = norm_stats(x_buf[rows, :].astype(F32))
        hbuf[...] = (normed * rep[0:1, :] + rep[1:2, :]).astype(BF16)

        groups = range(tp)
        for t_idx in groups:
            pre = dot_nn(hbuf[...], wq_t[t_idx]) + bias[t_idx, 1:2, :3 * group]
            for part in range(3):
                qkv[part, t_idx, rows, :] = pre[:, part * group:(part + 1) * group].astype(BF16)

        row_pos = c_idx * chunk + lax.rem(lax.broadcasted_iota(jnp.int32, (heads * chunk, seq_len), 0), chunk)
        causal = row_pos >= lax.broadcasted_iota(jnp.int32, (heads * chunk, seq_len), 1)
        all_scores = [dot_nt(stack_heads(qkv[0, t_idx, rows, :]), qkv[1, t_idx]) for t_idx in groups]
        all_probs = []
        for t_idx in groups:
            scores = jnp.where(causal, all_scores[t_idx], -1e30)
            expd = jnp.exp2((scores - jnp.max(scores, axis=-1, keepdims=True)) * (score_scale * LOG2_E))
            probs = expd * (1.0 / jnp.sum(expd, axis=-1, keepdims=True))
            prob[c_idx, t_idx] = probs
            all_probs.append(probs.astype(BF16))
        for t_idx in groups:
            mix[t_idx, rows, :] = unstack_heads(dot_nn(all_probs[t_idx], qkv[2, t_idx])).astype(BF16)

        full_mix = jnp.concatenate([mix[t_idx, rows, :] for t_idx in groups], axis=1)
        x_mid = (x_buf[rows, :].astype(F32) + dot_nn(full_mix, wo[...]) + rep[4:5, :]).astype(BF16)
        mid[rows, :] = x_mid
        if flipping:
            flip_wo()
        normed_two, _ = norm_stats(x_mid.astype(F32))
        hbuf[...] = (normed_two * rep[2:3, :] + rep[3:4, :]).astype(BF16)
        total = jnp.zeros((chunk, d_model), F32)
        for t_idx in groups:
            pre = dot_nn(hbuf[...], w1[t_idx]) + bias[t_idx, 0:1, :]
            cdf, slope = gelu_parts(pre)
            dgelu[t_idx, rows, :] = slope
            total = total + dot_nn((pre * cdf).astype(BF16), w2[t_idx])
            if flipping:
                flip_ff(w1, t_idx)

        y_buf[rows, :] = (mid[rows, :].astype(F32) + total + rep[5:6, :]).astype(BF16)

    gathers = ((y_buf, h_all), (mid, mid_all), (gin, gin_all))

    def row_copy(kind, c_idx, side):
        rows = pl.ds(c_idx * chunk, chunk)
        src, dst = gathers[kind]
        return remote(src.at[rows], dst.at[me, rows], row_send.at[kind, c_idx, side], row_recv.at[kind, c_idx, side], "tp", left if side else right)

    def row_forward(kind, c_idx, side):
        rows = pl.ds(c_idx * chunk + side * (chunk // 2), chunk // 2)
        block = gathers[kind][1].at[right if side else left, rows]
        return remote(block, block, row_send.at[kind, c_idx, 2 + side], row_recv.at[kind, c_idx, 2 + side], "tp", left if side else right)

    def start_rows(c_idx):
        for kind in range(2):
            for side in range(2):
                row_copy(kind, c_idx, side).start()

    prompt = (stage >= middle) | jnp.logical_not(even)

    def fwd_chunk(c_idx, carry):
        rows = pl.ds(pl.multiple_of(c_idx * chunk, chunk), chunk)

        @pl.when(not_first)
        def _():
            hop_copy(c_idx, True).wait_recv()

        turning = (stage == last) & (c_idx == chunks - 1)

        @pl.when(jnp.logical_not(turning))
        def _():
            layer_rows(c_idx, rows, False)

        @pl.when(turning)
        def _():
            layer_rows(c_idx, rows, True)

        @pl.when(not_last)
        def _():
            hop_copy(c_idx, True).start()

        @pl.when(prompt & even & (c_idx == 0))
        def _():
            pl.semaphore_wait(done_sem, 1)

        @pl.when(prompt)
        def _():
            start_rows(c_idx)

        return carry

    lax.fori_loop(0, chunks, fwd_chunk, 0)

    def mix_copy(slot):
        return remote(mix.at[peers[slot]], mix_all.at[me], mix_send.at[slot], mix_recv.at[slot], "tp", peers[slot])

    for slot in range(tp - 1):
        mix_copy(slot).start()
    fwd_out = [pltpu.make_async_copy(y_buf, h_all.at[me], out_sem.at[0]),
               pltpu.make_async_copy(mid, mid_all.at[me], out_sem.at[1]),
               pltpu.make_async_copy(mix.at[me], mix_all.at[me], out_sem.at[2]),
               pltpu.make_async_copy(x_buf, x_all.at[me], out_sem.at[3])]
    for out_copy in fwd_out:
        out_copy.start()

    def pass_x(slot):
        origin = peers[slot]
        return remote(h_all.at[origin], x_all.at[origin], px_send.at[slot], px_recv.at[slot], "pp", stage + 1)

    def forward_fwd_gather():
        for c_idx in range(chunks):
            for kind in range(2):
                for side in range(2):
                    row_copy(kind, c_idx, side).wait_recv()
                    row_forward(kind, c_idx, side).start()

    def finish_fwd_gather():
        for c_idx in range(chunks):
            for kind in range(2):
                for side in range(2):
                    row_forward(kind, c_idx, side).wait_recv()

        @pl.when(not_last)
        def _():
            for slot in range(tp - 1):
                pass_x(slot).start()

    @pl.loop(0, tp)
    def _(t_idx):
        flip_ff(w2, t_idx)

    @pl.when(not_last)
    def _():
        @pl.loop(0, tp)
        def _(t_idx):
            flip_ff(w1, t_idx)

        flip_wo()

    @pl.when(jnp.logical_not(prompt))
    def _():
        pl.semaphore_wait(done_sem, 1)
        for c_idx in range(chunks):
            start_rows(c_idx)

    @pl.when(stage < last - 1)
    def _():
        forward_fwd_gather()

    @pl.when(stage < stages // 2)
    def _():
        finish_fwd_gather()

    def gm_copy(side):
        return remote(gmid, gmid_all.at[me], gm_send.at[side], gm_recv.at[side], "tp", left if side else right)

    def gm_forward(side):
        rows = pl.ds(side * (seq_len // 2), seq_len // 2)
        block = gmid_all.at[right if side else left, rows]
        return remote(block, block, gm_send.at[2 + side], gm_recv.at[2 + side], "tp", left if side else right)

    def gqkv_of(t_idx):
        return wq_t.at[t_idx, pl.ds(0, seq_len)]

    def gq_copy(slot):
        return remote(gqkv_of(peers[slot]), gqkv_all.at[me], gq_send.at[slot], gq_recv.at[slot], "tp", peers[slot])

    gm_way = jnp.where(eased | easing, far, mate)
    gm_helping = (stage == middle) | easing

    def gl_copy(idx):
        return detour(gmid if idx else gqkv_of(across), land_gm if idx else land_gq, lg_send.at[idx], lg_recv.at[idx], gm_way if idx else mate, across)

    def gf_copy(idx):
        return detour(land_gm if idx else land_gq, (gmid_all if idx else gqkv_all).at[across], lg_send.at[2 + idx], lg_recv.at[2 + idx], gm_way if idx else mate, me)

    def pass_dy(c_idx, slot):
        rows = pl.ds(c_idx * chunk, chunk)
        origin = peers[slot]
        return remote(gin_all.at[origin, rows], dy_all.at[origin, rows], py_send.at[c_idx, slot], py_recv.at[c_idx, slot], "pp", stage - 1)

    def forward_chunk(c_idx):
        for side in range(2):
            row_copy(2, c_idx, side).wait_recv()
            row_forward(2, c_idx, side).start()

    def pass_chunk(c_idx):
        for side in range(2):
            row_forward(2, c_idx, side).wait_recv()

        @pl.when(not_first)
        def _():
            for slot in range(tp - 1):
                pass_dy(c_idx, slot).start()

    w1_own_t, w2_own_t = w1.at[me], w2.at[me]
    early = stage < stages // 2 - 1

    def prep(two_buf, one_buf, act_buf, keep_slopes):
        @pl.when(not_first)
        def _():
            for slot in range(tp - 1):
                pass_x(slot).wait_recv()

        def prep_seq(t_idx, carry):
            loads = [pltpu.make_async_copy(mid_all.at[t_idx], two_buf, prep_sem.at[0]), pltpu.make_async_copy(x_all.at[t_idx], one_buf, prep_sem.at[1])]
            for load in loads:
                load.start()
            for load in loads:
                load.wait()

            def prep_rows(c_idx, inner):
                rows = pl.ds(pl.multiple_of(c_idx * chunk, chunk), chunk)
                normed, _ = norm_stats(two_buf[rows, :].astype(F32))
                two_buf[rows, :] = (normed * rep[2:3, :] + rep[3:4, :]).astype(BF16)
                normed_one, _ = norm_stats(one_buf[rows, :].astype(F32))
                one_buf[rows, :] = (normed_one * rep[0:1, :] + rep[1:2, :]).astype(BF16)
                pre = dot_nt(two_buf[rows, :], w1_own_t[...]) + bias[me, 0:1, :]
                cdf, slope = gelu_parts(pre)
                act_buf[rows, :] = (pre * cdf).astype(BF16)
                if keep_slopes:
                    keep = pltpu.make_async_copy(acc, slope_all.at[t_idx, rows], prep_sem.at[2])

                    @pl.when(c_idx > 0)
                    def _():
                        keep.wait()

                    acc[...] = slope
                    keep.start()
                else:
                    dgelu[t_idx, rows, :] = slope
                return inner

            lax.fori_loop(0, chunks, prep_rows, 0)
            if keep_slopes:
                pltpu.make_async_copy(acc, slope_all.at[t_idx, pl.ds(0, chunk)], prep_sem.at[2]).wait()
            keeps = [pltpu.make_async_copy(two_buf, h_two_all.at[t_idx], prep_sem.at[0]), pltpu.make_async_copy(one_buf, h_one_all.at[t_idx], prep_sem.at[1]),
                     pltpu.make_async_copy(act_buf, act_all.at[t_idx], prep_sem.at[2])]
            for keep in keeps:
                keep.start()
            for keep in keeps:
                keep.wait()
            return carry

        lax.fori_loop(0, tp, prep_seq, 0)

    def end_fwd_sends():
        for c_idx in range(chunks):
            for kind in range(2):
                for side in range(2):
                    row_copy(kind, c_idx, side).wait_send()
        for slot in range(tp - 1):
            mix_copy(slot).wait_send()
        for out_copy in fwd_out:
            out_copy.wait()

        @pl.when(not_last)
        def _():
            for c_idx in range(chunks):
                hop_copy(c_idx, True).wait_send()

    @pl.when(early)
    def _():
        end_fwd_sends()
        prep(gmid, gin, y_buf, True)

    def bwd_chunk(step, carry):
        c_idx = chunks - 1 - step
        rows = pl.ds(pl.multiple_of(c_idx * chunk, chunk), chunk)

        @pl.when(not_last)
        def _():
            hop_copy(c_idx, False).wait_recv()

        groups = range(tp)
        g_h_sum = jnp.zeros((chunk, d_model), F32)
        for t_idx in groups:
            g_gelu = dot_nn(dy_buf[rows, :], w2[t_idx]).astype(BF16).astype(F32)
            g_h_sum = g_h_sum + dot_nn((g_gelu * dgelu[t_idx, rows, :]).astype(BF16), w1[t_idx])

        g_h_two = g_h_sum.astype(BF16).astype(F32)
        dy_wide = dy_buf[rows, :].astype(F32)
        g_ln, g_gain, g_shift = norm_backward(mid[rows, :].astype(F32), rep[2:3, :], g_h_two)
        g_mid = (dy_wide + g_ln.astype(BF16).astype(F32)).astype(BF16)
        gmid[rows, :] = g_mid
        small[me, 2:3, :] += g_gain
        small[me, 3:4, :] += g_shift
        small[me, 4:5, :] += jnp.sum(g_mid.astype(F32), axis=0, keepdims=True)
        small[me, 5:6, :] += jnp.sum(dy_wide, axis=0, keepdims=True)
        hbuf[...] = dot_nn(gmid[rows, :], wo[...]).astype(BF16)
        g_stacks = [stack_heads(hbuf[:, t_idx * group:(t_idx + 1) * group]) for t_idx in groups]
        g_probs = [dot_nt(g_stacks[t_idx], qkv[2, t_idx]).astype(BF16).astype(F32) for t_idx in groups]
        g_values = [dot_tn(prob[c_idx, t_idx, :, rows].astype(BF16), g_stacks[t_idx]) for t_idx in groups]
        for t_idx in groups:
            probs = prob[c_idx, t_idx]
            inner = jnp.sum(g_probs[t_idx] * probs, axis=-1, keepdims=True)
            gscore[t_idx] = (probs * (g_probs[t_idx] - inner)).astype(BF16)
            wq_t[t_idx, rows, 2 * group:3 * group] = (dkv[1, t_idx, rows, :] + g_values[t_idx]).astype(BF16)
        for t_idx in groups:
            wq_t[t_idx, rows, 0:group] = (unstack_heads(dot_nn(gscore[t_idx], qkv[1, t_idx])) * score_scale).astype(BF16)
            g_keys = dot_tn(gscore[t_idx, :, rows], stack_heads(qkv[0, t_idx, rows, :]))
            wq_t[t_idx, rows, group:2 * group] = ((dkv[0, t_idx, rows, :] + g_keys) * score_scale).astype(BF16)
        g_h_sum = jnp.zeros((chunk, d_model), F32)
        for t_idx in groups:
            g_h_sum = g_h_sum + dot_nn(wq_t[t_idx, rows, :], wq[t_idx])

        g_h_one = g_h_sum.astype(BF16).astype(F32)
        g_ln_one, g_gain_one, g_shift_one = norm_backward(x_buf[rows, :].astype(F32), rep[0:1, :], g_h_one)
        gin[rows, :] = (gmid[rows, :].astype(F32) + g_ln_one.astype(BF16).astype(F32)).astype(BF16)
        small[me, 0:1, :] += g_gain_one
        small[me, 1:2, :] += g_shift_one

        @pl.when(not_first)
        def _():
            hop_copy(c_idx, False).start()

        for side in range(2):
            row_copy(2, c_idx, side).start()

        def earlier_rows(block, inner):
            keys = pl.ds(pl.multiple_of(block * chunk, chunk), chunk)
            for t_idx in groups:
                dkv[0, t_idx, keys, :] += dot_tn(gscore[t_idx, :, keys], stack_heads(qkv[0, t_idx, rows, :]))
                g_stack = stack_heads(hbuf[:, t_idx * group:(t_idx + 1) * group])
                dkv[1, t_idx, keys, :] += dot_tn(prob[c_idx, t_idx, :, keys].astype(BF16), g_stack)
            return inner

        lax.fori_loop(0, c_idx, earlier_rows, 0)

        @pl.when((step >= 2) & (stage < last - 1))
        def _():
            forward_chunk(c_idx + 2)

        return carry

    lax.fori_loop(0, chunks, bwd_chunk, 0)

    def sum_copy(slot):
        return remote(small.at[me], small.at[me], sum_send.at[slot], sum_recv.at[slot], "tp", peers[slot])

    for slot in range(tp - 1):
        sum_copy(slot).start()
    bwd_out = [pltpu.make_async_copy(gin, gin_all.at[me], out_sem.at[4]),
               pltpu.make_async_copy(gmid, gmid_all.at[me], out_sem.at[5]),
               pltpu.make_async_copy(gqkv_of(me), gqkv_all.at[me], out_sem.at[6]),
               pltpu.make_async_copy(dy_buf, dy_all.at[me], out_sem.at[7])]
    for out_copy in bwd_out:
        out_copy.start()

    @pl.when(helped)
    def _():
        for idx in range(2):
            gl_copy(idx).start()


    @pl.when((stage >= stages // 2) & (stage < last - 1))
    def _():
        finish_fwd_gather()

    @pl.when(stage >= last - 1)
    def _():
        forward_fwd_gather()
        forward_chunk(chunks - 1)

    for c_idx in range(chunks - 2, -1, -1):
        forward_chunk(c_idx)

    @pl.when(stage >= last - 1)
    def _():
        finish_fwd_gather()

    for side in range(2):
        gm_copy(side).start()
    for slot in (0, 2, 1):
        if slot == 1:
            @pl.when(jnp.logical_not(helped))
            def _():
                gq_copy(slot).start()
        else:
            gq_copy(slot).start()

    def pass_all():
        for c_idx in range(chunks - 1, -1, -1):
            pass_chunk(c_idx)

    @pl.when(not_last)
    def _():
        pass_all()

    @pl.when(early)
    def _():
        slopes = pltpu.make_async_copy(slope_all, dgelu, prep_sem.at[0])
        slopes.start()
        slopes.wait()

    @pl.when(jnp.logical_not(early))
    def _():
        end_fwd_sends()
        prep(mid, x_buf, y_buf, False)

    @pl.when(stage == last)
    def _():
        pass_all()

    def finish_rows(t_idx, src, dst, rows):
        grad = dot_nn(src[rows, :], w2_own_t[...]).astype(BF16).astype(F32) * dgelu[t_idx, rows, :]
        small_out[6:7, :] += jnp.sum(grad, axis=0, keepdims=True)
        dst[rows, :] = grad.astype(BF16)

    def finish_own(c_idx, carry):
        finish_rows(me, dy_buf, y_buf, pl.ds(pl.multiple_of(c_idx * chunk, chunk), chunk))
        return carry

    lax.fori_loop(0, chunks, finish_own, 0)
    own_keep = pltpu.make_async_copy(y_buf, gpre_all.at[me], prep_sem.at[0])
    own_keep.start()
    @pl.when(helping)
    def _():
        gl_copy(0).wait_recv()
        gf_copy(0).start()

    @pl.when(gm_helping)
    def _():
        gl_copy(1).wait_recv()
        gf_copy(1).start()

    @pl.when(jnp.logical_not(helped))
    def _():
        for side in range(2):
            gm_copy(side).wait_recv()
            gm_forward(side).start()

    own_keep.wait()

    def finish_peers(step, carry):
        c_idx = chunks - 1 - step
        rows = pl.ds(pl.multiple_of(c_idx * chunk, chunk), chunk)
        bufs = (x_buf, mid, y_buf)

        @pl.when(not_last)
        def _():
            for slot in range(tp - 1):
                pass_dy(c_idx, slot).wait_recv()

        loads = [pltpu.make_async_copy(dy_all.at[peers[slot], rows], bufs[slot].at[rows], post_sem.at[slot]) for slot in range(tp - 1)]
        keeps = [pltpu.make_async_copy(bufs[slot].at[rows], gpre_all.at[peers[slot], rows], post_sem.at[slot]) for slot in range(tp - 1)]
        for load in loads:
            load.start()
        for slot in range(tp - 1):
            loads[slot].wait()
            finish_rows(peers[slot], bufs[slot], bufs[slot], rows)
            keeps[slot].start()
        for keep in keeps:
            keep.wait()
        return carry

    lax.fori_loop(0, chunks, finish_peers, 0)
    for slot in range(tp - 1):
        sum_copy(slot).wait()
    total_small = small[0, 0:6, :]
    for t_idx in range(1, tp):
        total_small = total_small + small[t_idx, 0:6, :]
    small_out[0:6, :] = total_small

    for slot in range(tp - 1):
        mix_copy(slot).wait_recv()
        if slot != 1:
            gq_copy(slot).wait()

    @pl.when(jnp.logical_not(helped))
    def _():
        gq_copy(1).wait()
        for side in range(2):
            gm_forward(side).wait()

    @pl.when(helped)
    def _():
        for side in range(2):
            gm_copy(side).wait_recv()
        for idx in range(2):
            gl_copy(idx).wait_send()
            gf_copy(idx).wait_recv()

    @pl.when(helping)
    def _():
        gf_copy(0).wait_send()

    @pl.when(gm_helping)
    def _():
        gf_copy(1).wait_send()

    for side in range(2):
        gm_copy(side).wait_send()
        for c_idx in range(chunks):
            for kind in range(2):
                row_forward(kind, c_idx, side).wait_send()
            row_copy(2, c_idx, side).wait_send()
            row_forward(2, c_idx, side).wait_send()
    for out_copy in bwd_out:
        out_copy.wait()

    @pl.when(not_last)
    def _():
        for slot in range(tp - 1):
            pass_x(slot).wait_send()

    @pl.when(not_first)
    def _():
        for c_idx in range(chunks):
            hop_copy(c_idx, False).wait_send()
            for slot in range(tp - 1):
                pass_dy(c_idx, slot).wait_send()


def run_chain(stages, tp, x_flat, dy_flat, wq, wo, w1, w2, ln_par, b_qkv, b_out, b_one, b_two, head_dim):
    _, seq_len, d_model = x_flat.shape
    chunk = min(128, seq_len)
    chunks = seq_len // chunk
    group = wo.shape[0]
    heads = group // head_dim
    ff_local = w1.shape[1]
    rows = (tp, seq_len, d_model)
    outs = [jax.ShapeDtypeStruct(rows, BF16)] * 4
    outs += [jax.ShapeDtypeStruct((tp, seq_len, group), BF16), jax.ShapeDtypeStruct((tp, seq_len, 3 * group), BF16)]
    outs += [jax.ShapeDtypeStruct(rows, BF16)] * 4 + [jax.ShapeDtypeStruct((tp, seq_len, ff_local), BF16)] * 2
    outs += [jax.ShapeDtypeStruct((tp, seq_len, ff_local), F32), jax.ShapeDtypeStruct(w1.shape, BF16), jax.ShapeDtypeStruct(w2.shape, BF16)]
    outs += [jax.ShapeDtypeStruct(wo.shape, BF16)]
    outs += [jax.ShapeDtypeStruct((seq_len, 3 * group), BF16), jax.ShapeDtypeStruct((seq_len, d_model), BF16), jax.ShapeDtypeStruct((8, d_model), F32)]
    act = pltpu.VMEM((seq_len, d_model), BF16)
    dma = pltpu.SemaphoreType.DMA
    scratch = [
        pltpu.VMEM((tp,) + wq.shape, BF16), pltpu.VMEM((tp,) + wq.shape[::-1], BF16), pltpu.VMEM((tp * group, d_model), BF16),
        pltpu.VMEM((tp,) + w1.shape, BF16), pltpu.VMEM((tp,) + w2.shape, BF16),
        pltpu.VMEM((tp, 8, d_model), F32),
        act, act,
        pltpu.VMEM((3, tp, seq_len, group), BF16), pltpu.VMEM((tp, seq_len, group), BF16),
        act, act, act, act,
        pltpu.VMEM((2, tp, seq_len, group), F32),
        pltpu.VMEM((chunks, tp, heads * chunk, seq_len), F32), pltpu.VMEM((tp, seq_len, ff_local), F32),
        pltpu.VMEM((chunk, d_model), F32), pltpu.VMEM((chunk, d_model), BF16), pltpu.VMEM((tp, 8, d_model), F32),
        pltpu.VMEM((8, d_model), F32), pltpu.VMEM((8, d_model), F32), pltpu.VMEM((tp, heads * chunk, seq_len), BF16),
        dma((9,)), pltpu.SemaphoreType.REGULAR, pltpu.SemaphoreType.REGULAR, dma((4, 2, 2)), dma((4, 2, 2)), dma((4, 2)), dma((4, 2)), dma((tp - 1,)), dma((tp - 1,)),
        dma((2, chunks)), dma((2, chunks)), dma((4,)), dma((4,)), dma((tp - 1,)), dma((tp - 1,)),
        dma((3, chunks, 4)), dma((3, chunks, 4)), dma((tp - 1,)), dma((tp - 1,)),
        dma((8,)), dma((tp - 1,)), dma((tp - 1,)), dma((chunks, tp - 1)), dma((chunks, tp - 1)), dma((tp - 1,)), dma((tp - 1,)), dma((3,)), dma((tp - 1,)),
        dma((4,)), dma((4,)), dma((4,)), dma((4,)), dma((4,)), dma((4,)),
    ]
    return pl.pallas_call(
        functools.partial(chain_kernel, stages, tp, chunk, head_dim),
        out_shape=outs,
        in_specs=[ANY] * 6 + [VMEM] * 5,
        out_specs=[ANY] * 18 + [VMEM],
        scratch_shapes=scratch,
        compiler_params=pltpu.CompilerParams(collective_id=0, has_side_effects=True, vmem_limit_bytes=67043328),
        name="chain",
    )(x_flat, dy_flat, wq, wo, w1, w2, ln_par, b_qkv, b_out, b_one, b_two)


def wgrad_kernel(act, dy, gpre, h_two, gqkv, h_one, mix, gmid, h_all, gin_all, small,
                 gw_two, gw_one, gw_qkv, gw_out, h_out, g_in, g_ln, gb_out, gb_two, gb_one, gb_qkv,
                 act_v, dy_v, gpre_v, h_two_v, gq_v, h_one_v, mix_v, gmid_v, h_v, gin_v, two_v, one_v, qkv_v, out_v,
                 in_sem, two_sem, one_sem, qkv_sem, res_sem, keep_sem):
    heads, head_dim = gb_qkv.shape[1:]
    group = heads * head_dim
    pairs = ((act, act_v), (dy, dy_v), (gpre, gpre_v), (h_two, h_two_v), (gqkv, gq_v), (h_one, h_one_v), (mix, mix_v), (gmid, gmid_v), (h_all, h_v), (gin_all, gin_v))
    loads = [pltpu.make_async_copy(src, dst, in_sem.at[idx]) for idx, (src, dst) in enumerate(pairs)]
    for load in loads:
        load.start()
    g_ln[...] = small[0:4, :]
    gb_out[...] = small[4:5, :]
    gb_two[...] = small[5:6, :]
    gb_one[...] = small[6:7, :]

    def product(lhs, rhs, buf, dst, sem, tiles):
        tile = buf.shape[0] // tiles

        def copy_of(row):
            rows = pl.ds(pl.multiple_of(row * tile, tile), tile)
            return pltpu.make_async_copy(buf.at[rows], dst.at[rows], sem.at[row])

        @pl.loop(0, tiles)
        def _(row):
            cols = pl.ds(pl.multiple_of(row * tile, tile), tile)
            buf[cols, :] = dot_tn(lhs[:, cols], rhs[...])
            copy_of(row).start()

        return lambda: [copy_of(row).wait() for row in range(tiles)]

    loads[0].wait()
    loads[1].wait()
    ends = [product(act_v, dy_v, two_v, gw_two, two_sem, 2)]
    loads[2].wait()
    loads[3].wait()
    ends.append(product(h_two_v, gpre_v, one_v, gw_one, one_sem, 2))
    loads[8].wait()
    loads[9].wait()
    keeps = [pltpu.make_async_copy(h_v, h_out, keep_sem.at[0]), pltpu.make_async_copy(gin_v, g_in, keep_sem.at[1])]
    for keep in keeps:
        keep.start()
    loads[4].wait()
    loads[5].wait()
    ends.append(product(gq_v, h_one_v, qkv_v, gw_qkv, qkv_sem, 2))
    for part in range(3):
        total = jnp.sum(gq_v[:, part * group:(part + 1) * group].astype(F32), axis=0, keepdims=True)
        for h_idx in range(heads):
            gb_qkv[part, h_idx:h_idx + 1, :] = total[:, h_idx * head_dim:(h_idx + 1) * head_dim]
    loads[6].wait()
    loads[7].wait()
    ends.append(product(mix_v, gmid_v, out_v, gw_out, res_sem, 1))
    for end in ends:
        end()
    for keep in keeps:
        keep.wait()


def run_wgrad(act, dy, gpre, h_two, gqkv, h_one, mix, gmid, h_all, gin_all, small, head_dim):
    def flat(array):
        return array.reshape(array.shape[0] * array.shape[1], array.shape[2])

    group, d_model, ff_local = mix.shape[2], dy.shape[2], act.shape[2]
    seqs, seq_len = dy.shape[:2]
    total = seqs * seq_len
    dma = pltpu.SemaphoreType.DMA
    grads = [(ff_local, d_model), (d_model, ff_local), (3 * group, d_model), (group, d_model)]
    rows = jax.ShapeDtypeStruct((total, d_model), BF16)
    smalls = [(4, d_model), (1, d_model), (1, d_model), (1, ff_local), (3, group // head_dim, head_dim)]
    widths = (ff_local, d_model, ff_local, d_model)
    return pl.pallas_call(
        wgrad_kernel,
        in_specs=[ANY] * 10 + [VMEM],
        out_specs=[ANY] * 6 + [VMEM] * 5,
        out_shape=[jax.ShapeDtypeStruct(shape, F32) for shape in grads] + [rows, rows] + [jax.ShapeDtypeStruct(shape, F32) for shape in smalls],
        scratch_shapes=[pltpu.VMEM((total, width), BF16) for width in widths]
        + [pltpu.VMEM((total, 3 * group), BF16), pltpu.VMEM((total, d_model), BF16), pltpu.VMEM((total, group), BF16)]
        + [pltpu.VMEM((total, d_model), BF16)] * 3 + [pltpu.VMEM(shape, F32) for shape in grads]
        + [dma((10,))] + [dma((shape[0] // group,)) for shape in grads] + [dma((2,))],
        compiler_params=pltpu.CompilerParams(vmem_limit_bytes=67043328),
        name="wgrad",
    )(flat(act), flat(dy), flat(gpre), flat(h_two), flat(gqkv), flat(h_one), flat(mix), flat(gmid), flat(h_all), flat(gin_all), small)


def solution(mesh):
    stages = mesh.shape["pp"]
    tp = mesh.shape["tp"]

    def stage_program(x_in, dy_out, w_qkv, b_qkv, w_out, b_out, ln_par, w_fc1, b_fc1, w_fc2, b_fc2):
        micro_count, batch_rows, seq_len, d_model = x_in.shape
        head_dim = w_qkv.shape[4]
        group = w_qkv.shape[3] * head_dim
        heads = group // head_dim
        seqs = micro_count * batch_rows
        wq = jnp.transpose(w_qkv[0], (0, 2, 3, 1)).reshape(3 * group, d_model)
        wo = w_out[0].reshape(group, d_model)
        w1, w2 = w_fc1[0], w_fc2[0]
        x_flat = x_in.reshape(seqs, seq_len, d_model)
        dy_flat = dy_out.reshape(seqs, seq_len, d_model)
        h_all, _, gin_all, gmid_all, mix_all, gqkv_all, _, dy_all, h_one, h_two, act, gpre, _, _, _, _, _, _, small = run_chain(
            stages, tp, x_flat, dy_flat, wq, wo, w1, w2, ln_par[0], b_qkv[0], b_out, b_fc1, b_fc2, head_dim)
        gw_two, gw_one, gw_qkv, gw_out, h_out, g_in, g_ln, gb_out, gb_two, gb_one, gb_qkv = run_wgrad(
            act, dy_all, gpre, h_two, gqkv_all, h_one, mix_all, gmid_all, h_all, gin_all, small, head_dim)
        gw_qkv = jnp.transpose(gw_qkv.reshape(3, heads, head_dim, d_model), (0, 3, 1, 2))
        shape = (1, micro_count, batch_rows, seq_len, d_model)
        return (h_out.reshape(shape), g_in.reshape(shape), gw_qkv[None], gb_qkv[None], gw_out.reshape(1, heads, head_dim, d_model), gb_out,
                g_ln[None], gw_one[None], gb_one, gw_two[None], gb_two)

    act_spec = P(None, "dp", None, None)
    arg_specs = (act_spec, act_spec,
                 P("pp", None, None, "tp", None), P("pp", None, "tp", None), P("pp", "tp", None, None),
                 P("pp", None), P("pp", None, None), P("pp", None, "tp"), P("pp", "tp"),
                 P("pp", "tp", None), P("pp", None))
    stage_spec = P("pp", None, "dp", None, None)
    grad_axes = ("dp", "pp")
    result_specs = (stage_spec, stage_spec,
                    P(grad_axes, None, None, "tp", None), P(grad_axes, None, "tp", None), P(grad_axes, "tp", None, None),
                    P(grad_axes, None), P(grad_axes, None, None), P(grad_axes, None, "tp"), P(grad_axes, "tp"),
                    P(grad_axes, "tp", None), P(grad_axes, None))
    return jax.shard_map(stage_program, mesh=mesh, in_specs=arg_specs, out_specs=result_specs, check_vma=False)
```
